256 devices in a mesh: sky: 64 (over x_hi, y, z), band: 4 (over x_lo, core).
Axes of the slice: x: 4 (x_hi: 2, x_lo: 2; x = x_hi * 2 + x_lo), y: 4, z: 8, core: 2. Of those that a mesh axis runs over, the one named last changes fastest.
Arguments:
- magnitudes: float32 [4, 8, 131072], P('band', None, 'sky'), may hold values from -7 to 7
- weights: float32 [4, 8, 131072], P('band', None, 'sky'), may hold values from 0.25 to 4
- slots: int32 [4, 8, 131072], P('band', None, 'sky'), may hold values from 0 to 31, as said below
- block_fields: int32 [512, 32], P('sky'), may hold values from 0 to 4096, as said below
- owner: int32 [4096], replicated, may hold values from 0 to 63, as said below
- colors: int32 [4096], replicated, may hold values from 0 to 7
- color_terms: float32 [4, 4], replicated, may hold values from -0.25 to 0.25
Outputs:
- zero_points: float32 [4, 4096], P('band', 'sky')
- star_mags: float32 [4, 131072], P('band', 'sky')
- misfit: float32 [4, 4], P(None, 'band')
The draws below stay inside these ranges and needn't reach their ends.
Inputs may be any that keep to these rules, and one draw needn't show every extreme that they name: `block_fields`: the live entries of each list come first, are distinct, and name fields owned by the block's own sky tile or by the tiles one index below or above it, cyclically over 64 tiles; the remaining entries equal 4096. A list holds 16 or more live entries, and every tile has a block with all 32 live. `owner`: each sky tile owns exactly 64 fields. `slots`: each observation names a live entry of its block's list.
All inputs are finite; a program needn't handle non-finite values.
Results may differ from the reference program's by a relative error of at most 0.00023.
Values sent between devices are 32-bit elements; how exact they have to be, the bound alone decides.
A program may use at most 64 MiB of HBM per device.

```python
import math
import jax
import jax.numpy as jnp
from jax import lax

F = 4096
COLORS = 8
SWEEPS = 4
OBS = 8
LIST = 32
ROWS = 256
BLK_DEV = 8
NBANDS = 4
TILES = 64
F_OWN = 64
NBLOCKS = 512
NSTARS = 131072


def layout(key):
    permuted = jax.random.permutation(jax.random.fold_in(key, 1), F)
    owner = (permuted // F_OWN).astype(jnp.int32)
    inverse = jnp.argsort(permuted, stable=True)
    tile_of = jnp.arange(NBLOCKS) // BLK_DEV
    offsets = jnp.arange(3 * F_OWN)
    nearby = (tile_of[:, None] + offsets[None, :] // F_OWN - 1) % TILES * F_OWN + offsets[None, :] % F_OWN
    candidates = inverse[nearby]
    pick_keys = jax.random.split(jax.random.fold_in(key, 2), NBLOCKS)
    shuffles = jax.vmap(lambda block_key: jax.random.permutation(block_key, 3 * F_OWN))(pick_keys)[:, :LIST]
    picked = jnp.take_along_axis(candidates, shuffles, axis=1)
    live_count = jax.random.randint(jax.random.fold_in(key, 3), (NBLOCKS,), LIST // 2, LIST + 1)
    full_block = tile_of * BLK_DEV + tile_of * 5 % BLK_DEV
    live_count = live_count.at[full_block].set(LIST)
    lists = jnp.where(jnp.arange(LIST)[None, :] < live_count[:, None], picked, F).astype(jnp.int32)
    raw_bits = jax.random.randint(jax.random.fold_in(key, 4), (NBANDS, OBS, NSTARS), 0, 1 << 20)
    star_live = jnp.repeat(live_count, ROWS)
    slot_values = (raw_bits % star_live[None, None, :]).astype(jnp.int32)
    return (owner, lists, slot_values)


def draw_block_fields(key, part):
    return layout(key)[1]


def draw_owner(key, part):
    return layout(key)[0]


def draw_slots(key, part):
    return layout(key)[2]


def draw_magnitudes(key, part):
    owner, lists, slot_values = layout(key)
    expanded = jnp.broadcast_to(lists[None, None, :, :], (NBANDS, OBS, NBLOCKS, LIST))
    field_ids = jnp.take_along_axis(expanded, slot_values.reshape(NBANDS, OBS, NBLOCKS, ROWS), axis=3).reshape(NBANDS, OBS, NSTARS)
    star_tint = jax.random.uniform(jax.random.fold_in(key, 11), (NSTARS,), jnp.float32, -1.0, 1.0)
    band_slope = jax.random.uniform(jax.random.fold_in(key, 12), (NBANDS,), jnp.float32, -1.0, 1.0)
    base_mag = jax.random.uniform(jax.random.fold_in(key, 13), (NSTARS,), jnp.float32, -3.0, 3.0)
    field_off = jax.random.uniform(jax.random.fold_in(key, 14), (NBANDS, F), jnp.float32, -1.0, 1.0)
    noise_term = 0.05 * jnp.clip(jax.random.normal(jax.random.fold_in(key, 15), (NBANDS, OBS, NSTARS), jnp.float32), -2.0, 2.0)
    star_part = base_mag[None, :] + band_slope[:, None] * star_tint[None, :]
    field_part = jax.vmap(jnp.take)(field_off, field_ids)
    return (star_part[:, None, :] + field_part + noise_term).astype(jnp.float32)


def place_ends(result, own_key, least, largest):
    place = [jax.random.randint(jax.random.fold_in(own_key, axis), (), 0, length) for axis, length in enumerate(result.shape)]
    widest = result.shape.index(max(result.shape))
    next_to = place[:widest] + [(place[widest] + 1) % result.shape[widest]] + place[widest + 1:]
    return result.at[tuple(place)].set(least).at[tuple(next_to)].set(largest)


def block_scale(stream_key, extent, cuts, smallest, largest):
    gain, own = 1.0, jax.random.fold_in(stream_key, 6)
    for position, blocks in cuts:
        draws = jnp.exp(jax.random.uniform(jax.random.fold_in(own, position), (blocks,), jnp.float32, smallest / len(cuts), largest / len(cuts)))
        gain = gain * jnp.repeat(draws, extent[position] // blocks).reshape([-1 if axis == position else 1 for axis in range(len(extent))])
    return gain


def setup_inputs(seed: int = 0) -> dict:
    seeds = jax.random.split(jax.random.key(seed), 8)
    magnitudes = draw_magnitudes(jax.random.fold_in(seeds[7], 71), 0)
    weights = jnp.clip(jnp.exp(math.log(4.0) - 2.7725887 * jax.random.uniform(seeds[1], (NBANDS, OBS, NSTARS), jnp.float32) ** block_scale(seeds[1], (NBANDS, OBS, NSTARS), ((0, 4), (2, 64)), -0.2, 0.2)), 0.25, 4.0)
    slots = draw_slots(jax.random.fold_in(seeds[7], 71), 0)
    block_fields = draw_block_fields(jax.random.fold_in(seeds[7], 71), 0)
    owner = draw_owner(jax.random.fold_in(seeds[7], 71), 0)
    colors = place_ends(jax.random.randint(seeds[5], (F,), 0, COLORS), jax.random.fold_in(seeds[5], 1), 0, COLORS - 1).astype(jnp.int32)
    color_terms = jnp.clip(jax.random.uniform(seeds[6], (NBANDS, NBANDS), jnp.float32, -0.25, 0.25), -0.25, 0.25)
    return {"magnitudes": magnitudes, "weights": weights, "slots": slots, "block_fields": block_fields, "owner": owner, "colors": colors, "color_terms": color_terms}


PRIOR_WEIGHT = 1.0


def field_table(block_fields, slots):
    band_count, obs_count, star_count = slots.shape
    block_count, list_len = block_fields.shape
    block_rows = star_count // block_count
    block_slots = slots.reshape(band_count, obs_count, block_count, block_rows)
    expanded = jnp.broadcast_to(block_fields[None, None, :, :], (band_count, obs_count, block_count, list_len))
    picked = jnp.take_along_axis(expanded, block_slots, axis=3)
    return picked.reshape(band_count, obs_count, star_count).astype(jnp.int32)


def reference(magnitudes, weights, slots, block_fields, owner, colors, color_terms):
    band_count, obs_count, star_count = magnitudes.shape
    fields = owner.shape[0]
    field_ids = field_table(block_fields, slots)
    star_weight = jnp.sum(weights, axis=1)

    def segment_one(band_values, band_ids):
        return jax.ops.segment_sum(band_values.reshape(-1), band_ids.reshape(-1), num_segments=fields)

    def field_sums(values):
        return jax.vmap(segment_one)(values, field_ids)

    denominators = field_sums(weights) + PRIOR_WEIGHT
    mixing = jnp.eye(band_count, dtype=jnp.float32) + color_terms - jnp.diag(jnp.sum(color_terms, axis=1))

    def predict(zero_pts):
        zp_obs = jax.vmap(jnp.take)(zero_pts, field_ids)
        star_means = jnp.sum(weights * (magnitudes - zp_obs), axis=1) / star_weight
        predicted = jnp.dot(mixing, star_means, precision=lax.Precision.HIGHEST)
        return zp_obs, star_means, predicted

    zero_pts = jnp.zeros((band_count, fields), jnp.float32)
    misfits = []
    for sweep_no in range(SWEEPS):
        for color_no in range(COLORS):
            zp_obs, star_means, predicted = predict(zero_pts)
            residual = magnitudes - predicted[:, None, :]
            if color_no == 0 and sweep_no > 0:
                misfits.append(jnp.sum(weights * (residual - zp_obs) ** 2, axis=(1, 2)))
            updated = field_sums(weights * residual) / denominators
            zero_pts = jnp.where((colors == color_no)[None, :], updated, zero_pts)
    zp_obs, star_means, predicted = predict(zero_pts)
    residual = magnitudes - predicted[:, None, :]
    misfits.append(jnp.sum(weights * (residual - zp_obs) ** 2, axis=(1, 2)))
    misfit = jnp.stack(misfits) / (obs_count * star_count)
    owner_order = jnp.argsort(owner, stable=True)
    return jnp.take(zero_pts, owner_order, axis=1), star_means, misfit
```

```python
import functools

import jax
import jax.numpy as jnp
from jax import lax
from jax.experimental import pallas as pl
from jax.experimental.pallas import tpu as pltpu
from jax.sharding import PartitionSpec as P

COLORS = 8
SWEEPS = 4
PRIOR_WEIGHT = 1.0

TILES = 64
BANDS = 4
OBS = 8
BLOCKS = 8
ROWS = 256
STARS = BLOCKS * ROWS
LIST = 32
OWN = 64
NEAR = 3 * OWN
WIDE = BANDS * NEAR
STEPS = COLORS * SWEEPS
MESH = pl.DeviceIdType.MESH
HIGH = lax.Precision.HIGHEST
F32 = jnp.float32
BF16 = jnp.bfloat16
A_MEAN, A_P, A_BF, A_NF, A_COL, A_END = 0, 256, 384, 512, 640, 768


def home_of(tile):
    half = tile // 32
    row = tile // 8
    y = row % 4
    z = tile % 8
    leg = z // 4
    y_new = y + half * (3 - 2 * y)
    z_new = z + leg * (7 - 2 * z)
    x_lo = (1 - half + row + leg) % 2
    return half * 32 + y_new * 8 + z_new, x_lo * 2 + 1


def tile_at(sky, band):
    half = sky // 32
    y_new = (sky // 8) % 4
    z_new = sky % 8
    y = y_new + half * (3 - 2 * y_new)
    row = half * 4 + y
    leg = (band // 2 + 1 + half + row) % 2
    z = z_new + leg * (7 - 2 * z_new)
    is_home = (band % 2 == 1) & (z_new < 4)
    return is_home, (row * 8 + z) % TILES


def iota(shape, dim):
    return lax.broadcasted_iota(jnp.int32, shape, dim)


def as_column(row, count):
    eye = iota((count, 128), 0) == iota((count, 128), 1)
    full = jnp.broadcast_to(row, (count, 128))
    return jnp.sum(jnp.where(eye, full, 0.0), axis=1, keepdims=True)


def ship_kernel(w_ref, s_ref, a_ref, bw_ref, bs_ref, ba_ref, send, recv, local):
    sky = lax.axis_index("sky")
    band = lax.axis_index("band")
    home_sky, home_band = home_of(sky)
    stays = (home_sky == sky) & (home_band == band)
    is_home, my_tile = tile_at(sky, band)
    pairs = ((w_ref, bw_ref), (s_ref, bs_ref), (a_ref, ba_ref))

    def remote(i, slot):
        src, dst = pairs[i]
        return pltpu.make_async_remote_copy(
            src_ref=src,
            dst_ref=dst.at[slot],
            send_sem=send.at[i],
            recv_sem=recv.at[slot, i],
            device_id=(home_sky, home_band),
            device_id_type=MESH,
        )

    @pl.when(jnp.logical_not(stays))
    def _():
        for i in range(3):
            remote(i, band).start()

    @pl.when(stays)
    def _():
        for i in range(3):
            pltpu.make_async_copy(pairs[i][0], pairs[i][1].at[band], local.at[i]).start()
        for i in range(3):
            pltpu.make_async_copy(pairs[i][0], pairs[i][1].at[band], local.at[i]).wait()

    @pl.when(jnp.logical_not(stays))
    def _():
        for i in range(3):
            remote(i, band).wait_send()

    for slot in range(BANDS):
        own = (my_tile == sky) & (band == slot)

        @pl.when(is_home & jnp.logical_not(own))
        def _():
            for i in range(3):
                remote(i, slot).wait_recv()


def ship(w, s, a):
    vmem = pl.BlockSpec(memory_space=pltpu.VMEM)
    return pl.pallas_call(
        ship_kernel,
        out_shape=(
            jax.ShapeDtypeStruct((BANDS, OBS, STARS), F32),
            jax.ShapeDtypeStruct((BANDS, OBS, STARS), jnp.int32),
            jax.ShapeDtypeStruct((BANDS, BLOCKS, A_END), F32),
        ),
        in_specs=[vmem] * 3,
        out_specs=(vmem,) * 3,
        scratch_shapes=[
            pltpu.SemaphoreType.DMA((3,)),
            pltpu.SemaphoreType.DMA((BANDS, 3)),
            pltpu.SemaphoreType.DMA((3,)),
        ],
        compiler_params=pltpu.CompilerParams(has_side_effects=True),
        name="ship",
    )(w, s, a)


def block_maps(a_ref, blk):
    col = as_column(a_ref[0, blk : blk + 1, A_BF : A_BF + 128], 128)
    row_band = iota((128, 128), 0) // LIST
    lane_band = iota((128, 128), 1) // OWN
    parts = []
    for q in range(6):
        near = a_ref[0, q : q + 1, A_NF : A_NF + 128]
        hit = (col == near) & (row_band == lane_band + 2 * (q % 2))
        parts.append(jnp.where(hit, 1.0, 0.0))
    return parts


def split3(x):
    hi = x.astype(BF16)
    rest = x - hi.astype(F32)
    mid = rest.astype(BF16)
    low = (rest - mid.astype(F32)).astype(BF16)
    return hi, mid, low


def build_kernel(mix_ref, w_ref, s_ref, a_ref, mt_ref, td_ref, u_ref, r_ref):
    row_band = iota((128, 128), 0) // LIST
    lane_band = iota((128, 128), 1) // LIST
    mix = jnp.zeros((128, 128), F32)
    for b2 in range(BANDS):
        for b in range(BANDS):
            mix = jnp.where((row_band == b2) & (lane_band == b), mix_ref[b, b2], mix)
    lane_row = iota((1, 128), 1) // LIST
    entries = iota((LIST, ROWS), 0)
    td_acc = [jnp.zeros((8, 128), F32) for _ in range(6)]
    for blk in range(BLOCKS):
        cols = slice(blk * ROWS, (blk + 1) * ROWS)
        wide, scaled, mean0 = [], [], []
        for b in range(BANDS):
            acc = jnp.zeros((LIST, ROWS), F32)
            star_w = jnp.zeros((1, ROWS), F32)
            for k in range(OBS):
                wk = w_ref[b, k : k + 1, cols]
                acc = acc + jnp.where(s_ref[b, k : k + 1, cols] == entries, wk, 0.0)
                star_w = star_w + wk
            wide.append(acc)
            scaled.append(acc / star_w)
            mean0.append(a_ref[b, blk : blk + 1, A_MEAN : A_MEAN + ROWS])
        pred0 = []
        for b in range(BANDS):
            total = mix_ref[b, 0] * mean0[0]
            for b2 in range(1, BANDS):
                total = total + mix_ref[b, b2] * mean0[b2]
            pred0.append(total)
        w_all = jnp.concatenate(wide, axis=0)
        u_all = jnp.concatenate(scaled, axis=0)
        u_ref[blk] = u_all
        extra = jnp.concatenate(
            pred0 + [jnp.ones((1, ROWS), F32), jnp.zeros((3, ROWS), F32)], axis=0
        )
        dims = (((1,), (1,)), ((), ()))
        gt = lax.dot_general(u_all, w_all, dims, precision=HIGH, preferred_element_type=F32)
        ex = lax.dot_general(extra, w_all, dims, precision=HIGH, preferred_element_type=F32)
        gt = gt * mix
        known = jnp.zeros((1, 128), F32)
        for b in range(BANDS):
            known = known + a_ref[b, blk : blk + 1, A_P : A_P + 128]
            known = known - jnp.where(lane_row == b, ex[b : b + 1, :], 0.0)
        dens = ex[BANDS : BANDS + 1, :]
        maps = [m.astype(BF16) for m in block_maps(a_ref, blk)]
        td = jnp.concatenate([*split3(known), *split3(dens), jnp.zeros((2, 128), BF16)], axis=0)
        parts = split3(gt)
        for q in range(6):
            td_acc[q] = td_acc[q] + jnp.dot(td, maps[q], preferred_element_type=F32)
            for i in range(3):
                moved = jnp.dot(parts[i], maps[q], preferred_element_type=F32).astype(BF16)
                for b2 in range(BANDS):
                    r_ref[i, b2, blk * LIST : (blk + 1) * LIST, q * 128 : (q + 1) * 128] = moved[
                        b2 * LIST : (b2 + 1) * LIST, :
                    ]
    for q in range(6):
        acc = td_acc[q]
        td_ref[0, q : q + 1, :] = acc[0:1] + acc[1:2] + acc[2:3]
        td_ref[1, q : q + 1, :] = acc[3:4] + acc[4:5] + acc[5:6]
    td_ref[:, 6:8, :] = jnp.zeros((2, 2, 128), F32)
    list_row = [a_ref[0, 6 + h : 7 + h, A_NF : A_NF + 128] for h in range(2)]
    pick = []
    for tr in range(3):
        col = as_column(a_ref[0, 2 * tr : 2 * tr + 1, A_NF : A_NF + 128], OWN)
        pick.append(
            jnp.concatenate([jnp.where(col == row, 1.0, 0.0) for row in list_row], axis=1)
        )
    pick = jnp.concatenate(pick, axis=0).astype(BF16)
    for b2 in range(BANDS):
        total = jnp.dot(pick, r_ref[0, b2], preferred_element_type=F32)
        total = total + jnp.dot(pick, r_ref[1, b2], preferred_element_type=F32)
        total = total + jnp.dot(pick, r_ref[2, b2], preferred_element_type=F32)
        mt_ref[b2 * NEAR : (b2 + 1) * NEAR, :] = total


def build(mixing, bw, bs, ba):
    vmem = pl.BlockSpec(memory_space=pltpu.VMEM)
    return pl.pallas_call(
        build_kernel,
        out_shape=(
            jax.ShapeDtypeStruct((WIDE, WIDE), F32),
            jax.ShapeDtypeStruct((2, 8, 128), F32),
            jax.ShapeDtypeStruct((BLOCKS, 128, ROWS), F32),
        ),
        in_specs=[pl.BlockSpec(memory_space=pltpu.SMEM), vmem, vmem, vmem],
        out_specs=(vmem,) * 3,
        scratch_shapes=[pltpu.VMEM((3, BANDS, BLOCKS * LIST, WIDE), BF16)],
        name="build",
    )(mixing, bw, bs, ba)


def sweep_kernel(
    mt_ref, td_ref, a_ref, zs_ref, first_out, first_in, out_buf, in_buf,
    first_send, first_recv, send, recv,
):
    sky = lax.axis_index("sky")
    band = lax.axis_index("band")
    is_home, tile = tile_at(sky, band)
    places = [home_of((tile + d + TILES) % TILES) for d in (1, -1, 2, -2)]

    def first_copy(slot, i):
        return pltpu.make_async_remote_copy(
            src_ref=first_out.at[i],
            dst_ref=first_in.at[i, slot],
            send_sem=first_send.at[i, slot],
            recv_sem=first_recv.at[i, slot],
            device_id=places[slot],
            device_id_type=MESH,
        )

    def step_copy(slot, p):
        return pltpu.make_async_remote_copy(
            src_ref=out_buf.at[p],
            dst_ref=in_buf.at[p, slot],
            send_sem=send.at[p, slot],
            recv_sem=recv.at[p, slot],
            device_id=places[slot],
            device_id_type=MESH,
        )

    def combine(own, got):
        below, above, far_below, far_above = range(4)
        low = [own[q] + got(below, q + 2) + got(far_below, q + 4) for q in (0, 1)]
        mid = [own[q] + got(below, q + 2) + got(above, q - 2) for q in (2, 3)]
        top = [own[q] + got(above, q - 2) + got(far_above, q - 4) for q in (4, 5)]
        return low + mid + top

    eye = iota((128, 128), 0) == iota((128, 128), 1)

    def apply_operator(z):
        acc = jnp.zeros((8, WIDE), F32)
        for r in range(6):
            full = jnp.where(eye, jnp.broadcast_to(z[r], (128, 128)), 0.0)
            col = jnp.sum(full, axis=1, keepdims=True)
            for half in range(2):
                b = (r % 2) * 2 + half
                base = b * NEAR + (r // 2) * OWN
                for i in range(0, OWN, 8):
                    at = half * OWN + i
                    acc = acc + mt_ref[base + i : base + i + 8, :] * col[at : at + 8, :]
        flat = jnp.sum(acc, axis=0, keepdims=True)
        return [flat[:, q * 128 : (q + 1) * 128] for q in range(6)]

    @pl.when(is_home)
    def _():
        for i in range(2):
            for q in range(6):
                first_out[i, q] = td_ref[i, q : q + 1, :]
        for i in range(2):
            for slot in range(4):
                first_copy(slot, i).start()
        for i in range(2):
            for slot in range(4):
                first_copy(slot, i).wait()
        known = combine([first_out[0, q] for q in range(6)], lambda s, q: first_in[0, s, q])
        dens = combine([first_out[1, q] for q in range(6)], lambda s, q: first_in[1, s, q])
        dens = [d + PRIOR_WEIGHT for d in dens]
        colors = [a_ref[0, q : q + 1, A_COL : A_COL + 128] for q in range(6)]
        zero = jnp.zeros((1, 128), F32)
        z0 = tuple(jnp.where(colors[q] == 0.0, known[q] / dens[q], zero) for q in range(6))

        def step(s, z):
            p = s % 2
            color = s % COLORS
            own = apply_operator(z)
            for q in range(6):
                out_buf[p, q] = own[q]
            for slot in range(4):
                step_copy(slot, p).start()
            for slot in range(4):
                step_copy(slot, p).wait()
            pulled = combine(own, lambda i, q: in_buf[p, i, q])
            z = tuple(
                jnp.where(
                    colors[q] == color.astype(F32), (known[q] + pulled[q]) / dens[q], z[q]
                )
                for q in range(6)
            )

            @pl.when(color == COLORS - 1)
            def _():
                for q in range(6):
                    zs_ref[s // COLORS, q] = z[q]

            return z

        lax.fori_loop(1, STEPS, step, z0)


def sweeps(mt, td, ba):
    vmem = pl.BlockSpec(memory_space=pltpu.VMEM)
    return pl.pallas_call(
        sweep_kernel,
        out_shape=jax.ShapeDtypeStruct((SWEEPS, 6, 1, 128), F32),
        in_specs=[vmem] * 3,
        out_specs=vmem,
        scratch_shapes=[
            pltpu.VMEM((2, 6, 1, 128), F32),
            pltpu.VMEM((2, 4, 6, 1, 128), F32),
            pltpu.VMEM((2, 6, 1, 128), F32),
            pltpu.VMEM((2, 4, 6, 1, 128), F32),
            pltpu.SemaphoreType.DMA((2, 4)),
            pltpu.SemaphoreType.DMA((2, 4)),
            pltpu.SemaphoreType.DMA((2, 4)),
            pltpu.SemaphoreType.DMA((2, 4)),
        ],
        compiler_params=pltpu.CompilerParams(has_side_effects=True),
        name="sweeps",
    )(mt, td, ba)


def finish_kernel(mix_ref, zs_ref, a_ref, u_ref, fin_ref):
    lane_band = iota((1, 128), 1) // LIST
    rows_mix, rows_one = [], []
    for b in range(BANDS):
        row = jnp.zeros((1, 128), F32)
        for b2 in range(BANDS):
            row = jnp.where(lane_band == b2, mix_ref[b, b2], row)
        rows_mix.append(row)
        rows_one.append(jnp.where(lane_band == b, 1.0, 0.0))
    snap = [
        jnp.concatenate([zs_ref[n, q] for n in range(SWEEPS)] + [jnp.zeros((4, 128), F32)], axis=0)
        for q in range(6)
    ]
    for blk in range(BLOCKS):
        cols = slice(blk * ROWS, (blk + 1) * ROWS)
        maps = block_maps(a_ref, blk)
        listed = jnp.zeros((8, 128), F32)
        for q in range(6):
            listed = listed + lax.dot_general(
                snap[q], maps[q], (((1,), (1,)), ((), ())), precision=HIGH,
                preferred_element_type=F32,
            )
        lhs = [listed[n : n + 1] * rows_mix[b] for n in range(SWEEPS) for b in range(BANDS)]
        lhs += [listed[SWEEPS - 1 : SWEEPS] * rows_one[b] for b in range(BANDS)]
        lhs.append(jnp.zeros((4, 128), F32))
        moved = jnp.dot(
            jnp.concatenate(lhs, axis=0), u_ref[blk], precision=HIGH, preferred_element_type=F32
        )
        mean0 = [a_ref[b, blk : blk + 1, A_MEAN : A_MEAN + ROWS] for b in range(BANDS)]
        for b in range(BANDS):
            pred0 = mix_ref[b, 0] * mean0[0]
            for b2 in range(1, BANDS):
                pred0 = pred0 + mix_ref[b, b2] * mean0[b2]
            for n in range(SWEEPS):
                at = n * BANDS + b
                fin_ref[b, n : n + 1, cols] = pred0 - moved[at : at + 1]
                to = ((n % 2) * BLOCKS + blk) * 128
                fin_ref[b, 5 + n // 2 : 6 + n // 2, to : to + 128] = listed[n : n + 1]
            at = SWEEPS * BANDS + b
            fin_ref[b, 4:5, cols] = mean0[b] - moved[at : at + 1]
    for b in range(BANDS):
        fin_ref[b, 7:8, :] = jnp.zeros((1, STARS), F32)
        fin_ref[b, 7:8, 0:128] = zs_ref[SWEEPS - 1, 2 + b // 2]


def finish(mixing, zs, ba, u):
    vmem = pl.BlockSpec(memory_space=pltpu.VMEM)
    return pl.pallas_call(
        finish_kernel,
        out_shape=jax.ShapeDtypeStruct((BANDS, 8, STARS), F32),
        in_specs=[pl.BlockSpec(memory_space=pltpu.SMEM), vmem, vmem, vmem],
        out_specs=vmem,
        name="finish",
    )(mixing, zs, ba, u)


def give_kernel(
    fin_ref, m_ref, w_ref, s_ref, zp_ref, means_ref, mis_ref, got, parts,
    send, recv, local, part_send, part_recv,
):
    sky = lax.axis_index("sky")
    band = lax.axis_index("band")
    home_sky, home_band = home_of(sky)
    is_home, tile = tile_at(sky, band)
    stays = (home_sky == sky) & (home_band == band)

    def copy(slot):
        return pltpu.make_async_remote_copy(
            src_ref=fin_ref.at[slot],
            dst_ref=got,
            send_sem=send.at[slot],
            recv_sem=recv,
            device_id=(tile, slot),
            device_id_type=MESH,
        )

    for slot in range(BANDS):
        own = (tile == sky) & (band == slot)

        @pl.when(is_home & jnp.logical_not(own))
        def _():
            copy(slot).start()

    @pl.when(stays)
    def _():
        mine = pltpu.make_async_copy(fin_ref.at[band], got, local)
        mine.start()
        mine.wait()

    for slot in range(BANDS):
        own = (tile == sky) & (band == slot)

        @pl.when(is_home & jnp.logical_not(own))
        def _():
            copy(slot).wait_send()

    @pl.when(jnp.logical_not(stays))
    def _():
        copy(0).wait_recv()

    means_ref[...] = got[4:5, :]
    pair = got[7:8, 0:128]
    zp_ref[...] = jnp.where(band % 2 == 0, pair[:, 0:OWN], pair[:, OWN : 2 * OWN])
    acc = [jnp.zeros((8, 128), F32) for _ in range(SWEEPS)]
    for blk in range(BLOCKS):
        for half in range(2):
            at = blk * ROWS + half * 128
            m = m_ref[:, at : at + 128]
            w = w_ref[:, at : at + 128]
            idx = s_ref[:, at : at + 128] + band * LIST
            for n in range(SWEEPS):
                to = ((n % 2) * BLOCKS + blk) * 128
                table = jnp.broadcast_to(got[5 + n // 2 : 6 + n // 2, to : to + 128], (8, 128))
                picked = jnp.take_along_axis(table, idx, axis=1)
                left = m - got[n : n + 1, at : at + 128] - picked
                acc[n] = acc[n] + w * left * left
    lane = iota((1, 128), 1)
    row = jnp.zeros((1, 128), F32)
    for n in range(SWEEPS):
        total = jnp.sum(jnp.sum(acc[n], axis=0, keepdims=True), axis=1, keepdims=True)
        row = jnp.where(lane == n, total, row)
    parts[0] = row

    def part(d):
        return pltpu.make_async_remote_copy(
            src_ref=parts.at[0],
            dst_ref=parts.at[d],
            send_sem=part_send,
            recv_sem=part_recv,
            device_id=((sky + TILES - d) % TILES, band),
            device_id_type=MESH,
        )

    def push(d, carry):
        part(d).start()
        return carry

    lax.fori_loop(1, TILES, push, 0)
    everyone = pltpu.make_async_remote_copy(
        src_ref=parts.at[pl.ds(1, TILES - 1)],
        dst_ref=parts.at[pl.ds(1, TILES - 1)],
        send_sem=part_send,
        recv_sem=part_recv,
        device_id=((sky + 1) % TILES, band),
        device_id_type=MESH,
    )
    everyone.wait()
    by_tile = pltpu.roll(parts[...].reshape(TILES, 128), sky, 0)
    mis_ref[...] = jnp.sum(by_tile, axis=0, keepdims=True)


def give_back(fin, m, w, s):
    vmem = pl.BlockSpec(memory_space=pltpu.VMEM)
    return pl.pallas_call(
        give_kernel,
        out_shape=(
            jax.ShapeDtypeStruct((1, OWN), F32),
            jax.ShapeDtypeStruct((1, STARS), F32),
            jax.ShapeDtypeStruct((1, 128), F32),
        ),
        in_specs=[vmem] * 4,
        out_specs=(vmem,) * 3,
        scratch_shapes=[
            pltpu.VMEM((8, STARS), F32),
            pltpu.VMEM((TILES, 1, 128), F32),
            pltpu.SemaphoreType.DMA((BANDS,)),
            pltpu.SemaphoreType.DMA,
            pltpu.SemaphoreType.DMA,
            pltpu.SemaphoreType.DMA,
            pltpu.SemaphoreType.DMA,
        ],
        compiler_params=pltpu.CompilerParams(has_side_effects=True),
        name="give_back",
    )(fin, m, w, s)


def body(magnitudes, weights, slots, block_fields, owner, colors, color_terms):
    my_tile = lax.axis_index("sky")
    my_band = lax.axis_index("band")
    m, w, s = magnitudes[0], weights[0], slots[0]
    fields = owner.shape[0]
    mixing = (
        jnp.eye(BANDS, dtype=F32) + color_terms - jnp.diag(jnp.sum(color_terms, axis=1))
    )
    mean0 = (jnp.sum(w * m, axis=0) / jnp.sum(w, axis=0)).reshape(BLOCKS, ROWS)
    grid = (w * m).reshape(OBS, BLOCKS, 1, ROWS)
    hits = s.reshape(OBS, BLOCKS, 1, ROWS) == jnp.arange(LIST, dtype=jnp.int32)[None, None, :, None]
    sums = jnp.sum(jnp.where(hits, grid, 0.0), axis=(0, 3))
    lane_band = jnp.arange(128, dtype=jnp.int32) // LIST
    sums = jnp.where(lane_band[None] == my_band, jnp.tile(sums, (1, BANDS)), 0.0)
    listed = block_fields.astype(F32)
    order = jnp.sort(owner * fields + jnp.arange(fields, dtype=jnp.int32)) % fields
    nearby = jnp.mod(my_tile + jnp.arange(3, dtype=jnp.int32) - 1, TILES)
    near = jnp.take(order.reshape(TILES, OWN), nearby, axis=0)
    near_colors = jnp.take(colors, near)

    def per_band(values):
        return jnp.tile(values.astype(F32)[:, None, None, :], (1, 2, 2, 1)).reshape(6, 128)

    lists = jnp.concatenate([per_band(near), listed.reshape(2, 128)], axis=0)
    cols = jnp.concatenate([per_band(near_colors), jnp.zeros((2, 128), F32)], axis=0)
    table = jnp.concatenate([mean0, sums, jnp.tile(listed, (1, BANDS)), lists, cols], axis=1)
    bw, bs, ba = ship(w, s, table)
    mt, td, u = build(mixing, bw, bs, ba)
    zs = sweeps(mt, td, ba)
    fin = finish(mixing, zs, ba, u)
    zp, means, mis = give_back(fin, m, w, s)
    misfit = mis[:, :SWEEPS] / (OBS * STARS * TILES)
    return zp, means, misfit.reshape(SWEEPS, 1)


def solution(mesh):
    in_specs = (
        P("band", None, "sky"),
        P("band", None, "sky"),
        P("band", None, "sky"),
        P("sky", None),
        P(),
        P(),
        P(),
    )
    out_specs = (P("band", "sky"), P("band", "sky"), P(None, "band"))
    return jax.shard_map(body, mesh=mesh, in_specs=in_specs, out_specs=out_specs, check_vma=False)
```

```python
import functools

import jax
import jax.numpy as jnp
from jax import lax
from jax.experimental import pallas as pl
from jax.experimental.pallas import tpu as pltpu
from jax.sharding import PartitionSpec as P

COLORS = 8
SWEEPS = 4
PRIOR_WEIGHT = 1.0

TILES = 64
BANDS = 4
OBS = 8
BLOCKS = 8
ROWS = 256
STARS = BLOCKS * ROWS
LIST = 32
OWN = 64
NEAR = 3 * OWN
CHUNKS = 4
PER = BLOCKS // CHUNKS
SPAN = PER * ROWS
WIDE = BANDS * NEAR
STEPS = COLORS * SWEEPS
MESH = pl.DeviceIdType.MESH
HIGH = lax.Precision.HIGHEST
F32 = jnp.float32
BF16 = jnp.bfloat16


def home_of(tile):
    half = tile // 32
    row = tile // 8
    y = row % 4
    z = tile % 8
    leg = z // 4
    y_new = y + half * (3 - 2 * y)
    z_new = z + leg * (7 - 2 * z)
    x_lo = (1 - half + row + leg) % 2
    return half * 32 + y_new * 8 + z_new, x_lo * 2 + 1


def tile_at(sky, band):
    half = sky // 32
    y_new = (sky // 8) % 4
    z_new = sky % 8
    y = y_new + half * (3 - 2 * y_new)
    row = half * 4 + y
    leg = (band // 2 + 1 + half + row) % 2
    z = z_new + leg * (7 - 2 * z_new)
    is_home = (band % 2 == 1) & (z_new < 4)
    return is_home, (row * 8 + z) % TILES


def iota(shape, dim):
    return lax.broadcasted_iota(jnp.int32, shape, dim)


def as_column(row, count):
    eye = iota((count, 128), 0) == iota((count, 128), 1)
    full = jnp.broadcast_to(row, (count, 128))
    return jnp.sum(jnp.where(eye, full, 0.0), axis=1, keepdims=True)


def as_row(col, shift):
    n = col.shape[0]
    hit = iota((n, 128), 1) == iota((n, 128), 0) + shift
    return jnp.sum(jnp.where(hit, col, 0.0), axis=0, keepdims=True)


def split(x, terms):
    parts = []
    for _ in range(terms - 1):
        part = x.astype(BF16)
        parts.append(part)
        x = x - part.astype(F32)
    return parts + [x.astype(BF16)]


def tile_tables(tile, own_ref, col_ref, lst_ref, near_ref):
    rows = own_ref.shape[0]
    until = jnp.where(iota((128, 128), 0) <= iota((128, 128), 1), 1.0, 0.0).astype(BF16)
    before = jnp.where(iota((rows, rows), 1) < iota((rows, rows), 0), 1.0, 0.0).astype(BF16)
    number = (iota((rows, 128), 0) * 128 + iota((rows, 128), 1)).astype(F32)
    shade = col_ref[...].astype(F32)
    rank_at = iota((OWN, 128), 0).astype(F32)
    for tr in range(3):
        mine = own_ref[...] == (tile + tr - 1 + TILES) % TILES
        one = jnp.where(mine, 1.0, 0.0)
        inside = jnp.dot(one.astype(BF16), until, preferred_element_type=F32)
        above = jnp.dot(before, one.astype(BF16), preferred_element_type=F32)
        above = jnp.sum(above, axis=1, keepdims=True)
        rank = jnp.where(mine, inside + above - 1.0, -1.0)
        ids = jnp.zeros((OWN, 128), F32)
        cols = jnp.zeros((OWN, 128), F32)
        for i in range(rows):
            hit = rank[i : i + 1] == rank_at
            ids = ids + jnp.where(hit, number[i : i + 1], 0.0)
            cols = cols + jnp.where(hit, shade[i : i + 1], 0.0)
        for value, at in ((ids, 0), (cols, 128)):
            col = jnp.sum(value, axis=1, keepdims=True)
            row = as_row(col, 0) + as_row(col, OWN)
            near_ref[2 * tr : 2 * tr + 1, at : at + 128] = row
            near_ref[2 * tr + 1 : 2 * tr + 2, at : at + 128] = row
    near_ref[6:8, 128:256] = jnp.zeros((2, 128), F32)
    near_ref[6:8, 0:128] = lst_ref[0:2, 0:128].astype(F32)
    near_ref[:, 256:384] = lst_ref[2:10, 0:128].astype(F32)


def star_tables(m_ref, w_ref, s_ref, aux_ref):
    entries = iota((LIST, ROWS), 0)
    sums = [jnp.zeros((1, 128), F32) for _ in range(2)]
    for blk in range(BLOCKS):
        cols = slice(blk * ROWS, (blk + 1) * ROWS)
        acc = jnp.zeros((LIST, ROWS), F32)
        for k in range(OBS):
            value = w_ref[k : k + 1, cols] * m_ref[k : k + 1, cols]
            acc = acc + jnp.where(s_ref[k : k + 1, cols] == entries, value, 0.0)
        top = jnp.sum(w_ref[:, cols] * m_ref[:, cols], axis=0, keepdims=True)
        aux_ref[blk : blk + 1, 0:ROWS] = top / jnp.sum(w_ref[:, cols], axis=0, keepdims=True)
        col = jnp.sum(acc, axis=1, keepdims=True)
        sums[blk // 4] = sums[blk // 4] + as_row(col, (blk % 4) * LIST)
    aux_ref[2:8, 256:384] = jnp.zeros((6, 128), F32)
    for h in range(2):
        aux_ref[h : h + 1, 256:384] = sums[h]


def solve_kernel(
    ct_ref, m_ref, w_ref, s_ref, own_ref, col_ref, lst_ref,
    out_ref, means_ref,
    aux, near, bw, bs, ba, bn, u_ref, r_ref, mt_ref, pick2_ref,
    first_out, first_in, out_buf, in_buf, fin, fin_means, got, got_means, parts,
    ship_send, ship_recv, tab_send, tab_recv, local,
    first_send, first_recv, send, recv,
    fin_send, fin_recv, mean_send, mean_recv, part_send, part_recv,
):
    sky = lax.axis_index("sky")
    band = lax.axis_index("band")
    home_sky, home_band = home_of(sky)
    stays = (home_sky == sky) & (home_band == band)
    moves = jnp.logical_not(stays)
    is_home, tile = tile_at(sky, band)
    places = [home_of((tile + d + TILES) % TILES) for d in (1, -1, 2, -2)]

    def owns(slot):
        return (tile == sky) & (band == slot)

    barrier = pltpu.get_barrier_semaphore()

    @pl.when(moves)
    def _():
        pl.semaphore_signal(barrier, inc=1, device_id=(home_sky, home_band), device_id_type=MESH)

    @pl.when(is_home)
    def _():
        for place in places:
            pl.semaphore_signal(barrier, inc=1, device_id=place, device_id_type=MESH)
        for slot in range(BANDS):

            @pl.when(jnp.logical_not(owns(slot)))
            def _():
                pl.semaphore_signal(barrier, inc=1, device_id=(tile, slot), device_id_type=MESH)

    star_tables(m_ref, w_ref, s_ref, aux)
    tile_tables(sky, own_ref, col_ref, lst_ref, near)

    @pl.when(is_home & moves)
    def _():
        pl.semaphore_wait(barrier, 9)

    @pl.when(is_home & stays)
    def _():
        pl.semaphore_wait(barrier, 7)

    @pl.when(jnp.logical_not(is_home))
    def _():
        pl.semaphore_wait(barrier, 1)

    def chunk(ref, slot, c):
        at = pl.ds(c * SPAN, SPAN)
        return ref.at[:, at] if slot is None else ref.at[slot, :, at]

    def ship_copy(i, slot, c):
        src, dst = ((w_ref, bw), (s_ref, bs))[i]
        return pltpu.make_async_remote_copy(
            src_ref=chunk(src, None, c),
            dst_ref=chunk(dst, slot, c),
            send_sem=ship_send.at[i, c],
            recv_sem=ship_recv.at[slot, i, c],
            device_id=(home_sky, home_band),
            device_id_type=MESH,
        )

    def table_copy(i, slot):
        src, dst = ((aux, ba.at[slot]), (near, bn))[i]
        return pltpu.make_async_remote_copy(
            src_ref=src,
            dst_ref=dst,
            send_sem=tab_send.at[i],
            recv_sem=tab_recv.at[slot, i],
            device_id=(home_sky, home_band),
            device_id_type=MESH,
        )

    teller = 0

    @pl.when(moves)
    def _():
        @pl.when(band == teller)
        def _():
            table_copy(1, band).start()

        table_copy(0, band).start()
        for c in range(CHUNKS):
            for i in range(2):
                ship_copy(i, band, c).start()

    @pl.when(stays)
    def _():
        copies = [
            pltpu.make_async_copy(aux, ba.at[band], local.at[0]),
            pltpu.make_async_copy(w_ref, bw.at[band], local.at[1]),
            pltpu.make_async_copy(s_ref, bs.at[band], local.at[2]),
        ]
        for copy in copies:
            copy.start()
        for copy in copies:
            copy.wait()

    mix = []
    for b in range(BANDS):
        total = ct_ref[b, 0]
        for b2 in range(1, BANDS):
            total = total + ct_ref[b, b2]
        mix.append([ct_ref[b, b2] + (1.0 - total if b == b2 else 0.0) for b2 in range(BANDS)])

    def await_tables():
        table_copy(1, teller).wait_recv()
        for slot in range(BANDS):

            @pl.when(jnp.logical_not(owns(slot)))
            def _():
                table_copy(0, slot).wait_recv()

    def await_chunk(c):
        for slot in range(BANDS):

            @pl.when(jnp.logical_not(owns(slot)))
            def _():
                for i in range(2):
                    ship_copy(i, slot, c).wait_recv()

    def build():
        row_band = iota((128, 128), 0) // LIST
        lane_list = iota((128, 128), 1) // LIST
        lane_own = iota((128, 128), 1) // OWN
        mixes = jnp.zeros((128, 128), F32)
        for b2 in range(BANDS):
            for b in range(BANDS):
                mixes = jnp.where((row_band == b2) & (lane_list == b), mix[b][b2], mixes)
        entries = iota((LIST, ROWS), 0)
        await_tables()
        known = [[ba[b, h : h + 1, 256:384] for h in range(2)] for b in range(BANDS)]
        dens = [[jnp.zeros((1, 128), F32) for _ in range(2)] for _ in range(BANDS)]
        for blk in range(BLOCKS):
            if blk % PER == 0:
                await_chunk(blk // PER)
            cols = slice(blk * ROWS, (blk + 1) * ROWS)
            wide, scaled = [], []
            mean0 = [ba[b, blk : blk + 1, 0:ROWS] for b in range(BANDS)]
            for b in range(BANDS):
                acc = jnp.zeros((LIST, ROWS), F32)
                for k in range(OBS):
                    wk = bw[b, k : k + 1, cols]
                    acc = acc + jnp.where(bs[b, k : k + 1, cols] == entries, wk, 0.0)
                star_w = jnp.sum(bw[b, :, cols], axis=0, keepdims=True)
                wide.append(acc)
                scaled.append(acc * (1.0 / star_w))
                u_ref[b, blk * LIST : (blk + 1) * LIST, :] = scaled[b]
                pred0 = mix[b][0] * mean0[0]
                for b2 in range(1, BANDS):
                    pred0 = pred0 + mix[b][b2] * mean0[b2]
                h, at = blk // 4, (blk % 4) * LIST
                pulled = jnp.sum(acc * pred0, axis=1, keepdims=True)
                known[b][h] = known[b][h] - as_row(pulled, at)
                dens[b][h] = dens[b][h] + as_row(jnp.sum(acc, axis=1, keepdims=True), at)
            w_hi, w_lo = split(jnp.concatenate(wide, axis=0), 2)
            u_hi, u_lo = split(jnp.concatenate(scaled, axis=0), 2)
            dims = (((1,), (1,)), ((), ()))
            both = lax.dot_general(
                jnp.concatenate([u_hi, u_lo], axis=0), w_hi, dims, preferred_element_type=F32
            )
            gt = both[0:128] + both[128:256]
            gt = gt + lax.dot_general(u_hi, w_lo, dims, preferred_element_type=F32)
            lhs = jnp.concatenate(split(gt * mixes, 2), axis=0)
            col = as_column(bn[blk : blk + 1, 256:384], 128)
            for q in range(6):
                hit = (col == bn[q : q + 1, 0:128]) & (row_band == lane_own + 2 * (q % 2))
                moved = jnp.dot(
                    lhs, jnp.where(hit, 1.0, 0.0).astype(BF16), preferred_element_type=F32
                ).astype(BF16)
                for i in range(2):
                    for b2 in range(BANDS):
                        at = i * 128 + b2 * LIST
                        r_ref[
                            i, b2, blk * LIST : (blk + 1) * LIST, q * 128 : (q + 1) * 128
                        ] = moved[at : at + LIST]
        pick = []
        for tr in range(3):
            col = as_column(bn[2 * tr : 2 * tr + 1, 0:128], OWN)
            one = jnp.concatenate(
                [jnp.where(col == bn[6 + h : 7 + h, 0:128], 1.0, 0.0) for h in range(2)], axis=1
            ).astype(BF16)
            none = jnp.zeros((OWN, 256), BF16)
            pick2_ref[tr, 0:OWN, 0:256] = one
            pick2_ref[tr, OWN:128, 0:256] = none
            pick2_ref[tr, 0:OWN, 256:512] = none
            pick2_ref[tr, OWN:128, 256:512] = one
            pick.append(one)
        pick = jnp.concatenate(pick, axis=0)
        rows = [jnp.concatenate(known[b], axis=1) for b in range(BANDS)]
        rows += [jnp.concatenate(dens[b], axis=1) for b in range(BANDS)]
        terms = jnp.concatenate(split(jnp.concatenate(rows, axis=0), 3), axis=0)
        sums = lax.dot_general(terms, pick, (((1,), (1,)), ((), ())), preferred_element_type=F32)
        sums = sums[0:8] + sums[8:16] + sums[16:24]
        for i in range(2):
            for q in range(6):
                tr, b = q // 2, 2 * (q % 2)
                at = slice(tr * OWN, (tr + 1) * OWN)
                low, high = i * BANDS + b, i * BANDS + b + 1
                first_out[i, q] = jnp.concatenate(
                    [sums[low : low + 1, at], sums[high : high + 1, at]], axis=1
                )
        for i in range(2):
            for slot in range(4):
                first_copy(slot, i).start()
        for b2 in range(BANDS):
            total = jnp.dot(pick, r_ref[0, b2], preferred_element_type=F32)
            total = total + jnp.dot(pick, r_ref[1, b2], preferred_element_type=F32)
            mt_ref[b2 * NEAR : (b2 + 1) * NEAR, :] = total

    def first_copy(slot, i):
        return pltpu.make_async_remote_copy(
            src_ref=first_out.at[i],
            dst_ref=first_in.at[i, slot],
            send_sem=first_send.at[i, slot],
            recv_sem=first_recv.at[i, slot],
            device_id=places[slot],
            device_id_type=MESH,
        )

    part_of = (pl.ds(2, 4), pl.ds(0, 4), pl.ds(4, 2), pl.ds(0, 2))

    def step_copy(slot, p):
        return pltpu.make_async_remote_copy(
            src_ref=out_buf.at[p, part_of[slot]],
            dst_ref=in_buf.at[p, slot, part_of[slot]],
            send_sem=send.at[p, slot],
            recv_sem=recv.at[p, slot],
            device_id=places[slot],
            device_id_type=MESH,
        )

    below, above, far_below, far_above = range(4)

    def combine_mid(own, got):
        return [own[q] + got(below, q + 2) + got(above, q - 2) for q in (2, 3)]

    def combine_rest(own, got):
        low = [own[q] + got(below, q + 2) + got(far_below, q + 4) for q in (0, 1)]
        top = [own[q] + got(above, q - 2) + got(far_above, q - 4) for q in (4, 5)]
        return low, top

    def columns(row):
        eye = iota((128, 128), 0) == iota((128, 128), 1)
        full = jnp.where(eye, jnp.broadcast_to(row, (128, 128)), 0.0)
        return jnp.sum(full, axis=1, keepdims=True)

    def pull(accs, pieces, cols):
        for r, col in cols.items():
            for half in range(2):
                b = (r % 2) * 2 + half
                base = b * NEAR + (r // 2) * OWN
                for i in range(0, OWN, 8):
                    at = half * OWN + i
                    c = col[at : at + 8, :]
                    for j, q in enumerate(pieces):
                        accs[j] = accs[j] + mt_ref[base + i : base + i + 8, q * 128 : (q + 1) * 128] * c
        return accs

    outer, inner = (0, 1, 4, 5), (2, 3)

    def evaluate(n, z, last):
        zb = [[None, None] for _ in range(BANDS)]
        total = jnp.zeros((8, 512), F32)
        for tr in range(3):
            pair = jnp.concatenate([z[2 * tr], z[2 * tr + 1]], axis=0)
            lhs = jnp.concatenate(split(pair, 3) + [jnp.zeros((2, 128), BF16)], axis=0)
            total = total + jnp.dot(lhs, pick2_ref[tr], preferred_element_type=F32)
        total = total[0:2] + total[2:4] + total[4:6]
        means = []
        for b in range(BANDS):
            rows = []
            for h in range(2):
                at = (b % 2) * 256 + h * 128
                row = total[b // 2 : b // 2 + 1, at : at + 128]
                fin[n, b, h : h + 1, 256:384] = row
                col = columns(row)
                for i in range(4):
                    blk = h * 4 + i
                    value = u_ref[b, blk * LIST : (blk + 1) * LIST, :] * col[i * LIST : (i + 1) * LIST, :]
                    rows.append(jnp.sum(value, axis=0, keepdims=True))
            means.append(ba[b, :, 0:ROWS] - jnp.concatenate(rows, axis=0))
            fin[n, b, 2:3, 256:384] = z[2 + b // 2]
            fin[n, b, 3:8, 256:384] = jnp.zeros((5, 128), F32)
        for b in range(BANDS):
            pred = mix[b][0] * means[0]
            for b2 in range(1, BANDS):
                pred = pred + mix[b][b2] * means[b2]
            fin[n, b, :, 0:ROWS] = pred
            if last:
                fin_means[b] = means[b]
        for slot in range(BANDS):

            @pl.when(jnp.logical_not(owns(slot)))
            def _():
                fin_copy(n, slot).start()
                if last:
                    mean_copy(slot).start()

    def fin_copy(n, slot):
        return pltpu.make_async_remote_copy(
            src_ref=fin.at[n, slot],
            dst_ref=got.at[n],
            send_sem=fin_send.at[n, slot],
            recv_sem=fin_recv.at[n],
            device_id=(tile, slot),
            device_id_type=MESH,
        )

    def mean_copy(slot):
        return pltpu.make_async_remote_copy(
            src_ref=fin_means.at[slot],
            dst_ref=got_means,
            send_sem=mean_send.at[slot],
            recv_sem=mean_recv,
            device_id=(tile, slot),
            device_id_type=MESH,
        )

    @pl.when(is_home)
    def _():
        build()
        for i in range(2):
            for slot in range(4):
                first_copy(slot, i).wait()
        start = []
        for i in range(2):
            own = [first_out[i, q] for q in range(6)]
            low, top = combine_rest(own, lambda s, q: first_in[i, s, q])
            start.append(low + combine_mid(own, lambda s, q: first_in[i, s, q]) + top)
        known, dens = start
        scale = [1.0 / (d + PRIOR_WEIGHT) for d in dens]
        colors = [bn[q : q + 1, 128:256] for q in range(6)]
        zero = jnp.zeros((1, 128), F32)
        z = [jnp.where(colors[q] == 0.0, known[q] * scale[q], zero) for q in range(6)]
        cols = {q: columns(z[q]) for q in range(6)}
        accs = pull([jnp.zeros((8, 128), F32) for _ in range(6)], range(6), cols)
        for q in range(6):
            out_buf[1, q] = jnp.sum(accs[q], axis=0, keepdims=True)
        for slot in (2, 3, 0, 1):
            step_copy(slot, 1).start()

        def renew(q, color, pulled, old):
            return jnp.where(colors[q] == color, (known[q] + pulled) * scale[q], old)

        def absorb(s, z, then):
            p = s % 2
            color = (s % COLORS).astype(F32) if not isinstance(s, int) else float(s % COLORS)
            own = [out_buf[p, q] for q in range(6)]
            take = lambda i, q: in_buf[p, i, q]
            z = list(z)
            for slot in (0, 1):
                step_copy(slot, p).wait_recv()
            mid = combine_mid(own, take)
            for q in inner:
                z[q] = renew(q, color, mid[q - 2], z[q])
            accs = None
            if then:
                cols = {q: columns(z[q]) for q in inner}
                accs = pull([jnp.zeros((8, 128), F32) for _ in range(6)], range(6), cols)
            for slot in (2, 3):
                step_copy(slot, p).wait_recv()
            low, top = combine_rest(own, take)
            for j, q in enumerate(outer):
                z[q] = renew(q, color, (low + top)[j], z[q])
            return z, accs

        def step(s, z):
            p = s % 2

            @pl.when(s % COLORS == 0)
            def _():
                evaluate(s // COLORS - 1, z, False)

            z, accs = absorb(s, z, True)
            cols = {q: columns(z[q]) for q in outer}
            far = pull([accs[q] for q in outer], outer, cols)
            for j, q in enumerate(outer):
                out_buf[1 - p, q] = jnp.sum(far[j], axis=0, keepdims=True)
            for slot in (2, 3):
                step_copy(slot, 1 - p).start()
            near_accs = pull([accs[q] for q in inner], inner, cols)
            for j, q in enumerate(inner):
                out_buf[1 - p, q] = jnp.sum(near_accs[j], axis=0, keepdims=True)
            for slot in (0, 1):
                step_copy(slot, 1 - p).start()
            for slot in range(4):
                step_copy(slot, p).wait_send()
            return tuple(z)

        z = lax.fori_loop(1, STEPS - 1, step, tuple(z))
        z, _ = absorb(STEPS - 1, z, False)
        evaluate(SWEEPS - 1, z, True)
        for slot in range(4):
            step_copy(slot, (STEPS - 1) % 2).wait_send()

    @pl.when(moves)
    def _():
        @pl.when(band == teller)
        def _():
            table_copy(1, band).wait_send()

        table_copy(0, band).wait_send()
        for c in range(CHUNKS):
            for i in range(2):
                ship_copy(i, band, c).wait_send()

    def squares(n):
        @pl.when(moves)
        def _():
            fin_copy(n, 0).wait_recv()

        @pl.when(stays)
        def _():
            mine = pltpu.make_async_copy(fin.at[n, band], got.at[n], local.at[0])
            mine.start()
            mine.wait()

        acc = jnp.zeros((8, 128), F32)
        for blk in range(BLOCKS):
            for half in range(2):
                at = blk * ROWS + half * 128
                table = jnp.broadcast_to(got[n, blk // 4 : blk // 4 + 1, 256:384], (8, 128))
                idx = s_ref[:, at : at + 128] + (blk % 4) * LIST
                picked = jnp.take_along_axis(table, idx, axis=1)
                left = m_ref[:, at : at + 128] - got[n, blk : blk + 1, half * 128 : half * 128 + 128]
                left = left - picked
                acc = acc + w_ref[:, at : at + 128] * left * left
        total = jnp.sum(jnp.sum(acc, axis=0, keepdims=True), axis=1, keepdims=True)
        return jnp.where(iota((1, 128), 1) == n, total, 0.0)

    row = squares(0)
    for n in range(1, SWEEPS):
        row = row + squares(n)
    parts[0] = row

    def part(d):
        return pltpu.make_async_remote_copy(
            src_ref=parts.at[0],
            dst_ref=parts.at[d],
            send_sem=part_send,
            recv_sem=part_recv,
            device_id=((sky + TILES - d) % TILES, band),
            device_id_type=MESH,
        )

    def push(d, carry):
        part(d).start()
        return carry

    lax.fori_loop(1, TILES, push, 0)

    @pl.when(moves)
    def _():
        mean_copy(0).wait_recv()

    @pl.when(stays)
    def _():
        mine = pltpu.make_async_copy(fin_means.at[band], got_means, local.at[1])
        mine.start()
        mine.wait()

    means_ref[...] = got_means[...]
    pair = got[SWEEPS - 1, 2:3, 256:384]
    own_zp = jnp.where(band % 2 == 0, pair, pltpu.roll(pair, OWN, 1))
    out_ref[...] = jnp.zeros((8, 128), F32)
    out_ref[0:1, :] = own_zp

    @pl.when(is_home)
    def _():
        for slot in range(BANDS):

            @pl.when(jnp.logical_not(owns(slot)))
            def _():
                for n in range(SWEEPS):
                    fin_copy(n, slot).wait_send()
                mean_copy(slot).wait_send()

    everyone = pltpu.make_async_remote_copy(
        src_ref=parts.at[pl.ds(1, TILES - 1)],
        dst_ref=parts.at[pl.ds(1, TILES - 1)],
        send_sem=part_send,
        recv_sem=part_recv,
        device_id=((sky + 1) % TILES, band),
        device_id_type=MESH,
    )
    everyone.wait()
    by_tile = pltpu.roll(parts[...].reshape(TILES, 128), sky, 0)
    out_ref[1:2, :] = jnp.sum(by_tile, axis=0, keepdims=True) * (1.0 / (OBS * STARS * TILES))


def solve(color_terms, m, w, s, owner, colors, lists):
    vmem = pl.BlockSpec(memory_space=pltpu.VMEM)
    dma = pltpu.SemaphoreType.DMA
    return pl.pallas_call(
        solve_kernel,
        out_shape=(
            jax.ShapeDtypeStruct((8, 128), F32),
            jax.ShapeDtypeStruct((BLOCKS, ROWS), F32),
        ),
        in_specs=[pl.BlockSpec(memory_space=pltpu.SMEM)] + [vmem] * 6,
        out_specs=(vmem,) * 2,
        scratch_shapes=[
            pltpu.VMEM((8, 384), F32),
            pltpu.VMEM((8, 384), F32),
            pltpu.VMEM((BANDS, OBS, STARS), F32),
            pltpu.VMEM((BANDS, OBS, STARS), jnp.int32),
            pltpu.VMEM((BANDS, 8, 384), F32),
            pltpu.VMEM((8, 384), F32),
            pltpu.VMEM((BANDS, BLOCKS * LIST, ROWS), F32),
            pltpu.VMEM((2, BANDS, BLOCKS * LIST, WIDE), BF16),
            pltpu.VMEM((WIDE, WIDE), F32),
            pltpu.VMEM((3, 128, 512), BF16),
            pltpu.VMEM((2, 6, 1, 128), F32),
            pltpu.VMEM((2, 4, 6, 1, 128), F32),
            pltpu.VMEM((2, 6, 1, 128), F32),
            pltpu.VMEM((2, 4, 6, 1, 128), F32),
            pltpu.VMEM((SWEEPS, BANDS, 8, 384), F32),
            pltpu.VMEM((BANDS, BLOCKS, ROWS), F32),
            pltpu.VMEM((SWEEPS, 8, 384), F32),
            pltpu.VMEM((BLOCKS, ROWS), F32),
            pltpu.VMEM((TILES, 1, 128), F32),
            dma((2, CHUNKS)),
            dma((BANDS, 2, CHUNKS)),
            dma((2,)),
            dma((BANDS, 2)),
            dma((3,)),
            dma((2, 4)),
            dma((2, 4)),
            dma((2, 4)),
            dma((2, 4)),
            dma((SWEEPS, BANDS)),
            dma((SWEEPS,)),
            dma((BANDS,)),
            dma,
            dma,
            dma,
        ],
        compiler_params=pltpu.CompilerParams(has_side_effects=True, collective_id=0),
        name="solve",
    )(color_terms, m, w, s, owner, colors, lists)


def unpack_kernel(out_ref, means_ref, zp_ref, mags_ref, mis_ref):
    zp_ref[...] = out_ref[0:1, 0:OWN]
    mis_ref[...] = out_ref[1:2, :]
    for blk in range(BLOCKS):
        mags_ref[0:1, blk * ROWS : (blk + 1) * ROWS] = means_ref[blk : blk + 1, :]


def body(magnitudes, weights, slots, block_fields, owner, colors, color_terms):
    lists = jnp.concatenate(
        [block_fields.reshape(2, 128), jnp.tile(block_fields, (1, BANDS))], axis=0
    )
    out, means = solve(
        color_terms, magnitudes[0], weights[0], slots[0],
        owner.reshape(-1, 128), colors.reshape(-1, 128), lists,
    )
    vmem = pl.BlockSpec(memory_space=pltpu.VMEM)
    zp, mags, misfit = pl.pallas_call(
        unpack_kernel,
        out_shape=(
            jax.ShapeDtypeStruct((1, OWN), F32),
            jax.ShapeDtypeStruct((1, STARS), F32),
            jax.ShapeDtypeStruct((1, 128), F32),
        ),
        in_specs=[vmem] * 2,
        out_specs=(vmem,) * 3,
        name="unpack",
    )(out, means)
    return zp, mags, misfit[:, :SWEEPS].reshape(SWEEPS, 1)


def solution(mesh):
    in_specs = (
        P("band", None, "sky"),
        P("band", None, "sky"),
        P("band", None, "sky"),
        P("sky", None),
        P(),
        P(),
        P(),
    )
    out_specs = (P("band", "sky"), P("band", "sky"), P(None, "band"))
    return jax.shard_map(body, mesh=mesh, in_specs=in_specs, out_specs=out_specs, check_vma=False)
```

```python
import functools

import jax
import jax.numpy as jnp
from jax import lax
from jax.experimental import pallas as pl
from jax.experimental.pallas import tpu as pltpu
from jax.sharding import PartitionSpec as P

COLORS = 8
SWEEPS = 4
PRIOR_WEIGHT = 1.0

TILES = 64
BANDS = 4
OBS = 8
BLOCKS = 8
ROWS = 256
STARS = BLOCKS * ROWS
LIST = 32
OWN = 64
NEAR = 3 * OWN
CHUNKS = 4
PER = BLOCKS // CHUNKS
SPAN = PER * ROWS
WIDE = BANDS * NEAR
STEPS = COLORS * SWEEPS
PLANE = [(i, j) for i in (2, 1, 3, 0) for j in (2, 1, 3, 0)][:-1]
LINE = [(k, c) for k in (4, 3, 5, 2, 6, 1, 7, 0) for c in (0, 1)][:-1]
MESH = pl.DeviceIdType.MESH
HIGH = lax.Precision.HIGHEST
F32 = jnp.float32
BF16 = jnp.bfloat16


def home_of(tile):
    half = tile // 32
    row = tile // 8
    y = row % 4
    z = tile % 8
    leg = z // 4
    y_new = y + half * (3 - 2 * y)
    z_new = z + leg * (7 - 2 * z)
    x_lo = (1 - half + row + leg) % 2
    return half * 32 + y_new * 8 + z_new, x_lo * 2 + 1


def tile_at(sky, band):
    half = sky // 32
    y_new = (sky // 8) % 4
    z_new = sky % 8
    y = y_new + half * (3 - 2 * y_new)
    row = half * 4 + y
    leg = (band // 2 + 1 + half + row) % 2
    z = z_new + leg * (7 - 2 * z_new)
    is_home = (band % 2 == 1) & (z_new < 4)
    return is_home, (row * 8 + z) % TILES


def iota(shape, dim):
    return lax.broadcasted_iota(jnp.int32, shape, dim)


def as_column(row, count):
    eye = iota((count, 128), 0) == iota((count, 128), 1)
    full = jnp.broadcast_to(row, (count, 128))
    return jnp.sum(jnp.where(eye, full, 0.0), axis=1, keepdims=True)


def as_row(col, shift):
    n = col.shape[0]
    hit = iota((n, 128), 1) == iota((n, 128), 0) + shift
    return jnp.sum(jnp.where(hit, col, 0.0), axis=0, keepdims=True)


def split(x, terms):
    parts = []
    for _ in range(terms - 1):
        part = x.astype(BF16)
        parts.append(part)
        x = x - part.astype(F32)
    return parts + [x.astype(BF16)]


def tile_tables(tile, own_ref, col_ref, lst_ref, near_ref):
    rows = own_ref.shape[0]
    until = jnp.where(iota((128, 128), 0) <= iota((128, 128), 1), 1.0, 0.0).astype(BF16)
    before = jnp.where(iota((rows, rows), 1) < iota((rows, rows), 0), 1.0, 0.0).astype(BF16)
    number = (iota((rows, 128), 0) * 128 + iota((rows, 128), 1)).astype(F32)
    shade = col_ref[...].astype(F32)
    rank_at = iota((OWN, 128), 0).astype(F32)
    for tr in range(3):
        mine = own_ref[...] == (tile + tr - 1 + TILES) % TILES
        one = jnp.where(mine, 1.0, 0.0)
        inside = jnp.dot(one.astype(BF16), until, preferred_element_type=F32)
        above = jnp.dot(before, one.astype(BF16), preferred_element_type=F32)
        above = jnp.sum(above, axis=1, keepdims=True)
        rank = jnp.where(mine, inside + above - 1.0, -1.0)
        ids = jnp.zeros((OWN, 128), F32)
        cols = jnp.zeros((OWN, 128), F32)
        for i in range(rows):
            hit = rank[i : i + 1] == rank_at
            ids = ids + jnp.where(hit, number[i : i + 1], 0.0)
            cols = cols + jnp.where(hit, shade[i : i + 1], 0.0)
        for value, at in ((ids, 0), (cols, 128)):
            col = jnp.sum(value, axis=1, keepdims=True)
            row = as_row(col, 0) + as_row(col, OWN)
            near_ref[2 * tr : 2 * tr + 1, at : at + 128] = row
            near_ref[2 * tr + 1 : 2 * tr + 2, at : at + 128] = row
    near_ref[6:8, 128:256] = jnp.zeros((2, 128), F32)
    listed = lst_ref[...].astype(F32)
    near_ref[:, 256:384] = jnp.concatenate([listed] * BANDS, axis=1)
    for h in range(2):
        row = [listed[i : i + 1] for i in range(4 * h, 4 * h + 4)]
        near_ref[6 + h : 7 + h, 0:128] = jnp.concatenate(row, axis=1)


def star_tables(m_ref, w_ref, s_ref, aux_ref):
    entries = iota((LIST, ROWS), 0)
    sums = [jnp.zeros((1, 128), F32) for _ in range(2)]
    for blk in range(BLOCKS):
        cols = slice(blk * ROWS, (blk + 1) * ROWS)
        acc = jnp.zeros((LIST, ROWS), F32)
        for k in range(OBS):
            value = w_ref[k : k + 1, cols] * m_ref[k : k + 1, cols]
            acc = acc + jnp.where(s_ref[k : k + 1, cols] == entries, value, 0.0)
        top = jnp.sum(w_ref[:, cols] * m_ref[:, cols], axis=0, keepdims=True)
        aux_ref[blk : blk + 1, 0:ROWS] = top / jnp.sum(w_ref[:, cols], axis=0, keepdims=True)
        col = jnp.sum(acc, axis=1, keepdims=True)
        sums[blk // 4] = sums[blk // 4] + as_row(col, (blk % 4) * LIST)
    aux_ref[2:8, 256:384] = jnp.zeros((6, 128), F32)
    for h in range(2):
        aux_ref[h : h + 1, 256:384] = sums[h]


def solve_kernel(
    ct_ref, m_hbm, w_hbm, s_hbm, own_ref, col_ref, lst_ref,
    out_ref,
    m_ref, w_ref, s_ref,
    aux, near, bm, bw, bs, ba, bn, u_ref, r_ref, mt_ref, pick2_ref,
    first_out, first_in, out_buf, in_buf, fin, got, row_buf, plane, line,
    load_sem, ship_send, ship_recv, mag_send, mag_recv, tab_send, tab_recv, local,
    first_send, first_recv, send, recv,
    fin_send, fin_recv, plane_send, plane_recv, line_send, line_recv, go,
):
    sky = lax.axis_index("sky")
    band = lax.axis_index("band")
    home_sky, home_band = home_of(sky)
    stays = (home_sky == sky) & (home_band == band)
    moves = jnp.logical_not(stays)
    is_home, tile = tile_at(sky, band)
    places = [home_of((tile + d + TILES) % TILES) for d in (1, -1, 2, -2)]

    def owns(slot):
        return (tile == sky) & (band == slot)

    barrier = pltpu.get_barrier_semaphore()

    @pl.when(moves)
    def _():
        pl.semaphore_signal(barrier, inc=1, device_id=(home_sky, home_band), device_id_type=MESH)

    @pl.when(is_home)
    def _():
        for place in places:
            pl.semaphore_signal(barrier, inc=1, device_id=place, device_id_type=MESH)
        for slot in range(BANDS):

            @pl.when(jnp.logical_not(owns(slot)))
            def _():
                pl.semaphore_signal(barrier, inc=1, device_id=(tile, slot), device_id_type=MESH)

    loads = [
        pltpu.make_async_copy(src, dst, load_sem.at[i])
        for i, (src, dst) in enumerate(((m_hbm, m_ref), (w_hbm, w_ref), (s_hbm, s_ref)))
    ]
    for load in loads:
        load.start()
    tile_tables(sky, own_ref, col_ref, lst_ref, near)
    for load in loads:
        load.wait()
    star_tables(m_ref, w_ref, s_ref, aux)

    @pl.when(is_home & moves)
    def _():
        pl.semaphore_wait(barrier, 9)

    @pl.when(is_home & stays)
    def _():
        pl.semaphore_wait(barrier, 7)

    @pl.when(jnp.logical_not(is_home))
    def _():
        pl.semaphore_wait(barrier, 1)

    def chunk(ref, slot, c):
        at = pl.ds(c * SPAN, SPAN)
        return ref.at[:, at] if slot is None else ref.at[slot, :, at]

    def ship_copy(i, slot, c):
        src, dst = ((w_ref, bw), (s_ref, bs))[i]
        return pltpu.make_async_remote_copy(
            src_ref=chunk(src, None, c),
            dst_ref=chunk(dst, slot, c),
            send_sem=ship_send.at[i, c],
            recv_sem=ship_recv.at[slot, i, c],
            device_id=(home_sky, home_band),
            device_id_type=MESH,
        )

    def mag_copy(slot):
        return pltpu.make_async_remote_copy(
            src_ref=m_ref,
            dst_ref=bm.at[slot],
            send_sem=mag_send,
            recv_sem=mag_recv.at[slot],
            device_id=(home_sky, home_band),
            device_id_type=MESH,
        )

    def table_copy(i, slot):
        src, dst = ((aux, ba.at[slot]), (near, bn))[i]
        return pltpu.make_async_remote_copy(
            src_ref=src,
            dst_ref=dst,
            send_sem=tab_send.at[i],
            recv_sem=tab_recv.at[slot, i],
            device_id=(home_sky, home_band),
            device_id_type=MESH,
        )

    teller = 0

    @pl.when(moves)
    def _():
        @pl.when(band == teller)
        def _():
            table_copy(1, band).start()

        table_copy(0, band).start()
        for c in range(CHUNKS):
            for i in range(2):
                ship_copy(i, band, c).start()

    @pl.when(stays)
    def _():
        copies = [
            pltpu.make_async_copy(aux, ba.at[band], local.at[0]),
            pltpu.make_async_copy(w_ref, bw.at[band], local.at[1]),
            pltpu.make_async_copy(s_ref, bs.at[band], local.at[2]),
            pltpu.make_async_copy(m_ref, bm.at[band], local.at[3]),
        ]
        for copy in copies:
            copy.start()
        for copy in copies:
            copy.wait()

    mix = []
    for b in range(BANDS):
        total = ct_ref[b, 0]
        for b2 in range(1, BANDS):
            total = total + ct_ref[b, b2]
        mix.append([ct_ref[b, b2] + (1.0 - total if b == b2 else 0.0) for b2 in range(BANDS)])

    def await_tables():
        table_copy(1, teller).wait_recv()
        for slot in range(BANDS):

            @pl.when(jnp.logical_not(owns(slot)))
            def _():
                table_copy(0, slot).wait_recv()

    def await_chunk(c):
        for slot in range(BANDS):

            @pl.when(jnp.logical_not(owns(slot)))
            def _():
                for i in range(2):
                    ship_copy(i, slot, c).wait_recv()

    def build():
        row_band = iota((128, 128), 0) // LIST
        lane_list = iota((128, 128), 1) // LIST
        lane_own = iota((128, 128), 1) // OWN
        mixes = jnp.zeros((128, 128), F32)
        for b2 in range(BANDS):
            for b in range(BANDS):
                mixes = jnp.where((row_band == b2) & (lane_list == b), mix[b][b2], mixes)
        entries = iota((LIST, ROWS), 0)
        await_tables()
        known = [[ba[b, h : h + 1, 256:384] for h in range(2)] for b in range(BANDS)]
        dens = [[jnp.zeros((1, 128), F32) for _ in range(2)] for _ in range(BANDS)]
        for blk in range(BLOCKS):
            if blk % PER == 0:
                await_chunk(blk // PER)
            if blk == BLOCKS - PER:
                for slot in range(BANDS):

                    @pl.when(jnp.logical_not(owns(slot)))
                    def _():
                        pl.semaphore_signal(go, inc=1, device_id=(tile, slot), device_id_type=MESH)

            cols = slice(blk * ROWS, (blk + 1) * ROWS)
            wide, scaled = [], []
            mean0 = [ba[b, blk : blk + 1, 0:ROWS] for b in range(BANDS)]
            for b in range(BANDS):
                acc = jnp.zeros((LIST, ROWS), F32)
                for k in range(OBS):
                    wk = bw[b, k : k + 1, cols]
                    acc = acc + jnp.where(bs[b, k : k + 1, cols] == entries, wk, 0.0)
                star_w = jnp.sum(bw[b, :, cols], axis=0, keepdims=True)
                wide.append(acc)
                scaled.append(acc * (1.0 / star_w))
                u_ref[b, blk * LIST : (blk + 1) * LIST, :] = scaled[b]
                pred0 = mix[b][0] * mean0[0]
                for b2 in range(1, BANDS):
                    pred0 = pred0 + mix[b][b2] * mean0[b2]
                h, at = blk // 4, (blk % 4) * LIST
                pulled = jnp.sum(acc * pred0, axis=1, keepdims=True)
                known[b][h] = known[b][h] - as_row(pulled, at)
                dens[b][h] = dens[b][h] + as_row(jnp.sum(acc, axis=1, keepdims=True), at)
            w_hi, w_lo = split(jnp.concatenate(wide, axis=0), 2)
            u_hi, u_lo = split(jnp.concatenate(scaled, axis=0), 2)
            dims = (((1,), (1,)), ((), ()))
            both = lax.dot_general(
                jnp.concatenate([u_hi, u_lo], axis=0), w_hi, dims, preferred_element_type=F32
            )
            gt = both[0:128] + both[128:256]
            gt = gt + lax.dot_general(u_hi, w_lo, dims, preferred_element_type=F32)
            lhs = jnp.concatenate(split(gt * mixes, 2), axis=0)
            col = as_column(bn[blk : blk + 1, 256:384], 128)
            for q in range(6):
                hit = (col == bn[q : q + 1, 0:128]) & (row_band == lane_own + 2 * (q % 2))
                moved = jnp.dot(
                    lhs, jnp.where(hit, 1.0, 0.0).astype(BF16), preferred_element_type=F32
                ).astype(BF16)
                for i in range(2):
                    for b2 in range(BANDS):
                        at = i * 128 + b2 * LIST
                        r_ref[
                            i, b2, blk * LIST : (blk + 1) * LIST, q * 128 : (q + 1) * 128
                        ] = moved[at : at + LIST]
        pick = []
        for tr in range(3):
            col = as_column(bn[2 * tr : 2 * tr + 1, 0:128], OWN)
            one = jnp.concatenate(
                [jnp.where(col == bn[6 + h : 7 + h, 0:128], 1.0, 0.0) for h in range(2)], axis=1
            ).astype(BF16)
            none = jnp.zeros((OWN, 256), BF16)
            pick2_ref[tr, 0:OWN, 0:256] = one
            pick2_ref[tr, OWN:128, 0:256] = none
            pick2_ref[tr, 0:OWN, 256:512] = none
            pick2_ref[tr, OWN:128, 256:512] = one
            pick.append(one)
        pick = jnp.concatenate(pick, axis=0)
        rows = [jnp.concatenate(known[b], axis=1) for b in range(BANDS)]
        rows += [jnp.concatenate(dens[b], axis=1) for b in range(BANDS)]
        terms = jnp.concatenate(split(jnp.concatenate(rows, axis=0), 3), axis=0)
        sums = lax.dot_general(terms, pick, (((1,), (1,)), ((), ())), preferred_element_type=F32)
        sums = sums[0:8] + sums[8:16] + sums[16:24]
        for i in range(2):
            for q in range(6):
                tr, b = q // 2, 2 * (q % 2)
                at = slice(tr * OWN, (tr + 1) * OWN)
                low, high = i * BANDS + b, i * BANDS + b + 1
                first_out[i, q] = jnp.concatenate(
                    [sums[low : low + 1, at], sums[high : high + 1, at]], axis=1
                )
        for i in range(2):
            for slot in range(4):
                first_copy(slot, i).start()
        for b2 in range(BANDS):
            total = jnp.dot(pick, r_ref[0, b2], preferred_element_type=F32)
            total = total + jnp.dot(pick, r_ref[1, b2], preferred_element_type=F32)
            mt_ref[b2 * NEAR : (b2 + 1) * NEAR, :] = total

    def first_copy(slot, i):
        return pltpu.make_async_remote_copy(
            src_ref=first_out.at[i],
            dst_ref=first_in.at[i, slot],
            send_sem=first_send.at[i, slot],
            recv_sem=first_recv.at[i, slot],
            device_id=places[slot],
            device_id_type=MESH,
        )

    part_of = (pl.ds(2, 4), pl.ds(0, 4), pl.ds(4, 2), pl.ds(0, 2))

    def step_copy(slot, p):
        return pltpu.make_async_remote_copy(
            src_ref=out_buf.at[p, part_of[slot]],
            dst_ref=in_buf.at[p, slot, part_of[slot]],
            send_sem=send.at[p, slot],
            recv_sem=recv.at[p, slot],
            device_id=places[slot],
            device_id_type=MESH,
        )

    below, above, far_below, far_above = range(4)

    def combine_mid(own, got):
        return [own[q] + got(below, q + 2) + got(above, q - 2) for q in (2, 3)]

    def combine_rest(own, got):
        low = [own[q] + got(below, q + 2) + got(far_below, q + 4) for q in (0, 1)]
        top = [own[q] + got(above, q - 2) + got(far_above, q - 4) for q in (4, 5)]
        return low, top

    def columns(row):
        eye = iota((128, 128), 0) == iota((128, 128), 1)
        full = jnp.where(eye, jnp.broadcast_to(row, (128, 128)), 0.0)
        return jnp.sum(full, axis=1, keepdims=True)

    def pull(accs, pieces, cols):
        for r, col in cols.items():
            for half in range(2):
                b = (r % 2) * 2 + half
                base = b * NEAR + (r // 2) * OWN
                for i in range(0, OWN, 8):
                    at = half * OWN + i
                    c = col[at : at + 8, :]
                    for j, q in enumerate(pieces):
                        accs[j] = accs[j] + mt_ref[base + i : base + i + 8, q * 128 : (q + 1) * 128] * c
        return accs

    outer, inner = (0, 1, 4, 5), (2, 3)

    def evaluate(n, z, last):
        total = jnp.zeros((8, 512), F32)
        for tr in range(3):
            pair = jnp.concatenate([z[2 * tr], z[2 * tr + 1]], axis=0)
            lhs = jnp.concatenate(split(pair, 3) + [jnp.zeros((2, 128), BF16)], axis=0)
            total = total + jnp.dot(lhs, pick2_ref[tr], preferred_element_type=F32)
        total = total[0:2] + total[2:4] + total[4:6]
        means, tables = [], []
        for b in range(BANDS):
            rows = []
            tables.append([])
            for h in range(2):
                at = (b % 2) * 256 + h * 128
                row = total[b // 2 : b // 2 + 1, at : at + 128]
                tables[b].append(jnp.broadcast_to(row, (8, 128)))
                col = columns(row)
                for i in range(4):
                    blk = h * 4 + i
                    value = u_ref[b, blk * LIST : (blk + 1) * LIST, :] * col[i * LIST : (i + 1) * LIST, :]
                    rows.append(jnp.sum(value, axis=0, keepdims=True))
            means.append(ba[b, :, 0:ROWS] - jnp.concatenate(rows, axis=0))
        if last:
            for b in range(BANDS):
                fin[b, :, 0:ROWS] = means[b]
                fin[b, 0:1, 256:384] = z[2 + b // 2]
                fin[b, 1:8, 256:384] = jnp.zeros((7, 128), F32)
            for slot in range(BANDS):

                @pl.when(jnp.logical_not(owns(slot)))
                def _():
                    fin_copy(slot).start()

        lane = iota((1, 128), 1)
        found = jnp.zeros((1, 128), F32)
        for b in range(BANDS):
            pred = mix[b][0] * means[0]
            for b2 in range(1, BANDS):
                pred = pred + mix[b][b2] * means[b2]
            acc = jnp.zeros((8, 128), F32)
            for blk in range(BLOCKS):
                for half in range(2):
                    at = blk * ROWS + half * 128
                    idx = bs[b, :, at : at + 128] + (blk % 4) * LIST
                    picked = jnp.take_along_axis(tables[b][blk // 4], idx, axis=1)
                    left = bm[b, :, at : at + 128] - pred[blk : blk + 1, half * 128 : half * 128 + 128]
                    left = left - picked
                    acc = acc + bw[b, :, at : at + 128] * left * left
            value = jnp.sum(jnp.sum(acc, axis=0, keepdims=True), axis=1, keepdims=True)
            found = jnp.where(lane == n + b * SWEEPS, value, found)
        row_buf[0] = row_buf[0] + found

    def fin_copy(slot):
        return pltpu.make_async_remote_copy(
            src_ref=fin.at[slot],
            dst_ref=got,
            send_sem=fin_send.at[slot],
            recv_sem=fin_recv,
            device_id=(tile, slot),
            device_id_type=MESH,
        )

    x = (sky // 32) * 2 + band // 2
    y = (sky // 8) % 4
    z_at = sky % 8

    def core_at(dx, dy, dz, core):
        x_to, y_to, z_to = (x + dx) % 4, (y + dy) % 4, (z_at + dz) % 8
        return (x_to // 2) * 32 + y_to * 8 + z_to, (x_to % 2) * 2 + core

    def plane_copy(i):
        return pltpu.make_async_remote_copy(
            src_ref=row_buf.at[0],
            dst_ref=plane.at[x * 4 + y],
            send_sem=plane_send.at[i],
            recv_sem=plane_recv,
            device_id=core_at(PLANE[i][0], PLANE[i][1], 0, 1),
            device_id_type=MESH,
        )

    def line_copy(i):
        return pltpu.make_async_remote_copy(
            src_ref=row_buf.at[1],
            dst_ref=line.at[z_at % 4],
            send_sem=line_send.at[i],
            recv_sem=line_recv,
            device_id=core_at(0, 0, LINE[i][0], LINE[i][1]),
            device_id_type=MESH,
        )

    def whole(ref, sem):
        return pltpu.make_async_copy(ref, ref, sem)

    @pl.when(is_home)
    def _():
        build()
        for i in range(2):
            for slot in range(4):
                first_copy(slot, i).wait()
        start = []
        for i in range(2):
            own = [first_out[i, q] for q in range(6)]
            low, top = combine_rest(own, lambda s, q: first_in[i, s, q])
            start.append(low + combine_mid(own, lambda s, q: first_in[i, s, q]) + top)
        known, dens = start
        scale = [1.0 / (d + PRIOR_WEIGHT) for d in dens]
        colors = [bn[q : q + 1, 128:256] for q in range(6)]
        zero = jnp.zeros((1, 128), F32)
        z = [jnp.where(colors[q] == 0.0, known[q] * scale[q], zero) for q in range(6)]
        cols = {q: columns(z[q]) for q in range(6)}
        accs = pull([jnp.zeros((8, 128), F32) for _ in range(6)], range(6), cols)
        for q in range(6):
            out_buf[1, q] = jnp.sum(accs[q], axis=0, keepdims=True)
        for slot in (2, 3, 0, 1):
            step_copy(slot, 1).start()
        row_buf[0] = zero

        def renew(q, color, pulled, old):
            return jnp.where(colors[q] == color, (known[q] + pulled) * scale[q], old)

        def absorb(s, z, then):
            p = s % 2
            color = (s % COLORS).astype(F32) if not isinstance(s, int) else float(s % COLORS)
            own = [out_buf[p, q] for q in range(6)]
            take = lambda i, q: in_buf[p, i, q]
            z = list(z)
            for slot in (0, 1):
                step_copy(slot, p).wait_recv()
            mid = combine_mid(own, take)
            for q in inner:
                z[q] = renew(q, color, mid[q - 2], z[q])
            accs = None
            if then:
                cols = {q: columns(z[q]) for q in inner}
                accs = pull([jnp.zeros((8, 128), F32) for _ in range(6)], range(6), cols)
            for slot in (2, 3):
                step_copy(slot, p).wait_recv()
            low, top = combine_rest(own, take)
            for j, q in enumerate(outer):
                z[q] = renew(q, color, (low + top)[j], z[q])
            return z, accs

        def step(s, z):
            p = s % 2

            @pl.when((s == 2) & moves)
            def _():
                pl.semaphore_wait(go, 1)
                mag_copy(band).start()

            @pl.when(s % COLORS == 0)
            def _():
                @pl.when(s == COLORS)
                def _():
                    for slot in range(BANDS):

                        @pl.when(jnp.logical_not(owns(slot)))
                        def _():
                            mag_copy(slot).wait_recv()

                evaluate(s // COLORS - 1, z, False)

            z, accs = absorb(s, z, True)
            cols = {q: columns(z[q]) for q in outer}
            far = pull([accs[q] for q in outer], outer, cols)
            for j, q in enumerate(outer):
                out_buf[1 - p, q] = jnp.sum(far[j], axis=0, keepdims=True)
            for slot in (2, 3):
                step_copy(slot, 1 - p).start()
            near_accs = pull([accs[q] for q in inner], inner, cols)
            for j, q in enumerate(inner):
                out_buf[1 - p, q] = jnp.sum(near_accs[j], axis=0, keepdims=True)
            for slot in (0, 1):
                step_copy(slot, 1 - p).start()
            for slot in range(4):
                step_copy(slot, p).wait_send()
            return tuple(z)

        z = lax.fori_loop(1, STEPS - 1, step, tuple(z))
        z, _ = absorb(STEPS - 1, z, False)
        evaluate(SWEEPS - 1, z, True)
        for i in range(len(PLANE)):
            plane_copy(i).start()
        mine = pltpu.make_async_copy(row_buf.at[0], plane.at[x * 4 + y], plane_recv)
        mine.start()
        whole(plane, plane_recv).wait()
        row_buf[1] = jnp.sum(plane[...].reshape(16, 128), axis=0, keepdims=True)
        for i in range(len(LINE)):
            line_copy(i).start()
        mine = pltpu.make_async_copy(row_buf.at[1], line.at[z_at % 4], line_recv)
        mine.start()
        for i in range(len(PLANE)):
            plane_copy(i).wait_send()
        for slot in range(4):
            step_copy(slot, (STEPS - 1) % 2).wait_send()

    @pl.when(jnp.logical_not(is_home))
    def _():
        pl.semaphore_wait(go, 1)
        mag_copy(band).start()

    @pl.when(moves)
    def _():
        @pl.when(band == teller)
        def _():
            table_copy(1, band).wait_send()

        table_copy(0, band).wait_send()
        for c in range(CHUNKS):
            for i in range(2):
                ship_copy(i, band, c).wait_send()
        mag_copy(band).wait_send()
        fin_copy(0).wait_recv()

    @pl.when(stays)
    def _():
        mine = pltpu.make_async_copy(fin.at[band], got, local.at[0])
        mine.start()
        mine.wait()

    out_ref[:, 0:256] = got[:, 0:256]
    pair = got[0:1, 256:384]
    out_ref[:, 256:512] = jnp.zeros((8, 256), F32)
    out_ref[0:1, 256:384] = jnp.where(band % 2 == 0, pair, pltpu.roll(pair, OWN, 1))

    whole(line, line_recv).wait()
    total = jnp.sum(line[...].reshape(4, 128), axis=0, keepdims=True)
    total = pltpu.roll(total, (128 - band * SWEEPS) % 128, 1)
    out_ref[0:1, 384:512] = total * (1.0 / (OBS * STARS * TILES))

    @pl.when(is_home)
    def _():
        for slot in range(BANDS):

            @pl.when(jnp.logical_not(owns(slot)))
            def _():
                fin_copy(slot).wait_send()

        for i in range(len(LINE)):
            line_copy(i).wait_send()


def solve(color_terms, m, w, s, owner, colors, lists):
    vmem = pl.BlockSpec(memory_space=pltpu.VMEM)
    hbm = pl.BlockSpec(memory_space=pl.ANY)
    dma = pltpu.SemaphoreType.DMA
    return pl.pallas_call(
        solve_kernel,
        out_shape=jax.ShapeDtypeStruct((8, 512), F32),
        in_specs=[pl.BlockSpec(memory_space=pltpu.SMEM)] + [hbm] * 3 + [vmem] * 3,
        out_specs=vmem,
        scratch_shapes=[
            pltpu.VMEM((OBS, STARS), F32),
            pltpu.VMEM((OBS, STARS), F32),
            pltpu.VMEM((OBS, STARS), jnp.int32),
            pltpu.VMEM((8, 384), F32),
            pltpu.VMEM((8, 384), F32),
            pltpu.VMEM((BANDS, OBS, STARS), F32),
            pltpu.VMEM((BANDS, OBS, STARS), F32),
            pltpu.VMEM((BANDS, OBS, STARS), jnp.int32),
            pltpu.VMEM((BANDS, 8, 384), F32),
            pltpu.VMEM((8, 384), F32),
            pltpu.VMEM((BANDS, BLOCKS * LIST, ROWS), F32),
            pltpu.VMEM((2, BANDS, BLOCKS * LIST, WIDE), BF16),
            pltpu.VMEM((WIDE, WIDE), F32),
            pltpu.VMEM((3, 128, 512), BF16),
            pltpu.VMEM((2, 6, 1, 128), F32),
            pltpu.VMEM((2, 4, 6, 1, 128), F32),
            pltpu.VMEM((2, 6, 1, 128), F32),
            pltpu.VMEM((2, 4, 6, 1, 128), F32),
            pltpu.VMEM((BANDS, 8, 384), F32),
            pltpu.VMEM((8, 384), F32),
            pltpu.VMEM((2, 1, 128), F32),
            pltpu.VMEM((16, 1, 128), F32),
            pltpu.VMEM((4, 1, 128), F32),
            dma((3,)),
            dma((2, CHUNKS)),
            dma((BANDS, 2, CHUNKS)),
            dma,
            dma((BANDS,)),
            dma((2,)),
            dma((BANDS, 2)),
            dma((4,)),
            dma((2, 4)),
            dma((2, 4)),
            dma((2, 4)),
            dma((2, 4)),
            dma((BANDS,)),
            dma,
            dma((len(PLANE),)),
            dma,
            dma((len(LINE),)),
            dma,
            pltpu.SemaphoreType.REGULAR,
        ],
        compiler_params=pltpu.CompilerParams(has_side_effects=True, collective_id=0),
        name="solve",
    )(color_terms, m, w, s, owner, colors, lists)


def unpack_kernel(out_ref, zp_ref, mags_ref, mis_ref):
    zp_ref[...] = out_ref[0:1, 256 : 256 + OWN]
    mis_ref[...] = out_ref[0:1, 384 : 384 + SWEEPS]
    for blk in range(BLOCKS):
        mags_ref[0:1, blk * ROWS : (blk + 1) * ROWS] = out_ref[blk : blk + 1, 0:ROWS]


def body(magnitudes, weights, slots, block_fields, owner, colors, color_terms):
    out = solve(
        color_terms, magnitudes[0], weights[0], slots[0],
        owner.reshape(-1, 128), colors.reshape(-1, 128), block_fields,
    )
    vmem = pl.BlockSpec(memory_space=pltpu.VMEM)
    zp, mags, misfit = pl.pallas_call(
        unpack_kernel,
        out_shape=(
            jax.ShapeDtypeStruct((1, OWN), F32),
            jax.ShapeDtypeStruct((1, STARS), F32),
            jax.ShapeDtypeStruct((1, SWEEPS), F32),
        ),
        in_specs=[vmem],
        out_specs=(vmem,) * 3,
        name="unpack",
    )(out)
    return zp, mags, misfit.T


def solution(mesh):
    in_specs = (
        P("band", None, "sky"),
        P("band", None, "sky"),
        P("band", None, "sky"),
        P("sky", None),
        P(),
        P(),
        P(),
    )
    out_specs = (P("band", "sky"), P("band", "sky"), P(None, "band"))
    return jax.shard_map(body, mesh=mesh, in_specs=in_specs, out_specs=out_specs, check_vma=False)
```

```python
import functools

import jax
import jax.numpy as jnp
from jax import lax
from jax.experimental import pallas as pl
from jax.experimental.pallas import tpu as pltpu
from jax.sharding import PartitionSpec as P

COLORS = 8
SWEEPS = 4
PRIOR_WEIGHT = 1.0

TILES = 64
BANDS = 4
OBS = 8
BLOCKS = 8
ROWS = 256
STARS = BLOCKS * ROWS
LIST = 32
OWN = 64
NEAR = 3 * OWN
CUTS = (0, 2, 4, 6, 7, 8)
CHUNKS = len(CUTS) - 1
EARLY = 2
WIDE = BANDS * NEAR
STEPS = COLORS * SWEEPS
PLANE = [(i, j) for i in (2, 1, 3, 0) for j in (2, 1, 3, 0)][:-1]
LINE = [(k, c) for k in (4, 3, 5, 2, 6, 1, 7, 0) for c in (0, 1)][:-1]
MESH = pl.DeviceIdType.MESH
HIGH = lax.Precision.HIGHEST
F32 = jnp.float32
BF16 = jnp.bfloat16


def home_of(tile):
    half = tile // 32
    row = tile // 8
    y = row % 4
    z = tile % 8
    leg = z // 4
    y_new = y + half * (3 - 2 * y)
    z_new = z + leg * (7 - 2 * z)
    x_lo = (1 - half + row + leg) % 2
    return half * 32 + y_new * 8 + z_new, x_lo * 2 + 1


def tile_at(sky, band):
    half = sky // 32
    y_new = (sky // 8) % 4
    z_new = sky % 8
    y = y_new + half * (3 - 2 * y_new)
    row = half * 4 + y
    leg = (band // 2 + 1 + half + row) % 2
    z = z_new + leg * (7 - 2 * z_new)
    is_home = (band % 2 == 1) & (z_new < 4)
    return is_home, (row * 8 + z) % TILES


def iota(shape, dim):
    return lax.broadcasted_iota(jnp.int32, shape, dim)


def as_column(row, count):
    eye = iota((count, 128), 0) == iota((count, 128), 1)
    full = jnp.broadcast_to(row, (count, 128))
    return jnp.sum(jnp.where(eye, full, 0.0), axis=1, keepdims=True)


def as_row(col, shift):
    n = col.shape[0]
    hit = iota((n, 128), 1) == iota((n, 128), 0) + shift
    return jnp.sum(jnp.where(hit, col, 0.0), axis=0, keepdims=True)


def split(x, terms):
    parts = []
    for _ in range(terms - 1):
        part = x.astype(BF16)
        parts.append(part)
        x = x - part.astype(F32)
    return parts + [x.astype(BF16)]


def tile_tables(tile, own_ref, col_ref, lst_ref, near_ref):
    rows = own_ref.shape[0]
    until = jnp.where(iota((128, 128), 0) <= iota((128, 128), 1), 1.0, 0.0).astype(BF16)
    before = jnp.where(iota((rows, rows), 1) < iota((rows, rows), 0), 1.0, 0.0).astype(BF16)
    number = (iota((rows, 128), 0) * 128 + iota((rows, 128), 1)).astype(F32)
    shade = col_ref[...].astype(F32)
    rank_at = iota((OWN, 128), 0).astype(F32)
    for tr in range(3):
        mine = own_ref[...] == (tile + tr - 1 + TILES) % TILES
        one = jnp.where(mine, 1.0, 0.0)
        inside = jnp.dot(one.astype(BF16), until, preferred_element_type=F32)
        above = jnp.dot(before, one.astype(BF16), preferred_element_type=F32)
        above = jnp.sum(above, axis=1, keepdims=True)
        rank = jnp.where(mine, inside + above - 1.0, -1.0)
        ids = jnp.zeros((OWN, 128), F32)
        cols = jnp.zeros((OWN, 128), F32)
        for i in range(rows):
            hit = rank[i : i + 1] == rank_at
            ids = ids + jnp.where(hit, number[i : i + 1], 0.0)
            cols = cols + jnp.where(hit, shade[i : i + 1], 0.0)
        for value, at in ((ids, 0), (cols, 128)):
            col = jnp.sum(value, axis=1, keepdims=True)
            row = as_row(col, 0) + as_row(col, OWN)
            near_ref[2 * tr : 2 * tr + 1, at : at + 128] = row
            near_ref[2 * tr + 1 : 2 * tr + 2, at : at + 128] = row
    near_ref[6:8, 128:256] = jnp.zeros((2, 128), F32)
    listed = lst_ref[...].astype(F32)
    near_ref[:, 256:384] = jnp.concatenate([listed] * BANDS, axis=1)
    for h in range(2):
        row = [listed[i : i + 1] for i in range(4 * h, 4 * h + 4)]
        near_ref[6 + h : 7 + h, 0:128] = jnp.concatenate(row, axis=1)


def star_means(m_ref, w_ref, mean_ref):
    for blk in range(BLOCKS):
        cols = slice(blk * ROWS, (blk + 1) * ROWS)
        top = jnp.sum(w_ref[:, cols] * m_ref[:, cols], axis=0, keepdims=True)
        mean_ref[blk : blk + 1, :] = top / jnp.sum(w_ref[:, cols], axis=0, keepdims=True)


def list_sums(m_ref, w_ref, s_ref, pred, aux_ref):
    entries = iota((LIST, ROWS), 0)
    rows = [jnp.zeros((1, 128), F32) for _ in range(4)]
    for blk in range(BLOCKS):
        cols = slice(blk * ROWS, (blk + 1) * ROWS)
        acc = jnp.zeros((LIST, ROWS), F32)
        wts = jnp.zeros((LIST, ROWS), F32)
        for k in range(OBS):
            hit = s_ref[k : k + 1, cols] == entries
            wk = w_ref[k : k + 1, cols]
            wts = wts + jnp.where(hit, wk, 0.0)
            acc = acc + jnp.where(hit, wk * (m_ref[k : k + 1, cols] - pred[blk : blk + 1]), 0.0)
        h, at = blk // 4, (blk % 4) * LIST
        rows[h] = rows[h] + as_row(jnp.sum(acc, axis=1, keepdims=True), at)
        rows[2 + h] = rows[2 + h] + as_row(jnp.sum(wts, axis=1, keepdims=True), at)
    aux_ref[...] = jnp.concatenate(rows + [jnp.zeros((4, 128), F32)], axis=0)


def solve_kernel(
    ct_ref, m_hbm, w_hbm, s_hbm, own_ref, col_ref, lst_ref,
    out_ref,
    m_ref, w_ref, s_ref,
    mean, mates, aux, near, bm, bw, bs, ba, bt, bn, u_ref, r_ref, mt_ref, pick2_ref,
    first_out, first_in, out_buf, in_buf, fin, got, row_buf, plane, line,
    load_sem, mate_send, mate_recv, ship_send, ship_recv, mag_send, mag_recv, tab_send, tab_recv, local,
    first_send, first_recv, send, recv,
    fin_send, fin_recv, plane_send, plane_recv, line_send, line_recv, go,
):
    sky = lax.axis_index("sky")
    band = lax.axis_index("band")
    home_sky, home_band = home_of(sky)
    stays = (home_sky == sky) & (home_band == band)
    moves = jnp.logical_not(stays)
    is_home, tile = tile_at(sky, band)
    places = [home_of((tile + d + TILES) % TILES) for d in (1, -1, 2, -2)]

    def owns(slot):
        return (tile == sky) & (band == slot)

    barrier = pltpu.get_barrier_semaphore()
    mates_of = [(band + i) % BANDS for i in range(1, BANDS)]
    for mate in mates_of:
        pl.semaphore_signal(barrier, inc=1, device_id=(sky, mate), device_id_type=MESH)

    @pl.when(moves)
    def _():
        pl.semaphore_signal(barrier, inc=1, device_id=(home_sky, home_band), device_id_type=MESH)

    @pl.when(is_home)
    def _():
        for place in places:
            pl.semaphore_signal(barrier, inc=1, device_id=place, device_id_type=MESH)
        for slot in range(BANDS):

            @pl.when(jnp.logical_not(owns(slot)))
            def _():
                pl.semaphore_signal(barrier, inc=1, device_id=(tile, slot), device_id_type=MESH)

    loads = [
        pltpu.make_async_copy(src, dst, load_sem.at[i])
        for i, (src, dst) in enumerate(((m_hbm, m_ref), (w_hbm, w_ref), (s_hbm, s_ref)))
    ]
    for load in loads:
        load.start()
    tile_tables(sky, own_ref, col_ref, lst_ref, near)
    for load in loads:
        load.wait()
    star_means(m_ref, w_ref, mean)

    @pl.when(is_home & moves)
    def _():
        pl.semaphore_wait(barrier, 12)

    @pl.when(is_home & stays)
    def _():
        pl.semaphore_wait(barrier, 10)

    @pl.when(jnp.logical_not(is_home))
    def _():
        pl.semaphore_wait(barrier, 4)

    def chunk(ref, slot, c):
        at = pl.ds(CUTS[c] * ROWS, (CUTS[c + 1] - CUTS[c]) * ROWS)
        return ref.at[:, at] if slot is None else ref.at[slot, :, at]

    def ship_copy(i, slot, c):
        src, dst = ((w_ref, bw), (s_ref, bs))[i]
        return pltpu.make_async_remote_copy(
            src_ref=chunk(src, None, c),
            dst_ref=chunk(dst, slot, c),
            send_sem=ship_send.at[i, c],
            recv_sem=ship_recv.at[slot, i, c],
            device_id=(home_sky, home_band),
            device_id_type=MESH,
        )

    def mag_copy(slot):
        return pltpu.make_async_remote_copy(
            src_ref=m_ref,
            dst_ref=bm.at[slot],
            send_sem=mag_send,
            recv_sem=mag_recv.at[slot],
            device_id=(home_sky, home_band),
            device_id_type=MESH,
        )

    def mate_copy(i):
        return pltpu.make_async_remote_copy(
            src_ref=mean,
            dst_ref=mates.at[band],
            send_sem=mate_send.at[i],
            recv_sem=mate_recv.at[i],
            device_id=(sky, mates_of[i]),
            device_id_type=MESH,
        )

    def table_copy(i, slot):
        src, dst = ((mean, ba.at[slot]), (near, bn), (aux, bt.at[slot]))[i]
        return pltpu.make_async_remote_copy(
            src_ref=src,
            dst_ref=dst,
            send_sem=tab_send.at[i],
            recv_sem=tab_recv.at[slot, i],
            device_id=(home_sky, home_band),
            device_id_type=MESH,
        )

    teller = 0

    for i in range(BANDS - 1):
        mate_copy(i).start()
    keep = pltpu.make_async_copy(mean, mates.at[band], local.at[4])
    keep.start()

    @pl.when(moves)
    def _():
        @pl.when(band == teller)
        def _():
            table_copy(1, band).start()

        table_copy(0, band).start()
        for c in range(EARLY):
            for i in range(2):
                ship_copy(i, band, c).start()

    mix = []
    for b in range(BANDS):
        total = ct_ref[b, 0]
        for b2 in range(1, BANDS):
            total = total + ct_ref[b, b2]
        mix.append([ct_ref[b, b2] + (1.0 - total if b == b2 else 0.0) for b2 in range(BANDS)])

    keep.wait()
    for i in range(BANDS - 1):
        mate_copy(i).wait_recv()
    pred = jnp.zeros((BLOCKS, ROWS), F32)
    for b2 in range(BANDS):
        factor = mix[0][b2]
        for b in range(1, BANDS):
            factor = jnp.where(band == b, mix[b][b2], factor)
        pred = pred + factor * mates[b2]
    list_sums(m_ref, w_ref, s_ref, pred, aux)

    @pl.when(moves)
    def _():
        table_copy(2, band).start()
        for c in range(EARLY, CHUNKS):
            for i in range(2):
                ship_copy(i, band, c).start()

    @pl.when(stays)
    def _():
        copies = [
            pltpu.make_async_copy(mean, ba.at[band], local.at[0]),
            pltpu.make_async_copy(w_ref, bw.at[band], local.at[1]),
            pltpu.make_async_copy(s_ref, bs.at[band], local.at[2]),
            pltpu.make_async_copy(m_ref, bm.at[band], local.at[3]),
            pltpu.make_async_copy(aux, bt.at[band], local.at[4]),
        ]
        for copy in copies:
            copy.start()
        for copy in copies:
            copy.wait()

    for i in range(BANDS - 1):
        mate_copy(i).wait_send()

    def await_tables():
        table_copy(1, teller).wait_recv()
        for slot in range(BANDS):

            @pl.when(jnp.logical_not(owns(slot)))
            def _():
                table_copy(0, slot).wait_recv()

    def await_sums():
        for slot in range(BANDS):

            @pl.when(jnp.logical_not(owns(slot)))
            def _():
                table_copy(2, slot).wait_recv()

    def await_chunk(c):
        for slot in range(BANDS):

            @pl.when(jnp.logical_not(owns(slot)))
            def _():
                for i in range(2):
                    ship_copy(i, slot, c).wait_recv()

    def build():
        row_band = iota((128, 128), 0) // LIST
        lane_list = iota((128, 128), 1) // LIST
        lane_own = iota((128, 128), 1) // OWN
        mixes = jnp.zeros((128, 128), F32)
        for b2 in range(BANDS):
            for b in range(BANDS):
                mixes = jnp.where((row_band == b2) & (lane_list == b), mix[b][b2], mixes)
        entries = iota((LIST, ROWS), 0)
        await_tables()
        pick = []
        for tr in range(3):
            col = as_column(bn[2 * tr : 2 * tr + 1, 0:128], OWN)
            one = jnp.concatenate(
                [jnp.where(col == bn[6 + h : 7 + h, 0:128], 1.0, 0.0) for h in range(2)], axis=1
            ).astype(BF16)
            none = jnp.zeros((OWN, 256), BF16)
            pick2_ref[tr, 0:OWN, 0:256] = one
            pick2_ref[tr, OWN:128, 0:256] = none
            pick2_ref[tr, 0:OWN, 256:512] = none
            pick2_ref[tr, OWN:128, 256:512] = one
            pick.append(one)
        pick = jnp.concatenate(pick, axis=0)
        for blk in range(BLOCKS):
            if blk in CUTS:
                await_chunk(CUTS.index(blk))
            if blk == CUTS[-2]:
                for slot in range(BANDS):

                    @pl.when(jnp.logical_not(owns(slot)))
                    def _():
                        pl.semaphore_signal(go, inc=1, device_id=(tile, slot), device_id_type=MESH)

            cols = slice(blk * ROWS, (blk + 1) * ROWS)
            wide, scaled = [], []
            for b in range(BANDS):
                acc = jnp.zeros((LIST, ROWS), F32)
                for k in range(OBS):
                    wk = bw[b, k : k + 1, cols]
                    acc = acc + jnp.where(bs[b, k : k + 1, cols] == entries, wk, 0.0)
                star_w = jnp.sum(bw[b, :, cols], axis=0, keepdims=True)
                wide.append(acc)
                scaled.append(acc * (1.0 / star_w))
                u_ref[b, blk * LIST : (blk + 1) * LIST, :] = scaled[b]
            w_hi, w_lo = split(jnp.concatenate(wide, axis=0), 2)
            u_hi, u_lo = split(jnp.concatenate(scaled, axis=0), 2)
            dims = (((1,), (1,)), ((), ()))
            both = lax.dot_general(
                jnp.concatenate([u_hi, u_lo], axis=0), w_hi, dims, preferred_element_type=F32
            )
            gt = both[0:128] + both[128:256]
            gt = gt + lax.dot_general(u_hi, w_lo, dims, preferred_element_type=F32)
            lhs = jnp.concatenate(split(gt * mixes, 2), axis=0)
            col = as_column(bn[blk : blk + 1, 256:384], 128)
            for q in range(6):
                hit = (col == bn[q : q + 1, 0:128]) & (row_band == lane_own + 2 * (q % 2))
                moved = jnp.dot(
                    lhs, jnp.where(hit, 1.0, 0.0).astype(BF16), preferred_element_type=F32
                ).astype(BF16)
                for i in range(2):
                    for b2 in range(BANDS):
                        at = i * 128 + b2 * LIST
                        r_ref[
                            i, b2, blk * LIST : (blk + 1) * LIST, q * 128 : (q + 1) * 128
                        ] = moved[at : at + LIST]
            if blk == CUTS[EARLY] - 1:
                await_sums()
                first_sums(pick)
            if blk in (3, 7):
                at = slice((blk - 3) * LIST, (blk + 1) * LIST)
                for b2 in range(BANDS):
                    total = jnp.dot(pick[:, at], r_ref[0, b2, at, :], preferred_element_type=F32)
                    total = total + jnp.dot(pick[:, at], r_ref[1, b2, at, :], preferred_element_type=F32)
                    rows = slice(b2 * NEAR, (b2 + 1) * NEAR)
                    mt_ref[rows, :] = total if blk == 3 else mt_ref[rows, :] + total

    def first_sums(pick):
        rows = [jnp.concatenate([bt[b, h : h + 1, :] for h in range(2)], axis=1) for b in range(BANDS)]
        rows += [jnp.concatenate([bt[b, h : h + 1, :] for h in (2, 3)], axis=1) for b in range(BANDS)]
        terms = jnp.concatenate(split(jnp.concatenate(rows, axis=0), 3), axis=0)
        sums = lax.dot_general(terms, pick, (((1,), (1,)), ((), ())), preferred_element_type=F32)
        sums = sums[0:8] + sums[8:16] + sums[16:24]
        for i in range(2):
            for q in range(6):
                tr, b = q // 2, 2 * (q % 2)
                at = slice(tr * OWN, (tr + 1) * OWN)
                low, high = i * BANDS + b, i * BANDS + b + 1
                first_out[i, q] = jnp.concatenate(
                    [sums[low : low + 1, at], sums[high : high + 1, at]], axis=1
                )
        for i in range(2):
            for slot in (2, 3, 0, 1):
                first_copy(slot, i).start()
    def first_copy(slot, i):
        return pltpu.make_async_remote_copy(
            src_ref=first_out.at[i],
            dst_ref=first_in.at[i, slot],
            send_sem=first_send.at[i, slot],
            recv_sem=first_recv.at[i, slot],
            device_id=places[slot],
            device_id_type=MESH,
        )

    part_of = (pl.ds(2, 4), pl.ds(0, 4), pl.ds(4, 2), pl.ds(0, 2))

    def step_copy(slot, p):
        return pltpu.make_async_remote_copy(
            src_ref=out_buf.at[p, part_of[slot]],
            dst_ref=in_buf.at[p, slot, part_of[slot]],
            send_sem=send.at[p, slot],
            recv_sem=recv.at[p, slot],
            device_id=places[slot],
            device_id_type=MESH,
        )

    below, above, far_below, far_above = range(4)

    def combine_mid(own, got):
        return [own[q] + got(below, q + 2) + got(above, q - 2) for q in (2, 3)]

    def combine_rest(own, got):
        low = [own[q] + got(below, q + 2) + got(far_below, q + 4) for q in (0, 1)]
        top = [own[q] + got(above, q - 2) + got(far_above, q - 4) for q in (4, 5)]
        return low, top

    def columns(row):
        eye = iota((128, 128), 0) == iota((128, 128), 1)
        full = jnp.where(eye, jnp.broadcast_to(row, (128, 128)), 0.0)
        return jnp.sum(full, axis=1, keepdims=True)

    def pull(accs, pieces, cols):
        for r, col in cols.items():
            for half in range(2):
                b = (r % 2) * 2 + half
                base = b * NEAR + (r // 2) * OWN
                for i in range(0, OWN, 8):
                    at = half * OWN + i
                    c = col[at : at + 8, :]
                    for j, q in enumerate(pieces):
                        accs[j] = accs[j] + mt_ref[base + i : base + i + 8, q * 128 : (q + 1) * 128] * c
        return accs

    outer, inner = (0, 1, 4, 5), (2, 3)

    def evaluate(n, z, last):
        total = jnp.zeros((8, 512), F32)
        for tr in range(3):
            pair = jnp.concatenate([z[2 * tr], z[2 * tr + 1]], axis=0)
            lhs = jnp.concatenate(split(pair, 3) + [jnp.zeros((2, 128), BF16)], axis=0)
            total = total + jnp.dot(lhs, pick2_ref[tr], preferred_element_type=F32)
        total = total[0:2] + total[2:4] + total[4:6]
        means, tables = [], []
        for b in range(BANDS):
            rows = []
            tables.append([])
            for h in range(2):
                at = (b % 2) * 256 + h * 128
                row = total[b // 2 : b // 2 + 1, at : at + 128]
                tables[b].append(jnp.broadcast_to(row, (8, 128)))
                col = columns(row)
                for i in range(4):
                    blk = h * 4 + i
                    value = u_ref[b, blk * LIST : (blk + 1) * LIST, :] * col[i * LIST : (i + 1) * LIST, :]
                    rows.append(jnp.sum(value, axis=0, keepdims=True))
            means.append(ba[b] - jnp.concatenate(rows, axis=0))
        if last:
            for b in range(BANDS):
                fin[b, :, 0:ROWS] = means[b]
                fin[b, 0:1, 256:384] = z[2 + b // 2]
                fin[b, 1:8, 256:384] = jnp.zeros((7, 128), F32)
            for slot in range(BANDS):

                @pl.when(jnp.logical_not(owns(slot)))
                def _():
                    fin_copy(slot).start()

        lane = iota((1, 128), 1)
        found = jnp.zeros((1, 128), F32)
        for b in range(BANDS):
            pred = mix[b][0] * means[0]
            for b2 in range(1, BANDS):
                pred = pred + mix[b][b2] * means[b2]
            acc = jnp.zeros((8, 128), F32)
            for blk in range(BLOCKS):
                for half in range(2):
                    at = blk * ROWS + half * 128
                    idx = bs[b, :, at : at + 128] + (blk % 4) * LIST
                    picked = jnp.take_along_axis(tables[b][blk // 4], idx, axis=1)
                    left = bm[b, :, at : at + 128] - pred[blk : blk + 1, half * 128 : half * 128 + 128]
                    left = left - picked
                    acc = acc + bw[b, :, at : at + 128] * left * left
            value = jnp.sum(jnp.sum(acc, axis=0, keepdims=True), axis=1, keepdims=True)
            found = jnp.where(lane == n + b * SWEEPS, value, found)
        row_buf[0] = row_buf[0] + found

    def fin_copy(slot):
        return pltpu.make_async_remote_copy(
            src_ref=fin.at[slot],
            dst_ref=got,
            send_sem=fin_send.at[slot],
            recv_sem=fin_recv,
            device_id=(tile, slot),
            device_id_type=MESH,
        )

    x = (sky // 32) * 2 + band // 2
    y = (sky // 8) % 4
    z_at = sky % 8

    def core_at(dx, dy, dz, core):
        x_to, y_to, z_to = (x + dx) % 4, (y + dy) % 4, (z_at + dz) % 8
        return (x_to // 2) * 32 + y_to * 8 + z_to, (x_to % 2) * 2 + core

    def plane_copy(i):
        return pltpu.make_async_remote_copy(
            src_ref=row_buf.at[0],
            dst_ref=plane.at[x * 4 + y],
            send_sem=plane_send.at[i],
            recv_sem=plane_recv,
            device_id=core_at(PLANE[i][0], PLANE[i][1], 0, 1),
            device_id_type=MESH,
        )

    def line_copy(i):
        return pltpu.make_async_remote_copy(
            src_ref=row_buf.at[1],
            dst_ref=line.at[z_at % 4],
            send_sem=line_send.at[i],
            recv_sem=line_recv,
            device_id=core_at(0, 0, LINE[i][0], LINE[i][1]),
            device_id_type=MESH,
        )

    def whole(ref, sem):
        return pltpu.make_async_copy(ref, ref, sem)

    @pl.when(is_home)
    def _():
        build()
        for i in range(2):
            for slot in range(4):
                first_copy(slot, i).wait()
        start = []
        for i in range(2):
            own = [first_out[i, q] for q in range(6)]
            low, top = combine_rest(own, lambda s, q: first_in[i, s, q])
            start.append(low + combine_mid(own, lambda s, q: first_in[i, s, q]) + top)
        known, dens = start
        scale = [1.0 / (d + PRIOR_WEIGHT) for d in dens]
        colors = [bn[q : q + 1, 128:256] for q in range(6)]
        zero = jnp.zeros((1, 128), F32)
        z = [jnp.where(colors[q] == 0.0, known[q] * scale[q], zero) for q in range(6)]
        cols = {q: columns(z[q]) for q in range(6)}
        accs = pull([jnp.zeros((8, 128), F32) for _ in range(6)], range(6), cols)
        for q in range(6):
            out_buf[1, q] = jnp.sum(accs[q], axis=0, keepdims=True)
        for slot in (2, 3, 0, 1):
            step_copy(slot, 1).start()
        row_buf[0] = zero

        def renew(q, color, pulled, old):
            return jnp.where(colors[q] == color, (known[q] + pulled) * scale[q], old)

        def absorb(s, z, then):
            p = s % 2
            color = (s % COLORS).astype(F32) if not isinstance(s, int) else float(s % COLORS)
            own = [out_buf[p, q] for q in range(6)]
            take = lambda i, q: in_buf[p, i, q]
            z = list(z)
            for slot in (0, 1):
                step_copy(slot, p).wait_recv()
            mid = combine_mid(own, take)
            for q in inner:
                z[q] = renew(q, color, mid[q - 2], z[q])
            accs = None
            if then:
                cols = {q: columns(z[q]) for q in inner}
                accs = pull([jnp.zeros((8, 128), F32) for _ in range(6)], range(6), cols)
            for slot in (2, 3):
                step_copy(slot, p).wait_recv()
            low, top = combine_rest(own, take)
            for j, q in enumerate(outer):
                z[q] = renew(q, color, (low + top)[j], z[q])
            return z, accs

        def step(s, z):
            p = s % 2

            @pl.when((s == 2) & moves)
            def _():
                pl.semaphore_wait(go, 1)
                mag_copy(band).start()

            @pl.when(s % COLORS == 0)
            def _():
                @pl.when(s == COLORS)
                def _():
                    for slot in range(BANDS):

                        @pl.when(jnp.logical_not(owns(slot)))
                        def _():
                            mag_copy(slot).wait_recv()

                evaluate(s // COLORS - 1, z, False)

            z, accs = absorb(s, z, True)
            cols = {q: columns(z[q]) for q in outer}
            far = pull([accs[q] for q in outer], outer, cols)
            for j, q in enumerate(outer):
                out_buf[1 - p, q] = jnp.sum(far[j], axis=0, keepdims=True)
            for slot in (2, 3):
                step_copy(slot, 1 - p).start()
            near_accs = pull([accs[q] for q in inner], inner, cols)
            for j, q in enumerate(inner):
                out_buf[1 - p, q] = jnp.sum(near_accs[j], axis=0, keepdims=True)
            for slot in (0, 1):
                step_copy(slot, 1 - p).start()
            for slot in range(4):
                step_copy(slot, p).wait_send()
            return tuple(z)

        z = lax.fori_loop(1, STEPS - 1, step, tuple(z))
        z, _ = absorb(STEPS - 1, z, False)
        evaluate(SWEEPS - 1, z, True)
        for i in range(len(PLANE)):
            plane_copy(i).start()
        mine = pltpu.make_async_copy(row_buf.at[0], plane.at[x * 4 + y], plane_recv)
        mine.start()
        whole(plane, plane_recv).wait()
        row_buf[1] = jnp.sum(plane[...].reshape(16, 128), axis=0, keepdims=True)
        for i in range(len(LINE)):
            line_copy(i).start()
        mine = pltpu.make_async_copy(row_buf.at[1], line.at[z_at % 4], line_recv)
        mine.start()
        for i in range(len(PLANE)):
            plane_copy(i).wait_send()
        for slot in range(4):
            step_copy(slot, (STEPS - 1) % 2).wait_send()

    @pl.when(jnp.logical_not(is_home))
    def _():
        pl.semaphore_wait(go, 1)
        mag_copy(band).start()

    @pl.when(moves)
    def _():
        @pl.when(band == teller)
        def _():
            table_copy(1, band).wait_send()

        table_copy(0, band).wait_send()
        table_copy(2, band).wait_send()
        for c in range(CHUNKS):
            for i in range(2):
                ship_copy(i, band, c).wait_send()
        mag_copy(band).wait_send()
        fin_copy(0).wait_recv()

    @pl.when(stays)
    def _():
        mine = pltpu.make_async_copy(fin.at[band], got, local.at[0])
        mine.start()
        mine.wait()

    out_ref[:, 0:256] = got[:, 0:256]
    pair = got[0:1, 256:384]
    out_ref[:, 256:512] = jnp.zeros((8, 256), F32)
    out_ref[0:1, 256:384] = jnp.where(band % 2 == 0, pair, pltpu.roll(pair, OWN, 1))

    whole(line, line_recv).wait()
    total = jnp.sum(line[...].reshape(4, 128), axis=0, keepdims=True)
    total = pltpu.roll(total, (128 - band * SWEEPS) % 128, 1)
    out_ref[0:1, 384:512] = total * (1.0 / (OBS * STARS * TILES))

    @pl.when(is_home)
    def _():
        for slot in range(BANDS):

            @pl.when(jnp.logical_not(owns(slot)))
            def _():
                fin_copy(slot).wait_send()

        for i in range(len(LINE)):
            line_copy(i).wait_send()


def solve(color_terms, m, w, s, owner, colors, lists):
    vmem = pl.BlockSpec(memory_space=pltpu.VMEM)
    hbm = pl.BlockSpec(memory_space=pl.ANY)
    dma = pltpu.SemaphoreType.DMA
    return pl.pallas_call(
        solve_kernel,
        out_shape=jax.ShapeDtypeStruct((8, 512), F32),
        in_specs=[pl.BlockSpec(memory_space=pltpu.SMEM)] + [hbm] * 3 + [vmem] * 3,
        out_specs=vmem,
        scratch_shapes=[
            pltpu.VMEM((OBS, STARS), F32),
            pltpu.VMEM((OBS, STARS), F32),
            pltpu.VMEM((OBS, STARS), jnp.int32),
            pltpu.VMEM((BLOCKS, ROWS), F32),
            pltpu.VMEM((BANDS, BLOCKS, ROWS), F32),
            pltpu.VMEM((8, 128), F32),
            pltpu.VMEM((8, 384), F32),
            pltpu.VMEM((BANDS, OBS, STARS), F32),
            pltpu.VMEM((BANDS, OBS, STARS), F32),
            pltpu.VMEM((BANDS, OBS, STARS), jnp.int32),
            pltpu.VMEM((BANDS, BLOCKS, ROWS), F32),
            pltpu.VMEM((BANDS, 8, 128), F32),
            pltpu.VMEM((8, 384), F32),
            pltpu.VMEM((BANDS, BLOCKS * LIST, ROWS), F32),
            pltpu.VMEM((2, BANDS, BLOCKS * LIST, WIDE), BF16),
            pltpu.VMEM((WIDE, WIDE), F32),
            pltpu.VMEM((3, 128, 512), BF16),
            pltpu.VMEM((2, 6, 1, 128), F32),
            pltpu.VMEM((2, 4, 6, 1, 128), F32),
            pltpu.VMEM((2, 6, 1, 128), F32),
            pltpu.VMEM((2, 4, 6, 1, 128), F32),
            pltpu.VMEM((BANDS, 8, 384), F32),
            pltpu.VMEM((8, 384), F32),
            pltpu.VMEM((2, 1, 128), F32),
            pltpu.VMEM((16, 1, 128), F32),
            pltpu.VMEM((4, 1, 128), F32),
            dma((3,)),
            dma((BANDS - 1,)),
            dma((BANDS - 1,)),
            dma((2, CHUNKS)),
            dma((BANDS, 2, CHUNKS)),
            dma,
            dma((BANDS,)),
            dma((3,)),
            dma((BANDS, 3)),
            dma((5,)),
            dma((2, 4)),
            dma((2, 4)),
            dma((2, 4)),
            dma((2, 4)),
            dma((BANDS,)),
            dma,
            dma((len(PLANE),)),
            dma,
            dma((len(LINE),)),
            dma,
            pltpu.SemaphoreType.REGULAR,
        ],
        compiler_params=pltpu.CompilerParams(has_side_effects=True, collective_id=0),
        name="solve",
    )(color_terms, m, w, s, owner, colors, lists)


def unpack_kernel(out_ref, zp_ref, mags_ref, mis_ref):
    zp_ref[...] = out_ref[0:1, 256 : 256 + OWN]
    mis_ref[...] = out_ref[0:1, 384 : 384 + SWEEPS]
    for blk in range(BLOCKS):
        mags_ref[0:1, blk * ROWS : (blk + 1) * ROWS] = out_ref[blk : blk + 1, 0:ROWS]


def body(magnitudes, weights, slots, block_fields, owner, colors, color_terms):
    out = solve(
        color_terms, magnitudes[0], weights[0], slots[0],
        owner.reshape(-1, 128), colors.reshape(-1, 128), block_fields,
    )
    vmem = pl.BlockSpec(memory_space=pltpu.VMEM)
    zp, mags, misfit = pl.pallas_call(
        unpack_kernel,
        out_shape=(
            jax.ShapeDtypeStruct((1, OWN), F32),
            jax.ShapeDtypeStruct((1, STARS), F32),
            jax.ShapeDtypeStruct((1, SWEEPS), F32),
        ),
        in_specs=[vmem],
        out_specs=(vmem,) * 3,
        name="unpack",
    )(out)
    return zp, mags, misfit.T


def solution(mesh):
    in_specs = (
        P("band", None, "sky"),
        P("band", None, "sky"),
        P("band", None, "sky"),
        P("sky", None),
        P(),
        P(),
        P(),
    )
    out_specs = (P("band", "sky"), P("band", "sky"), P(None, "band"))
    return jax.shard_map(body, mesh=mesh, in_specs=in_specs, out_specs=out_specs, check_vma=False)
```

```python
import functools

import jax
import jax.numpy as jnp
from jax import lax
from jax.experimental import pallas as pl
from jax.experimental.pallas import tpu as pltpu
from jax.sharding import PartitionSpec as P

COLORS = 8
SWEEPS = 4
PRIOR_WEIGHT = 1.0

TILES = 64
BANDS = 4
OBS = 8
BLOCKS = 8
ROWS = 256
STARS = BLOCKS * ROWS
LIST = 32
OWN = 64
NEAR = 3 * OWN
CUTS = (0, 2, 4, 6, 7, 8)
CHUNKS = len(CUTS) - 1
EARLY = 2
WIDE = BANDS * NEAR
STEPS = COLORS * SWEEPS
PLANE = [(i, j) for i in (2, 1, 3, 0) for j in (2, 1, 3, 0)][:-1]
LINE = [(k, c) for k in (4, 3, 5, 2, 6, 1, 7, 0) for c in (0, 1)][:-1]
MESH = pl.DeviceIdType.MESH
HIGH = lax.Precision.HIGHEST
F32 = jnp.float32
BF16 = jnp.bfloat16


def home_of(tile):
    half = tile // 32
    row = tile // 8
    y = row % 4
    z = tile % 8
    leg = z // 4
    y_new = y + half * (3 - 2 * y)
    z_new = z + leg * (7 - 2 * z)
    x_lo = (1 - half + row + leg) % 2
    return half * 32 + y_new * 8 + z_new, x_lo * 2 + 1


def tile_at(sky, band):
    half = sky // 32
    y_new = (sky // 8) % 4
    z_new = sky % 8
    y = y_new + half * (3 - 2 * y_new)
    row = half * 4 + y
    leg = (band // 2 + 1 + half + row) % 2
    z = z_new + leg * (7 - 2 * z_new)
    is_home = (band % 2 == 1) & (z_new < 4)
    return is_home, (row * 8 + z) % TILES


def iota(shape, dim):
    return lax.broadcasted_iota(jnp.int32, shape, dim)


def as_column(row, count):
    eye = iota((count, 128), 0) == iota((count, 128), 1)
    full = jnp.broadcast_to(row, (count, 128))
    return jnp.sum(jnp.where(eye, full, 0.0), axis=1, keepdims=True)


def as_row(col, shift):
    n = col.shape[0]
    hit = iota((n, 128), 1) == iota((n, 128), 0) + shift
    return jnp.sum(jnp.where(hit, col, 0.0), axis=0, keepdims=True)


def split(x, terms):
    parts = []
    for _ in range(terms - 1):
        part = x.astype(BF16)
        parts.append(part)
        x = x - part.astype(F32)
    return parts + [x.astype(BF16)]


def tile_tables(tile, own_ref, col_ref, lst_ref, near_ref):
    rows = own_ref.shape[0]
    until = jnp.where(iota((128, 128), 0) <= iota((128, 128), 1), 1.0, 0.0).astype(BF16)
    before = jnp.where(iota((rows, rows), 1) < iota((rows, rows), 0), 1.0, 0.0).astype(BF16)
    number = (iota((rows, 128), 0) * 128 + iota((rows, 128), 1)).astype(F32)
    shade = col_ref[...].astype(F32)
    rank_at = iota((OWN, 128), 0).astype(F32)
    for tr in range(3):
        mine = own_ref[...] == (tile + tr - 1 + TILES) % TILES
        one = jnp.where(mine, 1.0, 0.0)
        inside = jnp.dot(one.astype(BF16), until, preferred_element_type=F32)
        above = jnp.dot(before, one.astype(BF16), preferred_element_type=F32)
        above = jnp.sum(above, axis=1, keepdims=True)
        rank = jnp.where(mine, inside + above - 1.0, -1.0)
        ids = jnp.zeros((OWN, 128), F32)
        cols = jnp.zeros((OWN, 128), F32)
        for i in range(rows):
            hit = rank[i : i + 1] == rank_at
            ids = ids + jnp.where(hit, number[i : i + 1], 0.0)
            cols = cols + jnp.where(hit, shade[i : i + 1], 0.0)
        for value, at in ((ids, 0), (cols, 128)):
            col = jnp.sum(value, axis=1, keepdims=True)
            row = as_row(col, 0) + as_row(col, OWN)
            near_ref[2 * tr : 2 * tr + 1, at : at + 128] = row
            near_ref[2 * tr + 1 : 2 * tr + 2, at : at + 128] = row
    near_ref[6:8, 128:256] = jnp.zeros((2, 128), F32)
    listed = lst_ref[...].astype(F32)
    near_ref[:, 256:384] = jnp.concatenate([listed] * BANDS, axis=1)
    for h in range(2):
        row = [listed[i : i + 1] for i in range(4 * h, 4 * h + 4)]
        near_ref[6 + h : 7 + h, 0:128] = jnp.concatenate(row, axis=1)


def star_means(m_ref, w_ref, mean_ref):
    for blk in range(BLOCKS):
        cols = slice(blk * ROWS, (blk + 1) * ROWS)
        top = jnp.sum(w_ref[:, cols] * m_ref[:, cols], axis=0, keepdims=True)
        mean_ref[blk : blk + 1, :] = top / jnp.sum(w_ref[:, cols], axis=0, keepdims=True)


def list_sums(m_ref, w_ref, s_ref, pred, aux_ref):
    entries = iota((LIST, ROWS), 0)
    rows = [jnp.zeros((1, 128), F32) for _ in range(4)]
    for blk in range(BLOCKS):
        cols = slice(blk * ROWS, (blk + 1) * ROWS)
        acc = jnp.zeros((LIST, ROWS), F32)
        wts = jnp.zeros((LIST, ROWS), F32)
        for k in range(OBS):
            hit = s_ref[k : k + 1, cols] == entries
            wk = w_ref[k : k + 1, cols]
            wts = wts + jnp.where(hit, wk, 0.0)
            acc = acc + jnp.where(hit, wk * (m_ref[k : k + 1, cols] - pred[blk : blk + 1]), 0.0)
        h, at = blk // 4, (blk % 4) * LIST
        rows[h] = rows[h] + as_row(jnp.sum(acc, axis=1, keepdims=True), at)
        rows[2 + h] = rows[2 + h] + as_row(jnp.sum(wts, axis=1, keepdims=True), at)
    aux_ref[...] = jnp.concatenate(rows + [jnp.zeros((4, 128), F32)], axis=0)


def solve_kernel(
    ct_hbm, m_hbm, w_hbm, s_hbm, own_hbm, col_hbm, lst_hbm,
    out_ref,
    ct_ref, m_ref, w_ref, s_ref, own_ref, col_ref, lst_ref,
    mean, mates, aux, near, bm, bw, bs, ba, bt, bn, u_ref, r_ref, mt_ref, pick2_ref,
    first_out, first_in, out_buf, in_buf, fin, got, row_buf, plane, line,
    load_sem, mate_send, mate_recv, ship_send, ship_recv, mag_send, mag_recv, tab_send, tab_recv, local,
    first_send, first_recv, send, recv,
    fin_send, fin_recv, plane_send, plane_recv, line_send, line_recv, go,
):
    sky = lax.axis_index("sky")
    band = lax.axis_index("band")
    home_sky, home_band = home_of(sky)
    stays = (home_sky == sky) & (home_band == band)
    moves = jnp.logical_not(stays)
    is_home, tile = tile_at(sky, band)
    places = [home_of((tile + d + TILES) % TILES) for d in (1, -1, 2, -2)]

    def owns(slot):
        return (tile == sky) & (band == slot)

    barrier = pltpu.get_barrier_semaphore()
    mates_of = [(band + i) % BANDS for i in range(1, BANDS)]
    for mate in mates_of:
        pl.semaphore_signal(barrier, inc=1, device_id=(sky, mate), device_id_type=MESH)

    @pl.when(moves)
    def _():
        pl.semaphore_signal(barrier, inc=1, device_id=(home_sky, home_band), device_id_type=MESH)

    @pl.when(is_home)
    def _():
        for place in places:
            pl.semaphore_signal(barrier, inc=1, device_id=place, device_id_type=MESH)
        for slot in range(BANDS):

            @pl.when(jnp.logical_not(owns(slot)))
            def _():
                pl.semaphore_signal(barrier, inc=1, device_id=(tile, slot), device_id_type=MESH)

    loads = [
        pltpu.make_async_copy(src, dst, load_sem.at[i])
        for i, (src, dst) in enumerate(
            (
                (own_hbm, own_ref), (col_hbm, col_ref), (lst_hbm, lst_ref),
                (m_hbm, m_ref), (w_hbm, w_ref), (s_hbm, s_ref), (ct_hbm, ct_ref),
            )
        )
    ]
    for load in loads:
        load.start()
    for load in loads[:3]:
        load.wait()
    tile_tables(sky, own_ref, col_ref, lst_ref, near)
    for load in loads[3:]:
        load.wait()
    star_means(m_ref, w_ref, mean)

    @pl.when(is_home & moves)
    def _():
        pl.semaphore_wait(barrier, 12)

    @pl.when(is_home & stays)
    def _():
        pl.semaphore_wait(barrier, 10)

    @pl.when(jnp.logical_not(is_home))
    def _():
        pl.semaphore_wait(barrier, 4)

    def chunk(ref, slot, c):
        at = pl.ds(CUTS[c] * ROWS, (CUTS[c + 1] - CUTS[c]) * ROWS)
        return ref.at[:, at] if slot is None else ref.at[slot, :, at]

    def ship_copy(i, slot, c):
        src, dst = ((w_ref, bw), (s_ref, bs))[i]
        return pltpu.make_async_remote_copy(
            src_ref=chunk(src, None, c),
            dst_ref=chunk(dst, slot, c),
            send_sem=ship_send.at[i, c],
            recv_sem=ship_recv.at[slot, i, c],
            device_id=(home_sky, home_band),
            device_id_type=MESH,
        )

    def mag_copy(slot):
        return pltpu.make_async_remote_copy(
            src_ref=m_ref,
            dst_ref=bm.at[slot],
            send_sem=mag_send,
            recv_sem=mag_recv.at[slot],
            device_id=(home_sky, home_band),
            device_id_type=MESH,
        )

    def mate_copy(i):
        return pltpu.make_async_remote_copy(
            src_ref=mean,
            dst_ref=mates.at[band],
            send_sem=mate_send.at[i],
            recv_sem=mate_recv.at[i],
            device_id=(sky, mates_of[i]),
            device_id_type=MESH,
        )

    def table_copy(i, slot):
        src, dst = ((mean, ba.at[slot]), (near, bn), (aux, bt.at[slot]))[i]
        return pltpu.make_async_remote_copy(
            src_ref=src,
            dst_ref=dst,
            send_sem=tab_send.at[i],
            recv_sem=tab_recv.at[slot, i],
            device_id=(home_sky, home_band),
            device_id_type=MESH,
        )

    teller = 0

    for i in range(BANDS - 1):
        mate_copy(i).start()
    keep = pltpu.make_async_copy(mean, mates.at[band], local.at[4])
    keep.start()

    @pl.when(moves)
    def _():
        @pl.when(band == teller)
        def _():
            table_copy(1, band).start()

        table_copy(0, band).start()
        for c in range(EARLY):
            for i in range(2):
                ship_copy(i, band, c).start()

    mix = []
    for b in range(BANDS):
        total = ct_ref[b, 0]
        for b2 in range(1, BANDS):
            total = total + ct_ref[b, b2]
        mix.append([ct_ref[b, b2] + (1.0 - total if b == b2 else 0.0) for b2 in range(BANDS)])

    keep.wait()
    for i in range(BANDS - 1):
        mate_copy(i).wait_recv()
    pred = jnp.zeros((BLOCKS, ROWS), F32)
    for b2 in range(BANDS):
        factor = mix[0][b2]
        for b in range(1, BANDS):
            factor = jnp.where(band == b, mix[b][b2], factor)
        pred = pred + factor * mates[b2]
    list_sums(m_ref, w_ref, s_ref, pred, aux)

    @pl.when(moves)
    def _():
        table_copy(2, band).start()
        for c in range(EARLY, CHUNKS):
            for i in range(2):
                ship_copy(i, band, c).start()

    @pl.when(stays)
    def _():
        copies = [
            pltpu.make_async_copy(mean, ba.at[band], local.at[0]),
            pltpu.make_async_copy(w_ref, bw.at[band], local.at[1]),
            pltpu.make_async_copy(s_ref, bs.at[band], local.at[2]),
            pltpu.make_async_copy(m_ref, bm.at[band], local.at[3]),
            pltpu.make_async_copy(aux, bt.at[band], local.at[4]),
        ]
        for copy in copies:
            copy.start()
        for copy in copies:
            copy.wait()

    for i in range(BANDS - 1):
        mate_copy(i).wait_send()

    def await_tables():
        table_copy(1, teller).wait_recv()
        for slot in range(BANDS):

            @pl.when(jnp.logical_not(owns(slot)))
            def _():
                table_copy(0, slot).wait_recv()

    def await_sums():
        for slot in range(BANDS):

            @pl.when(jnp.logical_not(owns(slot)))
            def _():
                table_copy(2, slot).wait_recv()

    def await_chunk(c):
        for slot in range(BANDS):

            @pl.when(jnp.logical_not(owns(slot)))
            def _():
                for i in range(2):
                    ship_copy(i, slot, c).wait_recv()

    def build():
        row_band = iota((128, 128), 0) // LIST
        lane_list = iota((128, 128), 1) // LIST
        lane_own = iota((128, 128), 1) // OWN
        mixes = jnp.zeros((128, 128), F32)
        for b2 in range(BANDS):
            for b in range(BANDS):
                mixes = jnp.where((row_band == b2) & (lane_list == b), mix[b][b2], mixes)
        entries = iota((LIST, ROWS), 0)
        await_tables()
        pick = []
        for tr in range(3):
            col = as_column(bn[2 * tr : 2 * tr + 1, 0:128], OWN)
            one = jnp.concatenate(
                [jnp.where(col == bn[6 + h : 7 + h, 0:128], 1.0, 0.0) for h in range(2)], axis=1
            ).astype(BF16)
            none = jnp.zeros((OWN, 256), BF16)
            pick2_ref[tr, 0:OWN, 0:256] = one
            pick2_ref[tr, OWN:128, 0:256] = none
            pick2_ref[tr, 0:OWN, 256:512] = none
            pick2_ref[tr, OWN:128, 256:512] = one
            pick.append(one)
        pick = jnp.concatenate(pick, axis=0)
        for blk in range(BLOCKS):
            if blk in CUTS:
                await_chunk(CUTS.index(blk))
            if blk == CUTS[-2]:
                for slot in range(BANDS):

                    @pl.when(jnp.logical_not(owns(slot)))
                    def _():
                        pl.semaphore_signal(go, inc=1, device_id=(tile, slot), device_id_type=MESH)

            cols = slice(blk * ROWS, (blk + 1) * ROWS)
            wide, scaled = [], []
            for b in range(BANDS):
                acc = jnp.zeros((LIST, ROWS), F32)
                for k in range(OBS):
                    wk = bw[b, k : k + 1, cols]
                    acc = acc + jnp.where(bs[b, k : k + 1, cols] == entries, wk, 0.0)
                star_w = jnp.sum(bw[b, :, cols], axis=0, keepdims=True)
                wide.append(acc)
                scaled.append(acc * (1.0 / star_w))
                u_ref[b, blk * LIST : (blk + 1) * LIST, :] = scaled[b]
            w_hi, w_lo = split(jnp.concatenate(wide, axis=0), 2)
            u_hi, u_lo = split(jnp.concatenate(scaled, axis=0), 2)
            dims = (((1,), (1,)), ((), ()))
            both = lax.dot_general(
                jnp.concatenate([u_hi, u_lo], axis=0), w_hi, dims, preferred_element_type=F32
            )
            gt = both[0:128] + both[128:256]
            gt = gt + lax.dot_general(u_hi, w_lo, dims, preferred_element_type=F32)
            lhs = jnp.concatenate(split(gt * mixes, 2), axis=0)
            col = as_column(bn[blk : blk + 1, 256:384], 128)
            for q in range(6):
                hit = (col == bn[q : q + 1, 0:128]) & (row_band == lane_own + 2 * (q % 2))
                moved = jnp.dot(
                    lhs, jnp.where(hit, 1.0, 0.0).astype(BF16), preferred_element_type=F32
                ).astype(BF16)
                for i in range(2):
                    for b2 in range(BANDS):
                        at = i * 128 + b2 * LIST
                        r_ref[
                            i, b2, blk * LIST : (blk + 1) * LIST, q * 128 : (q + 1) * 128
                        ] = moved[at : at + LIST]
            if blk == CUTS[EARLY] - 1:
                await_sums()
                first_sums(pick)
            if blk in (3, 7):
                at = slice((blk - 3) * LIST, (blk + 1) * LIST)
                for b2 in range(BANDS):
                    total = jnp.dot(pick[:, at], r_ref[0, b2, at, :], preferred_element_type=F32)
                    total = total + jnp.dot(pick[:, at], r_ref[1, b2, at, :], preferred_element_type=F32)
                    rows = slice(b2 * NEAR, (b2 + 1) * NEAR)
                    mt_ref[rows, :] = total if blk == 3 else mt_ref[rows, :] + total

    def first_sums(pick):
        rows = [jnp.concatenate([bt[b, h : h + 1, :] for h in range(2)], axis=1) for b in range(BANDS)]
        rows += [jnp.concatenate([bt[b, h : h + 1, :] for h in (2, 3)], axis=1) for b in range(BANDS)]
        terms = jnp.concatenate(split(jnp.concatenate(rows, axis=0), 3), axis=0)
        sums = lax.dot_general(terms, pick, (((1,), (1,)), ((), ())), preferred_element_type=F32)
        sums = sums[0:8] + sums[8:16] + sums[16:24]
        for i in range(2):
            for q in range(6):
                tr, b = q // 2, 2 * (q % 2)
                at = slice(tr * OWN, (tr + 1) * OWN)
                low, high = i * BANDS + b, i * BANDS + b + 1
                first_out[i, q] = jnp.concatenate(
                    [sums[low : low + 1, at], sums[high : high + 1, at]], axis=1
                )
        for i in range(2):
            for slot in (2, 3, 0, 1):
                first_copy(slot, i).start()
    def first_copy(slot, i):
        return pltpu.make_async_remote_copy(
            src_ref=first_out.at[i],
            dst_ref=first_in.at[i, slot],
            send_sem=first_send.at[i, slot],
            recv_sem=first_recv.at[i, slot],
            device_id=places[slot],
            device_id_type=MESH,
        )

    part_of = (pl.ds(2, 4), pl.ds(0, 4), pl.ds(4, 2), pl.ds(0, 2))

    def step_copy(slot, p):
        return pltpu.make_async_remote_copy(
            src_ref=out_buf.at[p, part_of[slot]],
            dst_ref=in_buf.at[p, slot, part_of[slot]],
            send_sem=send.at[p, slot],
            recv_sem=recv.at[p, slot],
            device_id=places[slot],
            device_id_type=MESH,
        )

    below, above, far_below, far_above = range(4)

    def combine_mid(own, got):
        return [own[q] + got(below, q + 2) + got(above, q - 2) for q in (2, 3)]

    def combine_rest(own, got):
        low = [own[q] + got(below, q + 2) + got(far_below, q + 4) for q in (0, 1)]
        top = [own[q] + got(above, q - 2) + got(far_above, q - 4) for q in (4, 5)]
        return low, top

    def columns(row):
        eye = iota((128, 128), 0) == iota((128, 128), 1)
        full = jnp.where(eye, jnp.broadcast_to(row, (128, 128)), 0.0)
        return jnp.sum(full, axis=1, keepdims=True)

    def pull(accs, pieces, cols):
        for r, col in cols.items():
            for half in range(2):
                b = (r % 2) * 2 + half
                base = b * NEAR + (r // 2) * OWN
                for i in range(0, OWN, 8):
                    at = half * OWN + i
                    c = col[at : at + 8, :]
                    for j, q in enumerate(pieces):
                        accs[j] = accs[j] + mt_ref[base + i : base + i + 8, q * 128 : (q + 1) * 128] * c
        return accs

    outer, inner = (0, 1, 4, 5), (2, 3)

    def evaluate(n, z, last):
        total = jnp.zeros((8, 512), F32)
        for tr in range(3):
            pair = jnp.concatenate([z[2 * tr], z[2 * tr + 1]], axis=0)
            lhs = jnp.concatenate(split(pair, 3) + [jnp.zeros((2, 128), BF16)], axis=0)
            total = total + jnp.dot(lhs, pick2_ref[tr], preferred_element_type=F32)
        total = total[0:2] + total[2:4] + total[4:6]
        means, tables = [], []
        for b in range(BANDS):
            rows = []
            tables.append([])
            for h in range(2):
                at = (b % 2) * 256 + h * 128
                row = total[b // 2 : b // 2 + 1, at : at + 128]
                tables[b].append(jnp.broadcast_to(row, (8, 128)))
                col = columns(row)
                for i in range(4):
                    blk = h * 4 + i
                    value = u_ref[b, blk * LIST : (blk + 1) * LIST, :] * col[i * LIST : (i + 1) * LIST, :]
                    rows.append(jnp.sum(value, axis=0, keepdims=True))
            means.append(ba[b] - jnp.concatenate(rows, axis=0))
        if last:
            for b in range(BANDS):
                fin[b, :, 0:ROWS] = means[b]
                fin[b, 0:1, 256:384] = z[2 + b // 2]
                fin[b, 1:8, 256:384] = jnp.zeros((7, 128), F32)
            for slot in range(BANDS):

                @pl.when(jnp.logical_not(owns(slot)))
                def _():
                    fin_copy(slot).start()

        lane = iota((1, 128), 1)
        found = jnp.zeros((1, 128), F32)
        for b in range(BANDS):
            pred = mix[b][0] * means[0]
            for b2 in range(1, BANDS):
                pred = pred + mix[b][b2] * means[b2]
            acc = jnp.zeros((8, 128), F32)
            for blk in range(BLOCKS):
                for half in range(2):
                    at = blk * ROWS + half * 128
                    idx = bs[b, :, at : at + 128] + (blk % 4) * LIST
                    picked = jnp.take_along_axis(tables[b][blk // 4], idx, axis=1)
                    left = bm[b, :, at : at + 128] - pred[blk : blk + 1, half * 128 : half * 128 + 128]
                    left = left - picked
                    acc = acc + bw[b, :, at : at + 128] * left * left
            value = jnp.sum(jnp.sum(acc, axis=0, keepdims=True), axis=1, keepdims=True)
            found = jnp.where(lane == n + b * SWEEPS, value, found)
        row_buf[0] = row_buf[0] + found

    def fin_copy(slot):
        return pltpu.make_async_remote_copy(
            src_ref=fin.at[slot],
            dst_ref=got,
            send_sem=fin_send.at[slot],
            recv_sem=fin_recv,
            device_id=(tile, slot),
            device_id_type=MESH,
        )

    x = (sky // 32) * 2 + band // 2
    y = (sky // 8) % 4
    z_at = sky % 8

    def core_at(dx, dy, dz, core):
        x_to, y_to, z_to = (x + dx) % 4, (y + dy) % 4, (z_at + dz) % 8
        return (x_to // 2) * 32 + y_to * 8 + z_to, (x_to % 2) * 2 + core

    def plane_copy(i):
        return pltpu.make_async_remote_copy(
            src_ref=row_buf.at[0],
            dst_ref=plane.at[x * 4 + y],
            send_sem=plane_send.at[i],
            recv_sem=plane_recv,
            device_id=core_at(PLANE[i][0], PLANE[i][1], 0, 1),
            device_id_type=MESH,
        )

    def line_copy(i):
        return pltpu.make_async_remote_copy(
            src_ref=row_buf.at[1],
            dst_ref=line.at[z_at % 4],
            send_sem=line_send.at[i],
            recv_sem=line_recv,
            device_id=core_at(0, 0, LINE[i][0], LINE[i][1]),
            device_id_type=MESH,
        )

    def whole(ref, sem):
        return pltpu.make_async_copy(ref, ref, sem)

    @pl.when(is_home)
    def _():
        build()
        for i in range(2):
            for slot in range(4):
                first_copy(slot, i).wait()
        start = []
        for i in range(2):
            own = [first_out[i, q] for q in range(6)]
            low, top = combine_rest(own, lambda s, q: first_in[i, s, q])
            start.append(low + combine_mid(own, lambda s, q: first_in[i, s, q]) + top)
        known, dens = start
        scale = [1.0 / (d + PRIOR_WEIGHT) for d in dens]
        colors = [bn[q : q + 1, 128:256] for q in range(6)]
        zero = jnp.zeros((1, 128), F32)
        z = [jnp.where(colors[q] == 0.0, known[q] * scale[q], zero) for q in range(6)]
        cols = {q: columns(z[q]) for q in range(6)}
        accs = pull([jnp.zeros((8, 128), F32) for _ in range(6)], range(6), cols)
        for q in range(6):
            out_buf[1, q] = jnp.sum(accs[q], axis=0, keepdims=True)
        for slot in (2, 3, 0, 1):
            step_copy(slot, 1).start()
        row_buf[0] = zero

        def renew(q, color, pulled, old):
            return jnp.where(colors[q] == color, (known[q] + pulled) * scale[q], old)

        def absorb(s, z, then):
            p = s % 2
            color = (s % COLORS).astype(F32) if not isinstance(s, int) else float(s % COLORS)
            own = [out_buf[p, q] for q in range(6)]
            take = lambda i, q: in_buf[p, i, q]
            z = list(z)
            for slot in (0, 1):
                step_copy(slot, p).wait_recv()
            mid = combine_mid(own, take)
            for q in inner:
                z[q] = renew(q, color, mid[q - 2], z[q])
            accs = None
            if then:
                cols = {q: columns(z[q]) for q in inner}
                accs = pull([jnp.zeros((8, 128), F32) for _ in range(6)], range(6), cols)
            for slot in (2, 3):
                step_copy(slot, p).wait_recv()
            low, top = combine_rest(own, take)
            for j, q in enumerate(outer):
                z[q] = renew(q, color, (low + top)[j], z[q])
            return z, accs

        def step(s, z):
            p = s % 2

            @pl.when((s == 2) & moves)
            def _():
                pl.semaphore_wait(go, 1)
                mag_copy(band).start()

            @pl.when(s % COLORS == 0)
            def _():
                @pl.when(s == COLORS)
                def _():
                    for slot in range(BANDS):

                        @pl.when(jnp.logical_not(owns(slot)))
                        def _():
                            mag_copy(slot).wait_recv()

                evaluate(s // COLORS - 1, z, False)

            z, accs = absorb(s, z, True)
            cols = {q: columns(z[q]) for q in outer}
            far = pull([accs[q] for q in outer], outer, cols)
            for j, q in enumerate(outer):
                out_buf[1 - p, q] = jnp.sum(far[j], axis=0, keepdims=True)
            for slot in (2, 3):
                step_copy(slot, 1 - p).start()
            near_accs = pull([accs[q] for q in inner], inner, cols)
            for j, q in enumerate(inner):
                out_buf[1 - p, q] = jnp.sum(near_accs[j], axis=0, keepdims=True)
            for slot in (0, 1):
                step_copy(slot, 1 - p).start()
            for slot in range(4):
                step_copy(slot, p).wait_send()
            return tuple(z)

        z = lax.fori_loop(1, STEPS - 1, step, tuple(z))
        z, _ = absorb(STEPS - 1, z, False)
        evaluate(SWEEPS - 1, z, True)
        for i in range(len(PLANE)):
            plane_copy(i).start()
        mine = pltpu.make_async_copy(row_buf.at[0], plane.at[x * 4 + y], plane_recv)
        mine.start()
        whole(plane, plane_recv).wait()
        row_buf[1] = jnp.sum(plane[...].reshape(16, 128), axis=0, keepdims=True)
        for i in range(len(LINE)):
            line_copy(i).start()
        mine = pltpu.make_async_copy(row_buf.at[1], line.at[z_at % 4], line_recv)
        mine.start()
        for i in range(len(PLANE)):
            plane_copy(i).wait_send()
        for slot in range(4):
            step_copy(slot, (STEPS - 1) % 2).wait_send()

    @pl.when(jnp.logical_not(is_home))
    def _():
        pl.semaphore_wait(go, 1)
        mag_copy(band).start()

    @pl.when(moves)
    def _():
        @pl.when(band == teller)
        def _():
            table_copy(1, band).wait_send()

        table_copy(0, band).wait_send()
        table_copy(2, band).wait_send()
        for c in range(CHUNKS):
            for i in range(2):
                ship_copy(i, band, c).wait_send()
        mag_copy(band).wait_send()
        fin_copy(0).wait_recv()

    @pl.when(stays)
    def _():
        mine = pltpu.make_async_copy(fin.at[band], got, local.at[0])
        mine.start()
        mine.wait()

    out_ref[:, 0:256] = got[:, 0:256]
    pair = got[0:1, 256:384]
    out_ref[:, 256:512] = jnp.zeros((8, 256), F32)
    out_ref[0:1, 256:384] = jnp.where(band % 2 == 0, pair, pltpu.roll(pair, OWN, 1))

    whole(line, line_recv).wait()
    total = jnp.sum(line[...].reshape(4, 128), axis=0, keepdims=True)
    total = pltpu.roll(total, (128 - band * SWEEPS) % 128, 1)
    out_ref[0:1, 384:512] = total * (1.0 / (OBS * STARS * TILES))

    @pl.when(is_home)
    def _():
        for slot in range(BANDS):

            @pl.when(jnp.logical_not(owns(slot)))
            def _():
                fin_copy(slot).wait_send()

        for i in range(len(LINE)):
            line_copy(i).wait_send()


def solve(color_terms, m, w, s, owner, colors, lists):
    vmem = pl.BlockSpec(memory_space=pltpu.VMEM)
    hbm = pl.BlockSpec(memory_space=pl.ANY)
    dma = pltpu.SemaphoreType.DMA
    return pl.pallas_call(
        solve_kernel,
        out_shape=pltpu.VMEM((8, 512), F32),
        in_specs=[hbm] * 7,
        out_specs=vmem,
        scratch_shapes=[
            pltpu.SMEM(color_terms.shape, F32),
            pltpu.VMEM((OBS, STARS), F32),
            pltpu.VMEM((OBS, STARS), F32),
            pltpu.VMEM((OBS, STARS), jnp.int32),
            pltpu.VMEM(owner.shape, jnp.int32),
            pltpu.VMEM(colors.shape, jnp.int32),
            pltpu.VMEM(lists.shape, jnp.int32),
            pltpu.VMEM((BLOCKS, ROWS), F32),
            pltpu.VMEM((BANDS, BLOCKS, ROWS), F32),
            pltpu.VMEM((8, 128), F32),
            pltpu.VMEM((8, 384), F32),
            pltpu.VMEM((BANDS, OBS, STARS), F32),
            pltpu.VMEM((BANDS, OBS, STARS), F32),
            pltpu.VMEM((BANDS, OBS, STARS), jnp.int32),
            pltpu.VMEM((BANDS, BLOCKS, ROWS), F32),
            pltpu.VMEM((BANDS, 8, 128), F32),
            pltpu.VMEM((8, 384), F32),
            pltpu.VMEM((BANDS, BLOCKS * LIST, ROWS), F32),
            pltpu.VMEM((2, BANDS, BLOCKS * LIST, WIDE), BF16),
            pltpu.VMEM((WIDE, WIDE), F32),
            pltpu.VMEM((3, 128, 512), BF16),
            pltpu.VMEM((2, 6, 1, 128), F32),
            pltpu.VMEM((2, 4, 6, 1, 128), F32),
            pltpu.VMEM((2, 6, 1, 128), F32),
            pltpu.VMEM((2, 4, 6, 1, 128), F32),
            pltpu.VMEM((BANDS, 8, 384), F32),
            pltpu.VMEM((8, 384), F32),
            pltpu.VMEM((2, 1, 128), F32),
            pltpu.VMEM((16, 1, 128), F32),
            pltpu.VMEM((4, 1, 128), F32),
            dma((7,)),
            dma((BANDS - 1,)),
            dma((BANDS - 1,)),
            dma((2, CHUNKS)),
            dma((BANDS, 2, CHUNKS)),
            dma,
            dma((BANDS,)),
            dma((3,)),
            dma((BANDS, 3)),
            dma((5,)),
            dma((2, 4)),
            dma((2, 4)),
            dma((2, 4)),
            dma((2, 4)),
            dma((BANDS,)),
            dma,
            dma((len(PLANE),)),
            dma,
            dma((len(LINE),)),
            dma,
            pltpu.SemaphoreType.REGULAR,
        ],
        compiler_params=pltpu.CompilerParams(has_side_effects=True, collective_id=0),
        name="solve",
    )(color_terms, m, w, s, owner, colors, lists)


def unpack_kernel(out_ref, zp_ref, mags_ref, mis_ref):
    zp_ref[...] = out_ref[0:1, 256 : 256 + OWN]
    mis_ref[...] = out_ref[0:1, 384 : 384 + SWEEPS]
    for blk in range(BLOCKS):
        mags_ref[0:1, blk * ROWS : (blk + 1) * ROWS] = out_ref[blk : blk + 1, 0:ROWS]


def body(magnitudes, weights, slots, block_fields, owner, colors, color_terms):
    out = solve(
        color_terms, magnitudes[0], weights[0], slots[0],
        owner.reshape(-1, 128), colors.reshape(-1, 128), block_fields,
    )
    vmem = pl.BlockSpec(memory_space=pltpu.VMEM)
    out = pltpu.with_memory_space_constraint(out, pltpu.VMEM)
    zp, mags, misfit = pl.pallas_call(
        unpack_kernel,
        out_shape=(
            jax.ShapeDtypeStruct((1, OWN), F32),
            jax.ShapeDtypeStruct((1, STARS), F32),
            jax.ShapeDtypeStruct((1, SWEEPS), F32),
        ),
        in_specs=[vmem],
        out_specs=(vmem,) * 3,
        name="unpack",
    )(out)
    return zp, mags, misfit.T


def solution(mesh):
    in_specs = (
        P("band", None, "sky"),
        P("band", None, "sky"),
        P("band", None, "sky"),
        P("sky", None),
        P(),
        P(),
        P(),
    )
    out_specs = (P("band", "sky"), P("band", "sky"), P(None, "band"))
    return jax.shard_map(body, mesh=mesh, in_specs=in_specs, out_specs=out_specs, check_vma=False)
```

```python
import functools

import jax
import jax.numpy as jnp
from jax import lax
from jax.experimental import pallas as pl
from jax.experimental.pallas import tpu as pltpu
from jax.sharding import PartitionSpec as P

COLORS = 8
SWEEPS = 4
PRIOR_WEIGHT = 1.0

TILES = 64
BANDS = 4
OBS = 8
BLOCKS = 8
ROWS = 256
STARS = BLOCKS * ROWS
LIST = 32
OWN = 64
NEAR = 3 * OWN
CUTS = (0, 2, 4, 6, 7, 8)
CHUNKS = len(CUTS) - 1
EARLY = 2
WIDE = BANDS * NEAR
STEPS = COLORS * SWEEPS
PLANE = [(i, j) for i in (2, 1, 3, 0) for j in (2, 1, 3, 0)][:-1]
LINE = [(k, c) for k in (4, 3, 5, 2, 6, 1, 7, 0) for c in (0, 1)][:-1]
MESH = pl.DeviceIdType.MESH
HIGH = lax.Precision.HIGHEST
F32 = jnp.float32
BF16 = jnp.bfloat16


def home_of(tile):
    half = tile // 32
    row = tile // 8
    y = row % 4
    z = tile % 8
    leg = z // 4
    y_new = y + half * (3 - 2 * y)
    z_new = z + leg * (7 - 2 * z)
    x_lo = (1 - half + row + leg) % 2
    return half * 32 + y_new * 8 + z_new, x_lo * 2 + 1


def tile_at(sky, band):
    half = sky // 32
    y_new = (sky // 8) % 4
    z_new = sky % 8
    y = y_new + half * (3 - 2 * y_new)
    row = half * 4 + y
    leg = (band // 2 + 1 + half + row) % 2
    z = z_new + leg * (7 - 2 * z_new)
    is_home = (band % 2 == 1) & (z_new < 4)
    return is_home, (row * 8 + z) % TILES


def iota(shape, dim):
    return lax.broadcasted_iota(jnp.int32, shape, dim)


def as_column(row, count):
    eye = iota((count, 128), 0) == iota((count, 128), 1)
    full = jnp.broadcast_to(row, (count, 128))
    return jnp.sum(jnp.where(eye, full, 0.0), axis=1, keepdims=True)


def as_row(col, shift):
    n = col.shape[0]
    hit = iota((n, 128), 1) == iota((n, 128), 0) + shift
    return jnp.sum(jnp.where(hit, col, 0.0), axis=0, keepdims=True)


def split(x, terms):
    parts = []
    for _ in range(terms - 1):
        part = x.astype(BF16)
        parts.append(part)
        x = x - part.astype(F32)
    return parts + [x.astype(BF16)]


def tile_tables(tile, own_ref, col_ref, lst_ref, near_ref):
    rows = own_ref.shape[0]
    until = jnp.where(iota((128, 128), 0) <= iota((128, 128), 1), 1.0, 0.0).astype(BF16)
    before = jnp.where(iota((rows, rows), 1) < iota((rows, rows), 0), 1.0, 0.0).astype(BF16)
    number = (iota((rows, 128), 0) * 128 + iota((rows, 128), 1)).astype(F32)
    shade = col_ref[...].astype(F32)
    rank_at = iota((OWN, 128), 0).astype(F32)
    for tr in range(3):
        mine = own_ref[...] == (tile + tr - 1 + TILES) % TILES
        one = jnp.where(mine, 1.0, 0.0)
        inside = jnp.dot(one.astype(BF16), until, preferred_element_type=F32)
        above = jnp.dot(before, one.astype(BF16), preferred_element_type=F32)
        above = jnp.sum(above, axis=1, keepdims=True)
        rank = jnp.where(mine, inside + above - 1.0, -1.0)
        ids = jnp.zeros((OWN, 128), F32)
        cols = jnp.zeros((OWN, 128), F32)
        for i in range(rows):
            hit = rank[i : i + 1] == rank_at
            ids = ids + jnp.where(hit, number[i : i + 1], 0.0)
            cols = cols + jnp.where(hit, shade[i : i + 1], 0.0)
        for value, at in ((ids, 0), (cols, 128)):
            col = jnp.sum(value, axis=1, keepdims=True)
            row = as_row(col, 0) + as_row(col, OWN)
            near_ref[2 * tr : 2 * tr + 1, at : at + 128] = row
            near_ref[2 * tr + 1 : 2 * tr + 2, at : at + 128] = row
    near_ref[6:8, 128:256] = jnp.zeros((2, 128), F32)
    listed = lst_ref[...].astype(F32)
    near_ref[:, 256:384] = jnp.concatenate([listed] * BANDS, axis=1)
    for h in range(2):
        row = [listed[i : i + 1] for i in range(4 * h, 4 * h + 4)]
        near_ref[6 + h : 7 + h, 0:128] = jnp.concatenate(row, axis=1)


def star_means(m_ref, w_ref, mean_ref):
    for blk in range(BLOCKS):
        cols = slice(blk * ROWS, (blk + 1) * ROWS)
        top = jnp.sum(w_ref[:, cols] * m_ref[:, cols], axis=0, keepdims=True)
        mean_ref[blk : blk + 1, :] = top / jnp.sum(w_ref[:, cols], axis=0, keepdims=True)


def list_sums(m_ref, w_ref, s_ref, pred, aux_ref):
    entries = iota((LIST, ROWS), 0)
    rows = [jnp.zeros((1, 128), F32) for _ in range(4)]
    for blk in range(BLOCKS):
        cols = slice(blk * ROWS, (blk + 1) * ROWS)
        acc = jnp.zeros((LIST, ROWS), F32)
        wts = jnp.zeros((LIST, ROWS), F32)
        for k in range(OBS):
            hit = s_ref[k : k + 1, cols] == entries
            wk = w_ref[k : k + 1, cols]
            wts = wts + jnp.where(hit, wk, 0.0)
            acc = acc + jnp.where(hit, wk * (m_ref[k : k + 1, cols] - pred[blk : blk + 1]), 0.0)
        h, at = blk // 4, (blk % 4) * LIST
        rows[h] = rows[h] + as_row(jnp.sum(acc, axis=1, keepdims=True), at)
        rows[2 + h] = rows[2 + h] + as_row(jnp.sum(wts, axis=1, keepdims=True), at)
    aux_ref[...] = jnp.concatenate(rows + [jnp.zeros((4, 128), F32)], axis=0)


def solve_kernel(
    ct_hbm, m_hbm, w_hbm, s_hbm, own_hbm, col_hbm, lst_hbm,
    out_ref,
    ct_ref, m_ref, w_ref, s_ref, own_ref, col_ref, lst_ref,
    mean, mates, aux, near, bm, bw, bs, ba, bt, bn, u_ref, r_ref, mt_ref, pick2_ref,
    first_out, first_in, out_buf, in_buf, fin, got, row_buf, plane, line,
    load_sem, mate_send, mate_recv, ship_send, ship_recv, mag_send, mag_recv, tab_send, tab_recv, local,
    first_send, first_recv, send, recv,
    fin_send, fin_recv, plane_send, plane_recv, line_send, line_recv, go,
):
    sky = lax.axis_index("sky")
    band = lax.axis_index("band")
    home_sky, home_band = home_of(sky)
    stays = (home_sky == sky) & (home_band == band)
    moves = jnp.logical_not(stays)
    is_home, tile = tile_at(sky, band)
    places = [home_of((tile + d + TILES) % TILES) for d in (1, -1, 2, -2)]

    def owns(slot):
        return (tile == sky) & (band == slot)

    barrier = pltpu.get_barrier_semaphore()
    mates_of = [(band + i) % BANDS for i in range(1, BANDS)]
    for mate in mates_of:
        pl.semaphore_signal(barrier, inc=1, device_id=(sky, mate), device_id_type=MESH)

    @pl.when(moves)
    def _():
        pl.semaphore_signal(barrier, inc=1, device_id=(home_sky, home_band), device_id_type=MESH)

    @pl.when(is_home)
    def _():
        for place in places:
            pl.semaphore_signal(barrier, inc=1, device_id=place, device_id_type=MESH)
        for slot in range(BANDS):

            @pl.when(jnp.logical_not(owns(slot)))
            def _():
                pl.semaphore_signal(barrier, inc=1, device_id=(tile, slot), device_id_type=MESH)

    loads = [
        pltpu.make_async_copy(src, dst, load_sem.at[i])
        for i, (src, dst) in enumerate(
            (
                (w_hbm, w_ref), (s_hbm, s_ref), (m_hbm, m_ref),
                (own_hbm, own_ref), (col_hbm, col_ref), (lst_hbm, lst_ref), (ct_hbm, ct_ref),
            )
        )
    ]
    for load in loads:
        load.start()
    for load in loads[:3]:
        load.wait()
    star_means(m_ref, w_ref, mean)

    @pl.when(is_home & moves)
    def _():
        pl.semaphore_wait(barrier, 12)

    @pl.when(is_home & stays)
    def _():
        pl.semaphore_wait(barrier, 10)

    @pl.when(jnp.logical_not(is_home))
    def _():
        pl.semaphore_wait(barrier, 4)

    def chunk(ref, slot, c):
        at = pl.ds(CUTS[c] * ROWS, (CUTS[c + 1] - CUTS[c]) * ROWS)
        return ref.at[:, at] if slot is None else ref.at[slot, :, at]

    def ship_copy(i, slot, c):
        src, dst = ((w_ref, bw), (s_ref, bs))[i]
        return pltpu.make_async_remote_copy(
            src_ref=chunk(src, None, c),
            dst_ref=chunk(dst, slot, c),
            send_sem=ship_send.at[i, c],
            recv_sem=ship_recv.at[slot, i, c],
            device_id=(home_sky, home_band),
            device_id_type=MESH,
        )

    def mag_copy(slot):
        return pltpu.make_async_remote_copy(
            src_ref=m_ref,
            dst_ref=bm.at[slot],
            send_sem=mag_send,
            recv_sem=mag_recv.at[slot],
            device_id=(home_sky, home_band),
            device_id_type=MESH,
        )

    def mate_copy(i):
        return pltpu.make_async_remote_copy(
            src_ref=mean,
            dst_ref=mates.at[band],
            send_sem=mate_send.at[i],
            recv_sem=mate_recv.at[i],
            device_id=(sky, mates_of[i]),
            device_id_type=MESH,
        )

    def table_copy(i, slot):
        src, dst = ((mean, ba.at[slot]), (near, bn), (aux, bt.at[slot]))[i]
        return pltpu.make_async_remote_copy(
            src_ref=src,
            dst_ref=dst,
            send_sem=tab_send.at[i],
            recv_sem=tab_recv.at[slot, i],
            device_id=(home_sky, home_band),
            device_id_type=MESH,
        )

    teller = 0

    for i in range(BANDS - 1):
        mate_copy(i).start()
    keep = pltpu.make_async_copy(mean, mates.at[band], local.at[4])
    keep.start()

    @pl.when(moves)
    def _():
        for i in range(2):
            ship_copy(i, band, 0).start()

    for load in loads[3:]:
        load.wait()
    tile_tables(sky, own_ref, col_ref, lst_ref, near)

    @pl.when(moves)
    def _():
        @pl.when(band == teller)
        def _():
            table_copy(1, band).start()

        for c in range(1, EARLY):
            for i in range(2):
                ship_copy(i, band, c).start()

    mix = []
    for b in range(BANDS):
        total = ct_ref[b, 0]
        for b2 in range(1, BANDS):
            total = total + ct_ref[b, b2]
        mix.append([ct_ref[b, b2] + (1.0 - total if b == b2 else 0.0) for b2 in range(BANDS)])

    keep.wait()
    for i in range(BANDS - 1):
        mate_copy(i).wait_recv()
    pred = jnp.zeros((BLOCKS, ROWS), F32)
    for b2 in range(BANDS):
        factor = mix[0][b2]
        for b in range(1, BANDS):
            factor = jnp.where(band == b, mix[b][b2], factor)
        pred = pred + factor * mates[b2]
    list_sums(m_ref, w_ref, s_ref, pred, aux)

    @pl.when(moves)
    def _():
        table_copy(2, band).start()
        for c in range(EARLY, CHUNKS):
            for i in range(2):
                ship_copy(i, band, c).start()
        table_copy(0, band).start()

    @pl.when(stays)
    def _():
        copies = [
            pltpu.make_async_copy(mean, ba.at[band], local.at[0]),
            pltpu.make_async_copy(w_ref, bw.at[band], local.at[1]),
            pltpu.make_async_copy(s_ref, bs.at[band], local.at[2]),
            pltpu.make_async_copy(m_ref, bm.at[band], local.at[3]),
            pltpu.make_async_copy(aux, bt.at[band], local.at[4]),
        ]
        for copy in copies:
            copy.start()
        for copy in copies:
            copy.wait()

    for i in range(BANDS - 1):
        mate_copy(i).wait_send()

    def await_tables():
        table_copy(1, teller).wait_recv()

    def await_sums():
        for slot in range(BANDS):

            @pl.when(jnp.logical_not(owns(slot)))
            def _():
                table_copy(2, slot).wait_recv()

    def await_chunk(c):
        for slot in range(BANDS):

            @pl.when(jnp.logical_not(owns(slot)))
            def _():
                for i in range(2):
                    ship_copy(i, slot, c).wait_recv()

    def build():
        row_band = iota((128, 128), 0) // LIST
        lane_list = iota((128, 128), 1) // LIST
        lane_own = iota((128, 128), 1) // OWN
        mixes = jnp.zeros((128, 128), F32)
        for b2 in range(BANDS):
            for b in range(BANDS):
                mixes = jnp.where((row_band == b2) & (lane_list == b), mix[b][b2], mixes)
        entries = iota((LIST, ROWS), 0)
        await_tables()
        pick = []
        for tr in range(3):
            col = as_column(bn[2 * tr : 2 * tr + 1, 0:128], OWN)
            one = jnp.concatenate(
                [jnp.where(col == bn[6 + h : 7 + h, 0:128], 1.0, 0.0) for h in range(2)], axis=1
            ).astype(BF16)
            none = jnp.zeros((OWN, 256), BF16)
            pick2_ref[tr, 0:OWN, 0:256] = one
            pick2_ref[tr, OWN:128, 0:256] = none
            pick2_ref[tr, 0:OWN, 256:512] = none
            pick2_ref[tr, OWN:128, 256:512] = one
            pick.append(one)
        pick = jnp.concatenate(pick, axis=0)
        for blk in range(BLOCKS):
            if blk in CUTS:
                await_chunk(CUTS.index(blk))
            if blk == CUTS[-2]:
                for slot in range(BANDS):

                    @pl.when(jnp.logical_not(owns(slot)))
                    def _():
                        pl.semaphore_signal(go, inc=1, device_id=(tile, slot), device_id_type=MESH)

            cols = slice(blk * ROWS, (blk + 1) * ROWS)
            wide, scaled = [], []
            for b in range(BANDS):
                acc = jnp.zeros((LIST, ROWS), F32)
                for k in range(OBS):
                    wk = bw[b, k : k + 1, cols]
                    acc = acc + jnp.where(bs[b, k : k + 1, cols] == entries, wk, 0.0)
                star_w = jnp.sum(bw[b, :, cols], axis=0, keepdims=True)
                wide.append(acc)
                scaled.append(acc * (1.0 / star_w))
                u_ref[b, blk * LIST : (blk + 1) * LIST, :] = scaled[b]
            w_hi, w_lo = split(jnp.concatenate(wide, axis=0), 2)
            u_hi, u_lo = split(jnp.concatenate(scaled, axis=0), 2)
            dims = (((1,), (1,)), ((), ()))
            both = lax.dot_general(
                jnp.concatenate([u_hi, u_lo], axis=0), w_hi, dims, preferred_element_type=F32
            )
            gt = both[0:128] + both[128:256]
            gt = gt + lax.dot_general(u_hi, w_lo, dims, preferred_element_type=F32)
            lhs = jnp.concatenate(split(gt * mixes, 2), axis=0)
            col = as_column(bn[blk : blk + 1, 256:384], 128)
            for q in range(6):
                hit = (col == bn[q : q + 1, 0:128]) & (row_band == lane_own + 2 * (q % 2))
                moved = jnp.dot(
                    lhs, jnp.where(hit, 1.0, 0.0).astype(BF16), preferred_element_type=F32
                ).astype(BF16)
                for i in range(2):
                    for b2 in range(BANDS):
                        at = i * 128 + b2 * LIST
                        r_ref[
                            i, b2, blk * LIST : (blk + 1) * LIST, q * 128 : (q + 1) * 128
                        ] = moved[at : at + LIST]
            if blk == CUTS[EARLY] - 1:
                await_sums()
                first_sums(pick)
            if blk in (3, 7):
                at = slice((blk - 3) * LIST, (blk + 1) * LIST)
                for b2 in range(BANDS):
                    total = jnp.dot(pick[:, at], r_ref[0, b2, at, :], preferred_element_type=F32)
                    total = total + jnp.dot(pick[:, at], r_ref[1, b2, at, :], preferred_element_type=F32)
                    rows = slice(b2 * NEAR, (b2 + 1) * NEAR)
                    mt_ref[rows, :] = total if blk == 3 else mt_ref[rows, :] + total

    def first_sums(pick):
        rows = [jnp.concatenate([bt[b, h : h + 1, :] for h in range(2)], axis=1) for b in range(BANDS)]
        rows += [jnp.concatenate([bt[b, h : h + 1, :] for h in (2, 3)], axis=1) for b in range(BANDS)]
        terms = jnp.concatenate(split(jnp.concatenate(rows, axis=0), 3), axis=0)
        sums = lax.dot_general(terms, pick, (((1,), (1,)), ((), ())), preferred_element_type=F32)
        sums = sums[0:8] + sums[8:16] + sums[16:24]
        for i in range(2):
            for q in range(6):
                tr, b = q // 2, 2 * (q % 2)
                at = slice(tr * OWN, (tr + 1) * OWN)
                low, high = i * BANDS + b, i * BANDS + b + 1
                first_out[i, q] = jnp.concatenate(
                    [sums[low : low + 1, at], sums[high : high + 1, at]], axis=1
                )
        for i in range(2):
            for slot in (2, 3, 0, 1):
                first_copy(slot, i).start()
    def first_copy(slot, i):
        return pltpu.make_async_remote_copy(
            src_ref=first_out.at[i],
            dst_ref=first_in.at[i, slot],
            send_sem=first_send.at[i, slot],
            recv_sem=first_recv.at[i, slot],
            device_id=places[slot],
            device_id_type=MESH,
        )

    part_of = (pl.ds(2, 4), pl.ds(0, 4), pl.ds(4, 2), pl.ds(0, 2))

    def step_copy(slot, p):
        return pltpu.make_async_remote_copy(
            src_ref=out_buf.at[p, part_of[slot]],
            dst_ref=in_buf.at[p, slot, part_of[slot]],
            send_sem=send.at[p, slot],
            recv_sem=recv.at[p, slot],
            device_id=places[slot],
            device_id_type=MESH,
        )

    below, above, far_below, far_above = range(4)

    def combine_mid(own, got):
        return [own[q] + got(below, q + 2) + got(above, q - 2) for q in (2, 3)]

    def combine_rest(own, got):
        low = [own[q] + got(below, q + 2) + got(far_below, q + 4) for q in (0, 1)]
        top = [own[q] + got(above, q - 2) + got(far_above, q - 4) for q in (4, 5)]
        return low, top

    def columns(row):
        eye = iota((128, 128), 0) == iota((128, 128), 1)
        full = jnp.where(eye, jnp.broadcast_to(row, (128, 128)), 0.0)
        return jnp.sum(full, axis=1, keepdims=True)

    def pull(accs, pieces, cols):
        for r, col in cols.items():
            for half in range(2):
                b = (r % 2) * 2 + half
                base = b * NEAR + (r // 2) * OWN
                for i in range(0, OWN, 8):
                    at = half * OWN + i
                    c = col[at : at + 8, :]
                    for j, q in enumerate(pieces):
                        accs[j] = accs[j] + mt_ref[base + i : base + i + 8, q * 128 : (q + 1) * 128] * c
        return accs

    outer, inner = (0, 1, 4, 5), (2, 3)

    def evaluate(n, z, last):
        total = jnp.zeros((8, 512), F32)
        for tr in range(3):
            pair = jnp.concatenate([z[2 * tr], z[2 * tr + 1]], axis=0)
            lhs = jnp.concatenate(split(pair, 3) + [jnp.zeros((2, 128), BF16)], axis=0)
            total = total + jnp.dot(lhs, pick2_ref[tr], preferred_element_type=F32)
        total = total[0:2] + total[2:4] + total[4:6]
        means, tables = [], []
        for b in range(BANDS):
            rows = []
            tables.append([])
            for h in range(2):
                at = (b % 2) * 256 + h * 128
                row = total[b // 2 : b // 2 + 1, at : at + 128]
                tables[b].append(jnp.broadcast_to(row, (8, 128)))
                col = columns(row)
                for i in range(4):
                    blk = h * 4 + i
                    value = u_ref[b, blk * LIST : (blk + 1) * LIST, :] * col[i * LIST : (i + 1) * LIST, :]
                    rows.append(jnp.sum(value, axis=0, keepdims=True))
            means.append(ba[b] - jnp.concatenate(rows, axis=0))
        if last:
            for b in range(BANDS):
                fin[b, :, 0:ROWS] = means[b]
                fin[b, 0:1, 256:384] = z[2 + b // 2]
                fin[b, 1:8, 256:384] = jnp.zeros((7, 128), F32)
            for slot in range(BANDS):

                @pl.when(jnp.logical_not(owns(slot)))
                def _():
                    fin_copy(slot).start()

        lane = iota((1, 128), 1)
        found = jnp.zeros((1, 128), F32)
        for b in range(BANDS):
            pred = mix[b][0] * means[0]
            for b2 in range(1, BANDS):
                pred = pred + mix[b][b2] * means[b2]
            acc = jnp.zeros((8, 128), F32)
            for blk in range(BLOCKS):
                for half in range(2):
                    at = blk * ROWS + half * 128
                    idx = bs[b, :, at : at + 128] + (blk % 4) * LIST
                    picked = jnp.take_along_axis(tables[b][blk // 4], idx, axis=1)
                    left = bm[b, :, at : at + 128] - pred[blk : blk + 1, half * 128 : half * 128 + 128]
                    left = left - picked
                    acc = acc + bw[b, :, at : at + 128] * left * left
            value = jnp.sum(jnp.sum(acc, axis=0, keepdims=True), axis=1, keepdims=True)
            found = jnp.where(lane == n + b * SWEEPS, value, found)
        row_buf[0] = row_buf[0] + found

    def fin_copy(slot):
        return pltpu.make_async_remote_copy(
            src_ref=fin.at[slot],
            dst_ref=got,
            send_sem=fin_send.at[slot],
            recv_sem=fin_recv,
            device_id=(tile, slot),
            device_id_type=MESH,
        )

    x = (sky // 32) * 2 + band // 2
    y = (sky // 8) % 4
    z_at = sky % 8

    def core_at(dx, dy, dz, core):
        x_to, y_to, z_to = (x + dx) % 4, (y + dy) % 4, (z_at + dz) % 8
        return (x_to // 2) * 32 + y_to * 8 + z_to, (x_to % 2) * 2 + core

    def plane_copy(i):
        return pltpu.make_async_remote_copy(
            src_ref=row_buf.at[0],
            dst_ref=plane.at[x * 4 + y],
            send_sem=plane_send.at[i],
            recv_sem=plane_recv,
            device_id=core_at(PLANE[i][0], PLANE[i][1], 0, 1),
            device_id_type=MESH,
        )

    def line_copy(i):
        return pltpu.make_async_remote_copy(
            src_ref=row_buf.at[1],
            dst_ref=line.at[z_at % 4],
            send_sem=line_send.at[i],
            recv_sem=line_recv,
            device_id=core_at(0, 0, LINE[i][0], LINE[i][1]),
            device_id_type=MESH,
        )

    def whole(ref, sem):
        return pltpu.make_async_copy(ref, ref, sem)

    @pl.when(is_home)
    def _():
        build()
        for i in range(2):
            for slot in range(4):
                first_copy(slot, i).wait()
        start = []
        for i in range(2):
            own = [first_out[i, q] for q in range(6)]
            low, top = combine_rest(own, lambda s, q: first_in[i, s, q])
            start.append(low + combine_mid(own, lambda s, q: first_in[i, s, q]) + top)
        known, dens = start
        scale = [1.0 / (d + PRIOR_WEIGHT) for d in dens]
        colors = [bn[q : q + 1, 128:256] for q in range(6)]
        zero = jnp.zeros((1, 128), F32)
        z = [jnp.where(colors[q] == 0.0, known[q] * scale[q], zero) for q in range(6)]
        cols = {q: columns(z[q]) for q in range(6)}
        accs = pull([jnp.zeros((8, 128), F32) for _ in range(6)], range(6), cols)
        for q in range(6):
            out_buf[1, q] = jnp.sum(accs[q], axis=0, keepdims=True)
        for slot in (2, 3, 0, 1):
            step_copy(slot, 1).start()
        row_buf[0] = zero

        def renew(q, color, pulled, old):
            return jnp.where(colors[q] == color, (known[q] + pulled) * scale[q], old)

        def absorb(s, z, then):
            p = s % 2
            color = (s % COLORS).astype(F32) if not isinstance(s, int) else float(s % COLORS)
            own = [out_buf[p, q] for q in range(6)]
            take = lambda i, q: in_buf[p, i, q]
            z = list(z)
            for slot in (0, 1):
                step_copy(slot, p).wait_recv()
            mid = combine_mid(own, take)
            for q in inner:
                z[q] = renew(q, color, mid[q - 2], z[q])
            accs = None
            if then:
                cols = {q: columns(z[q]) for q in inner}
                accs = pull([jnp.zeros((8, 128), F32) for _ in range(6)], range(6), cols)
            for slot in (2, 3):
                step_copy(slot, p).wait_recv()
            low, top = combine_rest(own, take)
            for j, q in enumerate(outer):
                z[q] = renew(q, color, (low + top)[j], z[q])
            return z, accs

        def step(s, z):
            p = s % 2

            @pl.when((s == 2) & moves)
            def _():
                pl.semaphore_wait(go, 1)
                mag_copy(band).start()

            @pl.when(s % COLORS == 0)
            def _():
                @pl.when(s == COLORS)
                def _():
                    for slot in range(BANDS):

                        @pl.when(jnp.logical_not(owns(slot)))
                        def _():
                            table_copy(0, slot).wait_recv()
                            mag_copy(slot).wait_recv()

                evaluate(s // COLORS - 1, z, False)

            z, accs = absorb(s, z, True)
            cols = {q: columns(z[q]) for q in outer}
            far = pull([accs[q] for q in outer], outer, cols)
            for j, q in enumerate(outer):
                out_buf[1 - p, q] = jnp.sum(far[j], axis=0, keepdims=True)
            for slot in (2, 3):
                step_copy(slot, 1 - p).start()
            near_accs = pull([accs[q] for q in inner], inner, cols)
            for j, q in enumerate(inner):
                out_buf[1 - p, q] = jnp.sum(near_accs[j], axis=0, keepdims=True)
            for slot in (0, 1):
                step_copy(slot, 1 - p).start()
            for slot in range(4):
                step_copy(slot, p).wait_send()
            return tuple(z)

        z = lax.fori_loop(1, STEPS - 1, step, tuple(z))
        z, _ = absorb(STEPS - 1, z, False)
        evaluate(SWEEPS - 1, z, True)
        for i in range(len(PLANE)):
            plane_copy(i).start()
        mine = pltpu.make_async_copy(row_buf.at[0], plane.at[x * 4 + y], plane_recv)
        mine.start()
        whole(plane, plane_recv).wait()
        row_buf[1] = jnp.sum(plane[...].reshape(16, 128), axis=0, keepdims=True)
        for i in range(len(LINE)):
            line_copy(i).start()
        mine = pltpu.make_async_copy(row_buf.at[1], line.at[z_at % 4], line_recv)
        mine.start()
        for i in range(len(PLANE)):
            plane_copy(i).wait_send()
        for slot in range(4):
            step_copy(slot, (STEPS - 1) % 2).wait_send()

    @pl.when(jnp.logical_not(is_home))
    def _():
        pl.semaphore_wait(go, 1)
        mag_copy(band).start()

    @pl.when(moves)
    def _():
        @pl.when(band == teller)
        def _():
            table_copy(1, band).wait_send()

        table_copy(0, band).wait_send()
        table_copy(2, band).wait_send()
        for c in range(CHUNKS):
            for i in range(2):
                ship_copy(i, band, c).wait_send()
        mag_copy(band).wait_send()
        fin_copy(0).wait_recv()

    @pl.when(stays)
    def _():
        mine = pltpu.make_async_copy(fin.at[band], got, local.at[0])
        mine.start()
        mine.wait()

    out_ref[:, 0:256] = got[:, 0:256]
    pair = got[0:1, 256:384]
    out_ref[:, 256:512] = jnp.zeros((8, 256), F32)
    out_ref[0:1, 256:384] = jnp.where(band % 2 == 0, pair, pltpu.roll(pair, OWN, 1))

    whole(line, line_recv).wait()
    total = jnp.sum(line[...].reshape(4, 128), axis=0, keepdims=True)
    total = pltpu.roll(total, (128 - band * SWEEPS) % 128, 1)
    out_ref[0:1, 384:512] = total * (1.0 / (OBS * STARS * TILES))

    @pl.when(is_home)
    def _():
        for slot in range(BANDS):

            @pl.when(jnp.logical_not(owns(slot)))
            def _():
                fin_copy(slot).wait_send()

        for i in range(len(LINE)):
            line_copy(i).wait_send()


def solve(color_terms, m, w, s, owner, colors, lists):
    vmem = pl.BlockSpec(memory_space=pltpu.VMEM)
    hbm = pl.BlockSpec(memory_space=pl.ANY)
    dma = pltpu.SemaphoreType.DMA
    return pl.pallas_call(
        solve_kernel,
        out_shape=pltpu.VMEM((8, 512), F32),
        in_specs=[hbm] * 7,
        out_specs=vmem,
        scratch_shapes=[
            pltpu.SMEM(color_terms.shape, F32),
            pltpu.VMEM((OBS, STARS), F32),
            pltpu.VMEM((OBS, STARS), F32),
            pltpu.VMEM((OBS, STARS), jnp.int32),
            pltpu.VMEM(owner.shape, jnp.int32),
            pltpu.VMEM(colors.shape, jnp.int32),
            pltpu.VMEM(lists.shape, jnp.int32),
            pltpu.VMEM((BLOCKS, ROWS), F32),
            pltpu.VMEM((BANDS, BLOCKS, ROWS), F32),
            pltpu.VMEM((8, 128), F32),
            pltpu.VMEM((8, 384), F32),
            pltpu.VMEM((BANDS, OBS, STARS), F32),
            pltpu.VMEM((BANDS, OBS, STARS), F32),
            pltpu.VMEM((BANDS, OBS, STARS), jnp.int32),
            pltpu.VMEM((BANDS, BLOCKS, ROWS), F32),
            pltpu.VMEM((BANDS, 8, 128), F32),
            pltpu.VMEM((8, 384), F32),
            pltpu.VMEM((BANDS, BLOCKS * LIST, ROWS), F32),
            pltpu.VMEM((2, BANDS, BLOCKS * LIST, WIDE), BF16),
            pltpu.VMEM((WIDE, WIDE), F32),
            pltpu.VMEM((3, 128, 512), BF16),
            pltpu.VMEM((2, 6, 1, 128), F32),
            pltpu.VMEM((2, 4, 6, 1, 128), F32),
            pltpu.VMEM((2, 6, 1, 128), F32),
            pltpu.VMEM((2, 4, 6, 1, 128), F32),
            pltpu.VMEM((BANDS, 8, 384), F32),
            pltpu.VMEM((8, 384), F32),
            pltpu.VMEM((2, 1, 128), F32),
            pltpu.VMEM((16, 1, 128), F32),
            pltpu.VMEM((4, 1, 128), F32),
            dma((7,)),
            dma((BANDS - 1,)),
            dma((BANDS - 1,)),
            dma((2, CHUNKS)),
            dma((BANDS, 2, CHUNKS)),
            dma,
            dma((BANDS,)),
            dma((3,)),
            dma((BANDS, 3)),
            dma((5,)),
            dma((2, 4)),
            dma((2, 4)),
            dma((2, 4)),
            dma((2, 4)),
            dma((BANDS,)),
            dma,
            dma((len(PLANE),)),
            dma,
            dma((len(LINE),)),
            dma,
            pltpu.SemaphoreType.REGULAR,
        ],
        compiler_params=pltpu.CompilerParams(has_side_effects=True, collective_id=0),
        name="solve",
    )(color_terms, m, w, s, owner, colors, lists)


def unpack_kernel(out_ref, zp_ref, mags_ref, mis_ref):
    zp_ref[...] = out_ref[0:1, 256 : 256 + OWN]
    mis_ref[...] = out_ref[0:1, 384 : 384 + SWEEPS]
    for blk in range(BLOCKS):
        mags_ref[0:1, blk * ROWS : (blk + 1) * ROWS] = out_ref[blk : blk + 1, 0:ROWS]


def body(magnitudes, weights, slots, block_fields, owner, colors, color_terms):
    out = solve(
        color_terms, magnitudes[0], weights[0], slots[0],
        owner.reshape(-1, 128), colors.reshape(-1, 128), block_fields,
    )
    vmem = pl.BlockSpec(memory_space=pltpu.VMEM)
    out = pltpu.with_memory_space_constraint(out, pltpu.VMEM)
    zp, mags, misfit = pl.pallas_call(
        unpack_kernel,
        out_shape=(
            jax.ShapeDtypeStruct((1, OWN), F32),
            jax.ShapeDtypeStruct((1, STARS), F32),
            jax.ShapeDtypeStruct((1, SWEEPS), F32),
        ),
        in_specs=[vmem],
        out_specs=(vmem,) * 3,
        name="unpack",
    )(out)
    return zp, mags, misfit.T


def solution(mesh):
    in_specs = (
        P("band", None, "sky"),
        P("band", None, "sky"),
        P("band", None, "sky"),
        P("sky", None),
        P(),
        P(),
        P(),
    )
    out_specs = (P("band", "sky"), P("band", "sky"), P(None, "band"))
    return jax.shard_map(body, mesh=mesh, in_specs=in_specs, out_specs=out_specs, check_vma=False)
```

```python
import functools

import jax
import jax.numpy as jnp
from jax import lax
from jax.experimental import pallas as pl
from jax.experimental.pallas import tpu as pltpu
from jax.sharding import PartitionSpec as P

COLORS = 8
SWEEPS = 4
PRIOR_WEIGHT = 1.0

TILES = 64
BANDS = 4
OBS = 8
BLOCKS = 8
ROWS = 256
STARS = BLOCKS * ROWS
LIST = 32
OWN = 64
NEAR = 3 * OWN
CUTS = (0, 2, 4, 6, 8)
CHUNKS = len(CUTS) - 1
EARLY = 2
WIDE = BANDS * NEAR
STEPS = COLORS * SWEEPS
PLANE = [(i, j) for i in (2, 1, 3, 0) for j in (2, 1, 3, 0)][:-1]
LINE = [(k, c) for k in (4, 3, 5, 2, 6, 1, 7, 0) for c in (0, 1)][:-1]
MESH = pl.DeviceIdType.MESH
HIGH = lax.Precision.HIGHEST
F32 = jnp.float32
BF16 = jnp.bfloat16


def home_of(tile):
    half = tile // 32
    row = tile // 8
    y = row % 4
    z = tile % 8
    leg = z // 4
    y_new = y + half * (3 - 2 * y)
    z_new = z + leg * (7 - 2 * z)
    x_lo = (1 - half + row + leg) % 2
    return half * 32 + y_new * 8 + z_new, x_lo * 2 + 1


def tile_at(sky, band):
    half = sky // 32
    y_new = (sky // 8) % 4
    z_new = sky % 8
    y = y_new + half * (3 - 2 * y_new)
    row = half * 4 + y
    leg = (band // 2 + 1 + half + row) % 2
    z = z_new + leg * (7 - 2 * z_new)
    is_home = (band % 2 == 1) & (z_new < 4)
    return is_home, (row * 8 + z) % TILES


def iota(shape, dim):
    return lax.broadcasted_iota(jnp.int32, shape, dim)


def as_column(row, count):
    eye = iota((count, 128), 0) == iota((count, 128), 1)
    full = jnp.broadcast_to(row, (count, 128))
    return jnp.sum(jnp.where(eye, full, 0.0), axis=1, keepdims=True)


def as_row(col, shift):
    n = col.shape[0]
    hit = iota((n, 128), 1) == iota((n, 128), 0) + shift
    return jnp.sum(jnp.where(hit, col, 0.0), axis=0, keepdims=True)


def split(x, terms):
    parts = []
    for _ in range(terms - 1):
        part = x.astype(BF16)
        parts.append(part)
        x = x - part.astype(F32)
    return parts + [x.astype(BF16)]


def tile_tables(tile, own_ref, col_ref, lst_ref, near_ref):
    rows = own_ref.shape[0]
    until = jnp.where(iota((128, 128), 0) <= iota((128, 128), 1), 1.0, 0.0).astype(BF16)
    before = jnp.where(iota((rows, rows), 1) < iota((rows, rows), 0), 1.0, 0.0).astype(BF16)
    number = (iota((rows, 128), 0) * 128 + iota((rows, 128), 1)).astype(F32)
    shade = col_ref[...].astype(F32)
    rank_at = iota((OWN, 128), 0).astype(F32)
    for tr in range(3):
        mine = own_ref[...] == (tile + tr - 1 + TILES) % TILES
        one = jnp.where(mine, 1.0, 0.0)
        inside = jnp.dot(one.astype(BF16), until, preferred_element_type=F32)
        above = jnp.dot(before, one.astype(BF16), preferred_element_type=F32)
        above = jnp.sum(above, axis=1, keepdims=True)
        rank = jnp.where(mine, inside + above - 1.0, -1.0)
        ids = jnp.zeros((OWN, 128), F32)
        cols = jnp.zeros((OWN, 128), F32)
        for i in range(rows):
            hit = rank[i : i + 1] == rank_at
            ids = ids + jnp.where(hit, number[i : i + 1], 0.0)
            cols = cols + jnp.where(hit, shade[i : i + 1], 0.0)
        for value, at in ((ids, 0), (cols, 128)):
            col = jnp.sum(value, axis=1, keepdims=True)
            row = as_row(col, 0) + as_row(col, OWN)
            near_ref[2 * tr : 2 * tr + 1, at : at + 128] = row
            near_ref[2 * tr + 1 : 2 * tr + 2, at : at + 128] = row
    near_ref[6:8, 128:256] = jnp.zeros((2, 128), F32)
    listed = lst_ref[...].astype(F32)
    near_ref[:, 256:384] = jnp.concatenate([listed] * BANDS, axis=1)
    for h in range(2):
        row = [listed[i : i + 1] for i in range(4 * h, 4 * h + 4)]
        near_ref[6 + h : 7 + h, 0:128] = jnp.concatenate(row, axis=1)


def star_means(m_ref, w_ref, mean_ref):
    for blk in range(BLOCKS):
        cols = slice(blk * ROWS, (blk + 1) * ROWS)
        top = jnp.sum(w_ref[:, cols] * m_ref[:, cols], axis=0, keepdims=True)
        mean_ref[blk : blk + 1, :] = top / jnp.sum(w_ref[:, cols], axis=0, keepdims=True)


def list_sums(m_ref, w_ref, s_ref, pred, aux_ref):
    entries = iota((LIST, ROWS), 0)
    rows = [jnp.zeros((1, 128), F32) for _ in range(4)]
    for blk in range(BLOCKS):
        cols = slice(blk * ROWS, (blk + 1) * ROWS)
        acc = jnp.zeros((LIST, ROWS), F32)
        wts = jnp.zeros((LIST, ROWS), F32)
        for k in range(OBS):
            hit = s_ref[k : k + 1, cols] == entries
            wk = w_ref[k : k + 1, cols]
            wts = wts + jnp.where(hit, wk, 0.0)
            acc = acc + jnp.where(hit, wk * (m_ref[k : k + 1, cols] - pred[blk : blk + 1]), 0.0)
        h, at = blk // 4, (blk % 4) * LIST
        rows[h] = rows[h] + as_row(jnp.sum(acc, axis=1, keepdims=True), at)
        rows[2 + h] = rows[2 + h] + as_row(jnp.sum(wts, axis=1, keepdims=True), at)
    aux_ref[...] = jnp.concatenate(rows + [jnp.zeros((4, 128), F32)], axis=0)


def solve_kernel(
    ct_hbm, m_hbm, w_hbm, s_hbm, own_hbm, col_hbm, lst_hbm,
    out_ref,
    ct_ref, m_ref, w_ref, s_ref, own_ref, col_ref, lst_ref,
    mean, mates, aux, near, bm, bw, bs, ba, bt, bn, u_ref, r_ref, mt_ref, pick2_ref,
    first_out, first_in, out_buf, in_buf, fin, got, row_buf, plane, line,
    load_sem, mate_send, mate_recv, ship_send, ship_recv, mag_send, mag_recv, tab_send, tab_recv, local,
    first_send, first_recv, send, recv,
    fin_send, fin_recv, plane_send, plane_recv, line_send, line_recv, go,
):
    sky = lax.axis_index("sky")
    band = lax.axis_index("band")
    home_sky, home_band = home_of(sky)
    stays = (home_sky == sky) & (home_band == band)
    moves = jnp.logical_not(stays)
    is_home, tile = tile_at(sky, band)
    places = [home_of((tile + d + TILES) % TILES) for d in (1, -1, 2, -2)]

    def owns(slot):
        return (tile == sky) & (band == slot)

    barrier = pltpu.get_barrier_semaphore()
    mates_of = [(band + i) % BANDS for i in range(1, BANDS)]
    for mate in mates_of:
        pl.semaphore_signal(barrier, inc=1, device_id=(sky, mate), device_id_type=MESH)

    @pl.when(moves)
    def _():
        pl.semaphore_signal(barrier, inc=1, device_id=(home_sky, home_band), device_id_type=MESH)

    @pl.when(is_home)
    def _():
        for place in places:
            pl.semaphore_signal(barrier, inc=1, device_id=place, device_id_type=MESH)
        for slot in range(BANDS):

            @pl.when(jnp.logical_not(owns(slot)))
            def _():
                pl.semaphore_signal(barrier, inc=1, device_id=(tile, slot), device_id_type=MESH)

    loads = [
        pltpu.make_async_copy(src, dst, load_sem.at[i])
        for i, (src, dst) in enumerate(
            (
                (w_hbm, w_ref), (s_hbm, s_ref), (m_hbm, m_ref),
                (own_hbm, own_ref), (col_hbm, col_ref), (lst_hbm, lst_ref), (ct_hbm, ct_ref),
            )
        )
    ]
    for load in loads:
        load.start()
    for load in loads[:2]:
        load.wait()

    @pl.when(is_home & moves)
    def _():
        pl.semaphore_wait(barrier, 12)

    @pl.when(is_home & stays)
    def _():
        pl.semaphore_wait(barrier, 10)

    @pl.when(jnp.logical_not(is_home))
    def _():
        pl.semaphore_wait(barrier, 4)

    def chunk(ref, slot, c):
        at = pl.ds(CUTS[c] * ROWS, (CUTS[c + 1] - CUTS[c]) * ROWS)
        return ref.at[:, at] if slot is None else ref.at[slot, :, at]

    def ship_copy(i, slot, c):
        src, dst = ((w_ref, bw), (s_ref, bs))[i]
        return pltpu.make_async_remote_copy(
            src_ref=chunk(src, None, c),
            dst_ref=chunk(dst, slot, c),
            send_sem=ship_send.at[i, c],
            recv_sem=ship_recv.at[slot, i, c],
            device_id=(home_sky, home_band),
            device_id_type=MESH,
        )

    def mag_copy(slot):
        return pltpu.make_async_remote_copy(
            src_ref=m_ref,
            dst_ref=bm.at[slot],
            send_sem=mag_send,
            recv_sem=mag_recv.at[slot],
            device_id=(home_sky, home_band),
            device_id_type=MESH,
        )

    def mate_copy(i):
        return pltpu.make_async_remote_copy(
            src_ref=mean,
            dst_ref=mates.at[band],
            send_sem=mate_send.at[i],
            recv_sem=mate_recv.at[i],
            device_id=(sky, mates_of[i]),
            device_id_type=MESH,
        )

    def table_copy(i, slot):
        src, dst = ((mean, ba.at[slot]), (near, bn), (aux, bt.at[slot]))[i]
        return pltpu.make_async_remote_copy(
            src_ref=src,
            dst_ref=dst,
            send_sem=tab_send.at[i],
            recv_sem=tab_recv.at[slot, i],
            device_id=(home_sky, home_band),
            device_id_type=MESH,
        )

    teller = 0

    @pl.when(moves)
    def _():
        for i in range(2):
            ship_copy(i, band, 0).start()

    loads[2].wait()
    star_means(m_ref, w_ref, mean)
    for i in range(BANDS - 1):
        mate_copy(i).start()
    keep = pltpu.make_async_copy(mean, mates.at[band], local.at[4])
    keep.start()

    for load in loads[3:]:
        load.wait()
    tile_tables(sky, own_ref, col_ref, lst_ref, near)

    @pl.when(moves)
    def _():
        @pl.when(band == teller)
        def _():
            table_copy(1, band).start()

        for c in range(1, EARLY):
            for i in range(2):
                ship_copy(i, band, c).start()

    mix = []
    for b in range(BANDS):
        total = ct_ref[b, 0]
        for b2 in range(1, BANDS):
            total = total + ct_ref[b, b2]
        mix.append([ct_ref[b, b2] + (1.0 - total if b == b2 else 0.0) for b2 in range(BANDS)])

    keep.wait()
    for i in range(BANDS - 1):
        mate_copy(i).wait_recv()
    pred = jnp.zeros((BLOCKS, ROWS), F32)
    for b2 in range(BANDS):
        factor = mix[0][b2]
        for b in range(1, BANDS):
            factor = jnp.where(band == b, mix[b][b2], factor)
        pred = pred + factor * mates[b2]
    list_sums(m_ref, w_ref, s_ref, pred, aux)

    @pl.when(moves)
    def _():
        table_copy(2, band).start()
        for c in range(EARLY, CHUNKS):
            for i in range(2):
                ship_copy(i, band, c).start()
        table_copy(0, band).start()

    @pl.when(stays)
    def _():
        copies = [
            pltpu.make_async_copy(mean, ba.at[band], local.at[0]),
            pltpu.make_async_copy(w_ref, bw.at[band], local.at[1]),
            pltpu.make_async_copy(s_ref, bs.at[band], local.at[2]),
            pltpu.make_async_copy(m_ref, bm.at[band], local.at[3]),
            pltpu.make_async_copy(aux, bt.at[band], local.at[4]),
        ]
        for copy in copies:
            copy.start()
        for copy in copies:
            copy.wait()

    for i in range(BANDS - 1):
        mate_copy(i).wait_send()

    def await_tables():
        table_copy(1, teller).wait_recv()

    def await_sums():
        for slot in range(BANDS):

            @pl.when(jnp.logical_not(owns(slot)))
            def _():
                table_copy(2, slot).wait_recv()

    def await_chunk(c):
        for slot in range(BANDS):

            @pl.when(jnp.logical_not(owns(slot)))
            def _():
                for i in range(2):
                    ship_copy(i, slot, c).wait_recv()

    def build():
        row_band = iota((128, 128), 0) // LIST
        lane_list = iota((128, 128), 1) // LIST
        lane_own = iota((128, 128), 1) // OWN
        mixes = jnp.zeros((128, 128), F32)
        for b2 in range(BANDS):
            for b in range(BANDS):
                mixes = jnp.where((row_band == b2) & (lane_list == b), mix[b][b2], mixes)
        entries = iota((LIST, ROWS), 0)
        await_tables()
        pick = []
        for tr in range(3):
            col = as_column(bn[2 * tr : 2 * tr + 1, 0:128], OWN)
            one = jnp.concatenate(
                [jnp.where(col == bn[6 + h : 7 + h, 0:128], 1.0, 0.0) for h in range(2)], axis=1
            ).astype(BF16)
            none = jnp.zeros((OWN, 256), BF16)
            pick2_ref[tr, 0:OWN, 0:256] = one
            pick2_ref[tr, OWN:128, 0:256] = none
            pick2_ref[tr, 0:OWN, 256:512] = none
            pick2_ref[tr, OWN:128, 256:512] = one
            pick.append(one)
        pick = jnp.concatenate(pick, axis=0)
        for blk in range(BLOCKS):
            if blk in CUTS:
                await_chunk(CUTS.index(blk))
            if blk == CUTS[-2]:
                for slot in range(BANDS):

                    @pl.when(jnp.logical_not(owns(slot)))
                    def _():
                        pl.semaphore_signal(go, inc=1, device_id=(tile, slot), device_id_type=MESH)

            cols = slice(blk * ROWS, (blk + 1) * ROWS)
            wide, scaled = [], []
            for b in range(BANDS):
                acc = jnp.zeros((LIST, ROWS), F32)
                for k in range(OBS):
                    wk = bw[b, k : k + 1, cols]
                    acc = acc + jnp.where(bs[b, k : k + 1, cols] == entries, wk, 0.0)
                star_w = jnp.sum(bw[b, :, cols], axis=0, keepdims=True)
                wide.append(acc)
                scaled.append(acc * (1.0 / star_w))
                u_ref[b, blk * LIST : (blk + 1) * LIST, :] = scaled[b]
            w_hi, w_lo = split(jnp.concatenate(wide, axis=0), 2)
            u_hi, u_lo = split(jnp.concatenate(scaled, axis=0), 2)
            dims = (((1,), (1,)), ((), ()))
            both = lax.dot_general(
                jnp.concatenate([u_hi, u_lo], axis=0), w_hi, dims, preferred_element_type=F32
            )
            gt = both[0:128] + both[128:256]
            gt = gt + lax.dot_general(u_hi, w_lo, dims, preferred_element_type=F32)
            lhs = jnp.concatenate(split(gt * mixes, 2), axis=0)
            col = as_column(bn[blk : blk + 1, 256:384], 128)
            for q in range(6):
                hit = (col == bn[q : q + 1, 0:128]) & (row_band == lane_own + 2 * (q % 2))
                moved = jnp.dot(
                    lhs, jnp.where(hit, 1.0, 0.0).astype(BF16), preferred_element_type=F32
                ).astype(BF16)
                for i in range(2):
                    for b2 in range(BANDS):
                        at = i * 128 + b2 * LIST
                        r_ref[
                            i, b2, blk * LIST : (blk + 1) * LIST, q * 128 : (q + 1) * 128
                        ] = moved[at : at + LIST]
            if blk == CUTS[EARLY] - 1:
                await_sums()
                first_sums(pick)
            if blk in (3, 7):
                at = slice((blk - 3) * LIST, (blk + 1) * LIST)
                for b2 in range(BANDS):
                    total = jnp.dot(pick[:, at], r_ref[0, b2, at, :], preferred_element_type=F32)
                    total = total + jnp.dot(pick[:, at], r_ref[1, b2, at, :], preferred_element_type=F32)
                    rows = slice(b2 * NEAR, (b2 + 1) * NEAR)
                    mt_ref[rows, :] = total if blk == 3 else mt_ref[rows, :] + total

    def first_sums(pick):
        rows = [jnp.concatenate([bt[b, h : h + 1, :] for h in range(2)], axis=1) for b in range(BANDS)]
        rows += [jnp.concatenate([bt[b, h : h + 1, :] for h in (2, 3)], axis=1) for b in range(BANDS)]
        terms = jnp.concatenate(split(jnp.concatenate(rows, axis=0), 3), axis=0)
        sums = lax.dot_general(terms, pick, (((1,), (1,)), ((), ())), preferred_element_type=F32)
        sums = sums[0:8] + sums[8:16] + sums[16:24]
        for i in range(2):
            for q in range(6):
                tr, b = q // 2, 2 * (q % 2)
                at = slice(tr * OWN, (tr + 1) * OWN)
                low, high = i * BANDS + b, i * BANDS + b + 1
                first_out[i, q] = jnp.concatenate(
                    [sums[low : low + 1, at], sums[high : high + 1, at]], axis=1
                )
        for i in range(2):
            for slot in (2, 3, 0, 1):
                first_copy(slot, i).start()
    def first_copy(slot, i):
        return pltpu.make_async_remote_copy(
            src_ref=first_out.at[i],
            dst_ref=first_in.at[i, slot],
            send_sem=first_send.at[i, slot],
            recv_sem=first_recv.at[i, slot],
            device_id=places[slot],
            device_id_type=MESH,
        )

    part_of = (pl.ds(2, 4), pl.ds(0, 4), pl.ds(4, 2), pl.ds(0, 2))

    def step_copy(slot, p):
        return pltpu.make_async_remote_copy(
            src_ref=out_buf.at[p, part_of[slot]],
            dst_ref=in_buf.at[p, slot, part_of[slot]],
            send_sem=send.at[p, slot],
            recv_sem=recv.at[p, slot],
            device_id=places[slot],
            device_id_type=MESH,
        )

    below, above, far_below, far_above = range(4)

    def combine_mid(own, got):
        return [own[q] + got(below, q + 2) + got(above, q - 2) for q in (2, 3)]

    def combine_rest(own, got):
        low = [own[q] + got(below, q + 2) + got(far_below, q + 4) for q in (0, 1)]
        top = [own[q] + got(above, q - 2) + got(far_above, q - 4) for q in (4, 5)]
        return low, top

    def columns(row):
        eye = iota((128, 128), 0) == iota((128, 128), 1)
        full = jnp.where(eye, jnp.broadcast_to(row, (128, 128)), 0.0)
        return jnp.sum(full, axis=1, keepdims=True)

    def pull(accs, pieces, cols):
        for r, col in cols.items():
            for half in range(2):
                b = (r % 2) * 2 + half
                base = b * NEAR + (r // 2) * OWN
                for i in range(0, OWN, 8):
                    at = half * OWN + i
                    c = col[at : at + 8, :]
                    for j, q in enumerate(pieces):
                        accs[j] = accs[j] + mt_ref[base + i : base + i + 8, q * 128 : (q + 1) * 128] * c
        return accs

    outer, inner = (0, 1, 4, 5), (2, 3)

    def evaluate(n, z, last):
        total = jnp.zeros((8, 512), F32)
        for tr in range(3):
            pair = jnp.concatenate([z[2 * tr], z[2 * tr + 1]], axis=0)
            lhs = jnp.concatenate(split(pair, 3) + [jnp.zeros((2, 128), BF16)], axis=0)
            total = total + jnp.dot(lhs, pick2_ref[tr], preferred_element_type=F32)
        total = total[0:2] + total[2:4] + total[4:6]
        means, tables = [], []
        for b in range(BANDS):
            rows = []
            tables.append([])
            for h in range(2):
                at = (b % 2) * 256 + h * 128
                row = total[b // 2 : b // 2 + 1, at : at + 128]
                tables[b].append(jnp.broadcast_to(row, (8, 128)))
                col = columns(row)
                for i in range(4):
                    blk = h * 4 + i
                    value = u_ref[b, blk * LIST : (blk + 1) * LIST, :] * col[i * LIST : (i + 1) * LIST, :]
                    rows.append(jnp.sum(value, axis=0, keepdims=True))
            means.append(ba[b] - jnp.concatenate(rows, axis=0))
        if last:
            for b in range(BANDS):
                fin[b, :, 0:ROWS] = means[b]
                fin[b, 0:1, 256:384] = z[2 + b // 2]
                fin[b, 1:8, 256:384] = jnp.zeros((7, 128), F32)
            for slot in range(BANDS):

                @pl.when(jnp.logical_not(owns(slot)))
                def _():
                    fin_copy(slot).start()

        lane = iota((1, 128), 1)
        found = jnp.zeros((1, 128), F32)
        for b in range(BANDS):
            pred = mix[b][0] * means[0]
            for b2 in range(1, BANDS):
                pred = pred + mix[b][b2] * means[b2]
            acc = jnp.zeros((8, 128), F32)
            for blk in range(BLOCKS):
                for half in range(2):
                    at = blk * ROWS + half * 128
                    idx = bs[b, :, at : at + 128] + (blk % 4) * LIST
                    picked = jnp.take_along_axis(tables[b][blk // 4], idx, axis=1)
                    left = bm[b, :, at : at + 128] - pred[blk : blk + 1, half * 128 : half * 128 + 128]
                    left = left - picked
                    acc = acc + bw[b, :, at : at + 128] * left * left
            value = jnp.sum(jnp.sum(acc, axis=0, keepdims=True), axis=1, keepdims=True)
            found = jnp.where(lane == n + b * SWEEPS, value, found)
        row_buf[0] = row_buf[0] + found

    def fin_copy(slot):
        return pltpu.make_async_remote_copy(
            src_ref=fin.at[slot],
            dst_ref=got,
            send_sem=fin_send.at[slot],
            recv_sem=fin_recv,
            device_id=(tile, slot),
            device_id_type=MESH,
        )

    x = (sky // 32) * 2 + band // 2
    y = (sky // 8) % 4
    z_at = sky % 8

    def core_at(dx, dy, dz, core):
        x_to, y_to, z_to = (x + dx) % 4, (y + dy) % 4, (z_at + dz) % 8
        return (x_to // 2) * 32 + y_to * 8 + z_to, (x_to % 2) * 2 + core

    def plane_copy(i):
        return pltpu.make_async_remote_copy(
            src_ref=row_buf.at[0],
            dst_ref=plane.at[x * 4 + y],
            send_sem=plane_send.at[i],
            recv_sem=plane_recv,
            device_id=core_at(PLANE[i][0], PLANE[i][1], 0, 1),
            device_id_type=MESH,
        )

    def line_copy(i):
        return pltpu.make_async_remote_copy(
            src_ref=row_buf.at[1],
            dst_ref=line.at[z_at % 4],
            send_sem=line_send.at[i],
            recv_sem=line_recv,
            device_id=core_at(0, 0, LINE[i][0], LINE[i][1]),
            device_id_type=MESH,
        )

    def whole(ref, sem):
        return pltpu.make_async_copy(ref, ref, sem)

    @pl.when(is_home)
    def _():
        build()
        for i in range(2):
            for slot in range(4):
                first_copy(slot, i).wait()
        start = []
        for i in range(2):
            own = [first_out[i, q] for q in range(6)]
            low, top = combine_rest(own, lambda s, q: first_in[i, s, q])
            start.append(low + combine_mid(own, lambda s, q: first_in[i, s, q]) + top)
        known, dens = start
        scale = [1.0 / (d + PRIOR_WEIGHT) for d in dens]
        colors = [bn[q : q + 1, 128:256] for q in range(6)]
        zero = jnp.zeros((1, 128), F32)
        z = [jnp.where(colors[q] == 0.0, known[q] * scale[q], zero) for q in range(6)]
        cols = {q: columns(z[q]) for q in range(6)}
        accs = pull([jnp.zeros((8, 128), F32) for _ in range(6)], range(6), cols)
        for q in range(6):
            out_buf[1, q] = jnp.sum(accs[q], axis=0, keepdims=True)
        for slot in (2, 3, 0, 1):
            step_copy(slot, 1).start()
        row_buf[0] = zero

        def renew(q, color, pulled, old):
            return jnp.where(colors[q] == color, (known[q] + pulled) * scale[q], old)

        def absorb(s, z, then):
            p = s % 2
            color = (s % COLORS).astype(F32) if not isinstance(s, int) else float(s % COLORS)
            own = [out_buf[p, q] for q in range(6)]
            take = lambda i, q: in_buf[p, i, q]
            z = list(z)
            for slot in (0, 1):
                step_copy(slot, p).wait_recv()
            mid = combine_mid(own, take)
            for q in inner:
                z[q] = renew(q, color, mid[q - 2], z[q])
            accs = None
            if then:
                cols = {q: columns(z[q]) for q in inner}
                accs = pull([jnp.zeros((8, 128), F32) for _ in range(6)], range(6), cols)
            for slot in (2, 3):
                step_copy(slot, p).wait_recv()
            low, top = combine_rest(own, take)
            for j, q in enumerate(outer):
                z[q] = renew(q, color, (low + top)[j], z[q])
            return z, accs

        def step(s, z):
            p = s % 2

            @pl.when((s == 2) & moves)
            def _():
                pl.semaphore_wait(go, 1)
                mag_copy(band).start()

            @pl.when(s % COLORS == 0)
            def _():
                @pl.when(s == COLORS)
                def _():
                    for slot in range(BANDS):

                        @pl.when(jnp.logical_not(owns(slot)))
                        def _():
                            table_copy(0, slot).wait_recv()
                            mag_copy(slot).wait_recv()

                evaluate(s // COLORS - 1, z, False)

            z, accs = absorb(s, z, True)
            cols = {q: columns(z[q]) for q in outer}
            far = pull([accs[q] for q in outer], outer, cols)
            for j, q in enumerate(outer):
                out_buf[1 - p, q] = jnp.sum(far[j], axis=0, keepdims=True)
            for slot in (2, 3):
                step_copy(slot, 1 - p).start()
            near_accs = pull([accs[q] for q in inner], inner, cols)
            for j, q in enumerate(inner):
                out_buf[1 - p, q] = jnp.sum(near_accs[j], axis=0, keepdims=True)
            for slot in (0, 1):
                step_copy(slot, 1 - p).start()
            for slot in range(4):
                step_copy(slot, p).wait_send()
            return tuple(z)

        z = lax.fori_loop(1, STEPS - 1, step, tuple(z))
        z, _ = absorb(STEPS - 1, z, False)
        evaluate(SWEEPS - 1, z, True)
        for i in range(len(PLANE)):
            plane_copy(i).start()
        mine = pltpu.make_async_copy(row_buf.at[0], plane.at[x * 4 + y], plane_recv)
        mine.start()
        whole(plane, plane_recv).wait()
        row_buf[1] = jnp.sum(plane[...].reshape(16, 128), axis=0, keepdims=True)
        for i in range(len(LINE)):
            line_copy(i).start()
        mine = pltpu.make_async_copy(row_buf.at[1], line.at[z_at % 4], line_recv)
        mine.start()
        for i in range(len(PLANE)):
            plane_copy(i).wait_send()
        for slot in range(4):
            step_copy(slot, (STEPS - 1) % 2).wait_send()

    @pl.when(jnp.logical_not(is_home))
    def _():
        pl.semaphore_wait(go, 1)
        mag_copy(band).start()

    @pl.when(moves)
    def _():
        @pl.when(band == teller)
        def _():
            table_copy(1, band).wait_send()

        table_copy(0, band).wait_send()
        table_copy(2, band).wait_send()
        for c in range(CHUNKS):
            for i in range(2):
                ship_copy(i, band, c).wait_send()
        mag_copy(band).wait_send()
        fin_copy(0).wait_recv()

    @pl.when(stays)
    def _():
        mine = pltpu.make_async_copy(fin.at[band], got, local.at[0])
        mine.start()
        mine.wait()

    out_ref[:, 0:256] = got[:, 0:256]
    pair = got[0:1, 256:384]
    out_ref[:, 256:512] = jnp.zeros((8, 256), F32)
    out_ref[0:1, 256:384] = jnp.where(band % 2 == 0, pair, pltpu.roll(pair, OWN, 1))

    whole(line, line_recv).wait()
    total = jnp.sum(line[...].reshape(4, 128), axis=0, keepdims=True)
    total = pltpu.roll(total, (128 - band * SWEEPS) % 128, 1)
    out_ref[0:1, 384:512] = total * (1.0 / (OBS * STARS * TILES))

    @pl.when(is_home)
    def _():
        for slot in range(BANDS):

            @pl.when(jnp.logical_not(owns(slot)))
            def _():
                fin_copy(slot).wait_send()

        for i in range(len(LINE)):
            line_copy(i).wait_send()


def solve(color_terms, m, w, s, owner, colors, lists):
    vmem = pl.BlockSpec(memory_space=pltpu.VMEM)
    hbm = pl.BlockSpec(memory_space=pl.ANY)
    dma = pltpu.SemaphoreType.DMA
    return pl.pallas_call(
        solve_kernel,
        out_shape=pltpu.VMEM((8, 512), F32),
        in_specs=[hbm] * 7,
        out_specs=vmem,
        scratch_shapes=[
            pltpu.SMEM(color_terms.shape, F32),
            pltpu.VMEM((OBS, STARS), F32),
            pltpu.VMEM((OBS, STARS), F32),
            pltpu.VMEM((OBS, STARS), jnp.int32),
            pltpu.VMEM(owner.shape, jnp.int32),
            pltpu.VMEM(colors.shape, jnp.int32),
            pltpu.VMEM(lists.shape, jnp.int32),
            pltpu.VMEM((BLOCKS, ROWS), F32),
            pltpu.VMEM((BANDS, BLOCKS, ROWS), F32),
            pltpu.VMEM((8, 128), F32),
            pltpu.VMEM((8, 384), F32),
            pltpu.VMEM((BANDS, OBS, STARS), F32),
            pltpu.VMEM((BANDS, OBS, STARS), F32),
            pltpu.VMEM((BANDS, OBS, STARS), jnp.int32),
            pltpu.VMEM((BANDS, BLOCKS, ROWS), F32),
            pltpu.VMEM((BANDS, 8, 128), F32),
            pltpu.VMEM((8, 384), F32),
            pltpu.VMEM((BANDS, BLOCKS * LIST, ROWS), F32),
            pltpu.VMEM((2, BANDS, BLOCKS * LIST, WIDE), BF16),
            pltpu.VMEM((WIDE, WIDE), F32),
            pltpu.VMEM((3, 128, 512), BF16),
            pltpu.VMEM((2, 6, 1, 128), F32),
            pltpu.VMEM((2, 4, 6, 1, 128), F32),
            pltpu.VMEM((2, 6, 1, 128), F32),
            pltpu.VMEM((2, 4, 6, 1, 128), F32),
            pltpu.VMEM((BANDS, 8, 384), F32),
            pltpu.VMEM((8, 384), F32),
            pltpu.VMEM((2, 1, 128), F32),
            pltpu.VMEM((16, 1, 128), F32),
            pltpu.VMEM((4, 1, 128), F32),
            dma((7,)),
            dma((BANDS - 1,)),
            dma((BANDS - 1,)),
            dma((2, CHUNKS)),
            dma((BANDS, 2, CHUNKS)),
            dma,
            dma((BANDS,)),
            dma((3,)),
            dma((BANDS, 3)),
            dma((5,)),
            dma((2, 4)),
            dma((2, 4)),
            dma((2, 4)),
            dma((2, 4)),
            dma((BANDS,)),
            dma,
            dma((len(PLANE),)),
            dma,
            dma((len(LINE),)),
            dma,
            pltpu.SemaphoreType.REGULAR,
        ],
        compiler_params=pltpu.CompilerParams(has_side_effects=True, collective_id=0),
        name="solve",
    )(color_terms, m, w, s, owner, colors, lists)


def unpack_kernel(out_ref, zp_ref, mags_ref, mis_ref):
    zp_ref[...] = out_ref[0:1, 256 : 256 + OWN]
    mis_ref[...] = out_ref[0:1, 384 : 384 + SWEEPS]
    for blk in range(BLOCKS):
        mags_ref[0:1, blk * ROWS : (blk + 1) * ROWS] = out_ref[blk : blk + 1, 0:ROWS]


def body(magnitudes, weights, slots, block_fields, owner, colors, color_terms):
    out = solve(
        color_terms, magnitudes[0], weights[0], slots[0],
        owner.reshape(-1, 128), colors.reshape(-1, 128), block_fields,
    )
    vmem = pl.BlockSpec(memory_space=pltpu.VMEM)
    out = pltpu.with_memory_space_constraint(out, pltpu.VMEM)
    zp, mags, misfit = pl.pallas_call(
        unpack_kernel,
        out_shape=(
            jax.ShapeDtypeStruct((1, OWN), F32),
            jax.ShapeDtypeStruct((1, STARS), F32),
            jax.ShapeDtypeStruct((1, SWEEPS), F32),
        ),
        in_specs=[vmem],
        out_specs=(vmem,) * 3,
        name="unpack",
    )(out)
    return zp, mags, misfit.T


def solution(mesh):
    in_specs = (
        P("band", None, "sky"),
        P("band", None, "sky"),
        P("band", None, "sky"),
        P("sky", None),
        P(),
        P(),
        P(),
    )
    out_specs = (P("band", "sky"), P("band", "sky"), P(None, "band"))
    return jax.shard_map(body, mesh=mesh, in_specs=in_specs, out_specs=out_specs, check_vma=False)
```

```python
import functools

import jax
import jax.numpy as jnp
from jax import lax
from jax.experimental import pallas as pl
from jax.experimental.pallas import tpu as pltpu
from jax.sharding import PartitionSpec as P

COLORS = 8
SWEEPS = 4
PRIOR_WEIGHT = 1.0

TILES = 64
BANDS = 4
OBS = 8
BLOCKS = 8
ROWS = 256
STARS = BLOCKS * ROWS
LIST = 32
OWN = 64
NEAR = 3 * OWN
CUTS = (0, 2, 4, 6, 8)
CHUNKS = len(CUTS) - 1
EARLY = 2
WIDE = BANDS * NEAR
STEPS = COLORS * SWEEPS
PLANE = [(i, j) for i in (2, 1, 3, 0) for j in (2, 1, 3, 0)][:-1]
LINE = [(k, c) for k in (4, 3, 5, 2, 6, 1, 7, 0) for c in (0, 1)][:-1]
MESH = pl.DeviceIdType.MESH
HIGH = lax.Precision.HIGHEST
F32 = jnp.float32
BF16 = jnp.bfloat16


def home_of(tile):
    half = tile // 32
    row = tile // 8
    y = row % 4
    z = tile % 8
    leg = z // 4
    y_new = y + half * (3 - 2 * y)
    z_new = z + leg * (7 - 2 * z)
    x_lo = (1 - half + row + leg) % 2
    return half * 32 + y_new * 8 + z_new, x_lo * 2 + 1


def tile_at(sky, band):
    half = sky // 32
    y_new = (sky // 8) % 4
    z_new = sky % 8
    y = y_new + half * (3 - 2 * y_new)
    row = half * 4 + y
    leg = (band // 2 + 1 + half + row) % 2
    z = z_new + leg * (7 - 2 * z_new)
    is_home = (band % 2 == 1) & (z_new < 4)
    return is_home, (row * 8 + z) % TILES


def iota(shape, dim):
    return lax.broadcasted_iota(jnp.int32, shape, dim)


def as_column(row, count):
    eye = iota((count, 128), 0) == iota((count, 128), 1)
    full = jnp.broadcast_to(row, (count, 128))
    return jnp.sum(jnp.where(eye, full, 0.0), axis=1, keepdims=True)


def as_row(col, shift):
    n = col.shape[0]
    hit = iota((n, 128), 1) == iota((n, 128), 0) + shift
    return jnp.sum(jnp.where(hit, col, 0.0), axis=0, keepdims=True)


def split(x, terms):
    parts = []
    for _ in range(terms - 1):
        part = x.astype(BF16)
        parts.append(part)
        x = x - part.astype(F32)
    return parts + [x.astype(BF16)]


def tile_tables(tile, own_ref, col_ref, lst_ref, near_ref):
    rows = own_ref.shape[0]
    until = jnp.where(iota((128, 128), 0) <= iota((128, 128), 1), 1.0, 0.0).astype(BF16)
    before = jnp.where(iota((rows, rows), 1) < iota((rows, rows), 0), 1.0, 0.0).astype(BF16)
    number = (iota((rows, 128), 0) * 128 + iota((rows, 128), 1)).astype(F32)
    shade = col_ref[...].astype(F32)
    rank_at = iota((OWN, 128), 0).astype(F32)
    for tr in range(3):
        mine = own_ref[...] == (tile + tr - 1 + TILES) % TILES
        one = jnp.where(mine, 1.0, 0.0)
        inside = jnp.dot(one.astype(BF16), until, preferred_element_type=F32)
        above = jnp.dot(before, one.astype(BF16), preferred_element_type=F32)
        above = jnp.sum(above, axis=1, keepdims=True)
        rank = jnp.where(mine, inside + above - 1.0, -1.0)
        ids = jnp.zeros((OWN, 128), F32)
        cols = jnp.zeros((OWN, 128), F32)
        for i in range(rows):
            hit = rank[i : i + 1] == rank_at
            ids = ids + jnp.where(hit, number[i : i + 1], 0.0)
            cols = cols + jnp.where(hit, shade[i : i + 1], 0.0)
        for value, at in ((ids, 0), (cols, 128)):
            col = jnp.sum(value, axis=1, keepdims=True)
            row = as_row(col, 0) + as_row(col, OWN)
            near_ref[2 * tr : 2 * tr + 1, at : at + 128] = row
            near_ref[2 * tr + 1 : 2 * tr + 2, at : at + 128] = row
    near_ref[6:8, 128:256] = jnp.zeros((2, 128), F32)
    listed = lst_ref[...].astype(F32)
    near_ref[:, 256:384] = jnp.concatenate([listed] * BANDS, axis=1)
    for h in range(2):
        row = [listed[i : i + 1] for i in range(4 * h, 4 * h + 4)]
        near_ref[6 + h : 7 + h, 0:128] = jnp.concatenate(row, axis=1)


def star_means(m_ref, w_ref, mean_ref):
    for blk in range(BLOCKS):
        cols = slice(blk * ROWS, (blk + 1) * ROWS)
        top = jnp.sum(w_ref[:, cols] * m_ref[:, cols], axis=0, keepdims=True)
        mean_ref[blk : blk + 1, :] = top / jnp.sum(w_ref[:, cols], axis=0, keepdims=True)


def list_sums(m_ref, w_ref, s_ref, pred, aux_ref):
    entries = iota((LIST, ROWS), 0)
    rows = [jnp.zeros((1, 128), F32) for _ in range(4)]
    for blk in range(BLOCKS):
        cols = slice(blk * ROWS, (blk + 1) * ROWS)
        acc = jnp.zeros((LIST, ROWS), F32)
        wts = jnp.zeros((LIST, ROWS), F32)
        for k in range(OBS):
            hit = s_ref[k : k + 1, cols] == entries
            wk = w_ref[k : k + 1, cols]
            wts = wts + jnp.where(hit, wk, 0.0)
            acc = acc + jnp.where(hit, wk * (m_ref[k : k + 1, cols] - pred[blk : blk + 1]), 0.0)
        h, at = blk // 4, (blk % 4) * LIST
        rows[h] = rows[h] + as_row(jnp.sum(acc, axis=1, keepdims=True), at)
        rows[2 + h] = rows[2 + h] + as_row(jnp.sum(wts, axis=1, keepdims=True), at)
    aux_ref[...] = jnp.concatenate(rows + [jnp.zeros((4, 128), F32)], axis=0)


def solve_kernel(
    ct_hbm, m_hbm, w_hbm, s_hbm, own_hbm, col_hbm, lst_hbm,
    out_ref,
    ct_ref, m_ref, w_ref, s_ref, own_ref, col_ref, lst_ref,
    mean, mates, aux, near, bm, bw, bs, ba, bt, bn, u_ref, r_ref, mt_ref, pick2_ref,
    first_out, first_in, out_buf, in_buf, fin, got, row_buf, plane, line,
    load_sem, mate_send, mate_recv, ship_send, ship_recv, mag_send, mag_recv, tab_send, tab_recv, local,
    first_send, first_recv, send, recv,
    fin_send, fin_recv, plane_send, plane_recv, line_send, line_recv, go,
):
    sky = lax.axis_index("sky")
    band = lax.axis_index("band")
    home_sky, home_band = home_of(sky)
    stays = (home_sky == sky) & (home_band == band)
    moves = jnp.logical_not(stays)
    is_home, tile = tile_at(sky, band)
    places = [home_of((tile + d + TILES) % TILES) for d in (1, -1, 2, -2)]

    def owns(slot):
        return (tile == sky) & (band == slot)

    barrier = pltpu.get_barrier_semaphore()
    mates_of = [(band + i) % BANDS for i in range(1, BANDS)]
    for mate in mates_of:
        pl.semaphore_signal(barrier, inc=1, device_id=(sky, mate), device_id_type=MESH)

    @pl.when(moves)
    def _():
        pl.semaphore_signal(barrier, inc=1, device_id=(home_sky, home_band), device_id_type=MESH)

    @pl.when(is_home)
    def _():
        for place in places:
            pl.semaphore_signal(barrier, inc=1, device_id=place, device_id_type=MESH)
        for slot in range(BANDS):

            @pl.when(jnp.logical_not(owns(slot)))
            def _():
                pl.semaphore_signal(barrier, inc=1, device_id=(tile, slot), device_id_type=MESH)

    loads = [
        pltpu.make_async_copy(src, dst, load_sem.at[i])
        for i, (src, dst) in enumerate(
            (
                (w_hbm, w_ref), (s_hbm, s_ref), (m_hbm, m_ref),
                (own_hbm, own_ref), (col_hbm, col_ref), (lst_hbm, lst_ref), (ct_hbm, ct_ref),
            )
        )
    ]
    for load in loads:
        load.start()
    for load in loads[:2]:
        load.wait()

    @pl.when(is_home & moves)
    def _():
        pl.semaphore_wait(barrier, 12)

    @pl.when(is_home & stays)
    def _():
        pl.semaphore_wait(barrier, 10)

    @pl.when(jnp.logical_not(is_home))
    def _():
        pl.semaphore_wait(barrier, 4)

    def chunk(ref, slot, c):
        at = pl.ds(CUTS[c] * ROWS, (CUTS[c + 1] - CUTS[c]) * ROWS)
        return ref.at[:, at] if slot is None else ref.at[slot, :, at]

    def ship_copy(i, slot, c):
        src, dst = ((w_ref, bw), (s_ref, bs))[i]
        return pltpu.make_async_remote_copy(
            src_ref=chunk(src, None, c),
            dst_ref=chunk(dst, slot, c),
            send_sem=ship_send.at[i, c],
            recv_sem=ship_recv.at[slot, i, c],
            device_id=(home_sky, home_band),
            device_id_type=MESH,
        )

    def mag_copy(slot):
        return pltpu.make_async_remote_copy(
            src_ref=m_ref,
            dst_ref=bm.at[slot],
            send_sem=mag_send,
            recv_sem=mag_recv.at[slot],
            device_id=(home_sky, home_band),
            device_id_type=MESH,
        )

    def mate_copy(i):
        return pltpu.make_async_remote_copy(
            src_ref=mean,
            dst_ref=mates.at[band],
            send_sem=mate_send.at[i],
            recv_sem=mate_recv.at[i],
            device_id=(sky, mates_of[i]),
            device_id_type=MESH,
        )

    def table_copy(i, slot):
        src, dst = ((mean, ba.at[slot]), (near, bn), (aux, bt.at[slot]))[i]
        return pltpu.make_async_remote_copy(
            src_ref=src,
            dst_ref=dst,
            send_sem=tab_send.at[i],
            recv_sem=tab_recv.at[slot, i],
            device_id=(home_sky, home_band),
            device_id_type=MESH,
        )

    teller = 0

    @pl.when(moves)
    def _():
        for i in range(2):
            ship_copy(i, band, 0).start()

    loads[2].wait()
    star_means(m_ref, w_ref, mean)
    for i in range(BANDS - 1):
        mate_copy(i).start()
    keep = pltpu.make_async_copy(mean, mates.at[band], local.at[4])
    keep.start()

    for load in loads[3:]:
        load.wait()
    tile_tables(sky, own_ref, col_ref, lst_ref, near)

    @pl.when(moves)
    def _():
        @pl.when(band == teller)
        def _():
            table_copy(1, band).start()

        for c in range(1, EARLY):
            for i in range(2):
                ship_copy(i, band, c).start()

    mix = []
    for b in range(BANDS):
        total = ct_ref[b, 0]
        for b2 in range(1, BANDS):
            total = total + ct_ref[b, b2]
        mix.append([ct_ref[b, b2] + (1.0 - total if b == b2 else 0.0) for b2 in range(BANDS)])

    keep.wait()
    for i in range(BANDS - 1):
        mate_copy(i).wait_recv()
    pred = jnp.zeros((BLOCKS, ROWS), F32)
    for b2 in range(BANDS):
        factor = mix[0][b2]
        for b in range(1, BANDS):
            factor = jnp.where(band == b, mix[b][b2], factor)
        pred = pred + factor * mates[b2]
    list_sums(m_ref, w_ref, s_ref, pred, aux)

    @pl.when(moves)
    def _():
        table_copy(2, band).start()
        for c in range(EARLY, CHUNKS):
            for i in range(2):
                ship_copy(i, band, c).start()
        table_copy(0, band).start()

    @pl.when(stays)
    def _():
        copies = [
            pltpu.make_async_copy(mean, ba.at[band], local.at[0]),
            pltpu.make_async_copy(w_ref, bw.at[band], local.at[1]),
            pltpu.make_async_copy(s_ref, bs.at[band], local.at[2]),
            pltpu.make_async_copy(m_ref, bm.at[band], local.at[3]),
            pltpu.make_async_copy(aux, bt.at[band], local.at[4]),
        ]
        for copy in copies:
            copy.start()
        for copy in copies:
            copy.wait()

    for i in range(BANDS - 1):
        mate_copy(i).wait_send()

    def await_tables():
        table_copy(1, teller).wait_recv()

    def await_sums():
        for slot in range(BANDS):

            @pl.when(jnp.logical_not(owns(slot)))
            def _():
                table_copy(2, slot).wait_recv()

    def await_chunk(c):
        for slot in range(BANDS):

            @pl.when(jnp.logical_not(owns(slot)))
            def _():
                for i in range(2):
                    ship_copy(i, slot, c).wait_recv()

    def build():
        row_band = iota((128, 128), 0) // LIST
        lane_list = iota((128, 128), 1) // LIST
        lane_own = iota((128, 128), 1) // OWN
        mixes = jnp.zeros((128, 128), F32)
        for b2 in range(BANDS):
            for b in range(BANDS):
                mixes = jnp.where((row_band == b2) & (lane_list == b), mix[b][b2], mixes)
        entries = iota((LIST, ROWS), 0)
        await_tables()
        pick = []
        for tr in range(3):
            col = as_column(bn[2 * tr : 2 * tr + 1, 0:128], OWN)
            one = jnp.concatenate(
                [jnp.where(col == bn[6 + h : 7 + h, 0:128], 1.0, 0.0) for h in range(2)], axis=1
            ).astype(BF16)
            none = jnp.zeros((OWN, 256), BF16)
            pick2_ref[tr, 0:OWN, 0:256] = one
            pick2_ref[tr, OWN:128, 0:256] = none
            pick2_ref[tr, 0:OWN, 256:512] = none
            pick2_ref[tr, OWN:128, 256:512] = one
            pick.append(one)
        pick = jnp.concatenate(pick, axis=0)
        for blk in range(BLOCKS):
            if blk in CUTS:
                await_chunk(CUTS.index(blk))
            if blk == CUTS[-2]:
                for slot in range(BANDS):

                    @pl.when(jnp.logical_not(owns(slot)))
                    def _():
                        pl.semaphore_signal(go, inc=1, device_id=(tile, slot), device_id_type=MESH)

            cols = slice(blk * ROWS, (blk + 1) * ROWS)
            wide, scaled = [], []
            for b in range(BANDS):
                acc = jnp.zeros((LIST, ROWS), F32)
                for k in range(OBS):
                    wk = bw[b, k : k + 1, cols]
                    acc = acc + jnp.where(bs[b, k : k + 1, cols] == entries, wk, 0.0)
                star_w = jnp.sum(bw[b, :, cols], axis=0, keepdims=True)
                wide.append(acc)
                scaled.append(acc * (1.0 / star_w))
                u_ref[b, blk * LIST : (blk + 1) * LIST, :] = scaled[b]
            w_hi, w_lo = split(jnp.concatenate(wide, axis=0), 2)
            u_hi, u_lo = split(jnp.concatenate(scaled, axis=0), 2)
            dims = (((1,), (1,)), ((), ()))
            both = lax.dot_general(
                jnp.concatenate([u_hi, u_lo], axis=0), w_hi, dims, preferred_element_type=F32
            )
            gt = both[0:128] + both[128:256]
            gt = gt + lax.dot_general(u_hi, w_lo, dims, preferred_element_type=F32)
            lhs = jnp.concatenate(split(gt * mixes, 2), axis=0)
            col = as_column(bn[blk : blk + 1, 256:384], 128)
            for q in range(6):
                hit = (col == bn[q : q + 1, 0:128]) & (row_band == lane_own + 2 * (q % 2))
                moved = jnp.dot(
                    lhs, jnp.where(hit, 1.0, 0.0).astype(BF16), preferred_element_type=F32
                ).astype(BF16)
                for i in range(2):
                    for b2 in range(BANDS):
                        at = i * 128 + b2 * LIST
                        r_ref[
                            i, b2, blk * LIST : (blk + 1) * LIST, q * 128 : (q + 1) * 128
                        ] = moved[at : at + LIST]
            if blk == CUTS[EARLY] - 1:
                await_sums()
                first_sums(pick)
            if blk in (3, 7):
                at = slice((blk - 3) * LIST, (blk + 1) * LIST)
                for b2 in range(BANDS):
                    total = jnp.dot(pick[:, at], r_ref[0, b2, at, :], preferred_element_type=F32)
                    total = total + jnp.dot(pick[:, at], r_ref[1, b2, at, :], preferred_element_type=F32)
                    rows = slice(b2 * NEAR, (b2 + 1) * NEAR)
                    mt_ref[rows, :] = total if blk == 3 else mt_ref[rows, :] + total

    def first_sums(pick):
        rows = [jnp.concatenate([bt[b, h : h + 1, :] for h in range(2)], axis=1) for b in range(BANDS)]
        rows += [jnp.concatenate([bt[b, h : h + 1, :] for h in (2, 3)], axis=1) for b in range(BANDS)]
        terms = jnp.concatenate(split(jnp.concatenate(rows, axis=0), 3), axis=0)
        sums = lax.dot_general(terms, pick, (((1,), (1,)), ((), ())), preferred_element_type=F32)
        sums = sums[0:8] + sums[8:16] + sums[16:24]
        for i in range(2):
            for q in range(6):
                tr, b = q // 2, 2 * (q % 2)
                at = slice(tr * OWN, (tr + 1) * OWN)
                low, high = i * BANDS + b, i * BANDS + b + 1
                first_out[i, q] = jnp.concatenate(
                    [sums[low : low + 1, at], sums[high : high + 1, at]], axis=1
                )
        for i in range(2):
            for slot in (2, 3, 0, 1):
                first_copy(slot, i).start()
    def first_copy(slot, i):
        return pltpu.make_async_remote_copy(
            src_ref=first_out.at[i],
            dst_ref=first_in.at[i, slot],
            send_sem=first_send.at[i, slot],
            recv_sem=first_recv.at[i, slot],
            device_id=places[slot],
            device_id_type=MESH,
        )

    part_of = (pl.ds(2, 4), pl.ds(0, 4), pl.ds(4, 2), pl.ds(0, 2))

    def step_copy(slot, p):
        return pltpu.make_async_remote_copy(
            src_ref=out_buf.at[p, part_of[slot]],
            dst_ref=in_buf.at[p, slot, part_of[slot]],
            send_sem=send.at[p, slot],
            recv_sem=recv.at[p, slot],
            device_id=places[slot],
            device_id_type=MESH,
        )

    below, above, far_below, far_above = range(4)

    def combine_mid(own, got):
        return [own[q] + got(below, q + 2) + got(above, q - 2) for q in (2, 3)]

    def combine_rest(own, got):
        low = [own[q] + got(below, q + 2) + got(far_below, q + 4) for q in (0, 1)]
        top = [own[q] + got(above, q - 2) + got(far_above, q - 4) for q in (4, 5)]
        return low, top

    def columns(row):
        eye = iota((128, 128), 0) == iota((128, 128), 1)
        full = jnp.where(eye, jnp.broadcast_to(row, (128, 128)), 0.0)
        return jnp.sum(full, axis=1, keepdims=True)

    def pull(accs, pieces, cols):
        for r, col in cols.items():
            for half in range(2):
                b = (r % 2) * 2 + half
                base = b * NEAR + (r // 2) * OWN
                for i in range(0, OWN, 8):
                    at = half * OWN + i
                    c = col[at : at + 8, :]
                    for j, q in enumerate(pieces):
                        accs[j] = accs[j] + mt_ref[base + i : base + i + 8, q * 128 : (q + 1) * 128] * c
        return accs

    outer, inner = (0, 1, 4, 5), (2, 3)

    def evaluate(n, z, last):
        total = jnp.zeros((8, 512), F32)
        for tr in range(3):
            pair = jnp.concatenate([z[2 * tr], z[2 * tr + 1]], axis=0)
            lhs = jnp.concatenate(split(pair, 3) + [jnp.zeros((2, 128), BF16)], axis=0)
            total = total + jnp.dot(lhs, pick2_ref[tr], preferred_element_type=F32)
        total = total[0:2] + total[2:4] + total[4:6]
        means, tables = [], []
        for b in range(BANDS):
            rows = []
            tables.append([])
            for h in range(2):
                at = (b % 2) * 256 + h * 128
                row = total[b // 2 : b // 2 + 1, at : at + 128]
                tables[b].append(jnp.broadcast_to(row, (8, 128)))
                col = columns(row)
                for i in range(4):
                    blk = h * 4 + i
                    value = u_ref[b, blk * LIST : (blk + 1) * LIST, :] * col[i * LIST : (i + 1) * LIST, :]
                    rows.append(jnp.sum(value, axis=0, keepdims=True))
            means.append(ba[b] - jnp.concatenate(rows, axis=0))
        if last:
            for b in range(BANDS):
                fin[b, :, 0:ROWS] = means[b]
                fin[b, 0:1, 256:384] = z[2 + b // 2]
                fin[b, 1:8, 256:384] = jnp.zeros((7, 128), F32)
            for slot in range(BANDS):

                @pl.when(jnp.logical_not(owns(slot)))
                def _():
                    fin_copy(slot).start()

        lane = iota((1, 128), 1)
        found = jnp.zeros((1, 128), F32)
        for b in range(BANDS):
            pred = mix[b][0] * means[0]
            for b2 in range(1, BANDS):
                pred = pred + mix[b][b2] * means[b2]
            acc = jnp.zeros((8, 128), F32)
            for blk in range(BLOCKS):
                for half in range(2):
                    at = blk * ROWS + half * 128
                    idx = bs[b, :, at : at + 128] + (blk % 4) * LIST
                    picked = jnp.take_along_axis(tables[b][blk // 4], idx, axis=1)
                    left = bm[b, :, at : at + 128] - pred[blk : blk + 1, half * 128 : half * 128 + 128]
                    left = left - picked
                    acc = acc + bw[b, :, at : at + 128] * left * left
            value = jnp.sum(jnp.sum(acc, axis=0, keepdims=True), axis=1, keepdims=True)
            found = jnp.where(lane == n + b * SWEEPS, value, found)
        row_buf[0] = row_buf[0] + found

    def fin_copy(slot):
        return pltpu.make_async_remote_copy(
            src_ref=fin.at[slot],
            dst_ref=got,
            send_sem=fin_send.at[slot],
            recv_sem=fin_recv,
            device_id=(tile, slot),
            device_id_type=MESH,
        )

    x = (sky // 32) * 2 + band // 2
    y = (sky // 8) % 4
    z_at = sky % 8

    def core_at(dx, dy, dz, core):
        x_to, y_to, z_to = (x + dx) % 4, (y + dy) % 4, (z_at + dz) % 8
        return (x_to // 2) * 32 + y_to * 8 + z_to, (x_to % 2) * 2 + core

    def plane_copy(i):
        return pltpu.make_async_remote_copy(
            src_ref=row_buf.at[0],
            dst_ref=plane.at[x * 4 + y],
            send_sem=plane_send.at[i],
            recv_sem=plane_recv,
            device_id=core_at(PLANE[i][0], PLANE[i][1], 0, 1),
            device_id_type=MESH,
        )

    def line_copy(i):
        return pltpu.make_async_remote_copy(
            src_ref=row_buf.at[1],
            dst_ref=line.at[z_at % 4],
            send_sem=line_send.at[i],
            recv_sem=line_recv,
            device_id=core_at(0, 0, LINE[i][0], LINE[i][1]),
            device_id_type=MESH,
        )

    def whole(ref, sem):
        return pltpu.make_async_copy(ref, ref, sem)

    @pl.when(is_home)
    def _():
        build()
        for i in range(2):
            for slot in range(4):
                first_copy(slot, i).wait()
        start = []
        for i in range(2):
            own = [first_out[i, q] for q in range(6)]
            low, top = combine_rest(own, lambda s, q: first_in[i, s, q])
            start.append(low + combine_mid(own, lambda s, q: first_in[i, s, q]) + top)
        known, dens = start
        scale = [1.0 / (d + PRIOR_WEIGHT) for d in dens]
        colors = [bn[q : q + 1, 128:256] for q in range(6)]
        zero = jnp.zeros((1, 128), F32)
        z = [jnp.where(colors[q] == 0.0, known[q] * scale[q], zero) for q in range(6)]
        cols = {q: columns(z[q]) for q in range(6)}
        for pieces, slots in ((outer, (2, 3)), (inner, (0, 1))):
            accs = pull([jnp.zeros((8, 128), F32) for _ in pieces], pieces, cols)
            for j, q in enumerate(pieces):
                out_buf[1, q] = jnp.sum(accs[j], axis=0, keepdims=True)
            for slot in slots:
                step_copy(slot, 1).start()
        row_buf[0] = zero

        def renew(q, color, pulled, old):
            return jnp.where(colors[q] == color, (known[q] + pulled) * scale[q], old)

        def absorb(s, z, then):
            p = s % 2
            color = (s % COLORS).astype(F32) if not isinstance(s, int) else float(s % COLORS)
            own = [out_buf[p, q] for q in range(6)]
            take = lambda i, q: in_buf[p, i, q]
            z = list(z)
            for slot in (0, 1):
                step_copy(slot, p).wait_recv()
            mid = combine_mid(own, take)
            for q in inner:
                z[q] = renew(q, color, mid[q - 2], z[q])
            accs = None
            if then:
                cols = {q: columns(z[q]) for q in inner}
                accs = pull([jnp.zeros((8, 128), F32) for _ in range(6)], range(6), cols)
            for slot in (2, 3):
                step_copy(slot, p).wait_recv()
            low, top = combine_rest(own, take)
            for j, q in enumerate(outer):
                z[q] = renew(q, color, (low + top)[j], z[q])
            return z, accs

        def step(s, z):
            p = s % 2

            @pl.when((s == 2) & moves)
            def _():
                pl.semaphore_wait(go, 1)
                mag_copy(band).start()

            @pl.when(s % COLORS == 0)
            def _():
                @pl.when(s == COLORS)
                def _():
                    for slot in range(BANDS):

                        @pl.when(jnp.logical_not(owns(slot)))
                        def _():
                            table_copy(0, slot).wait_recv()
                            mag_copy(slot).wait_recv()

                evaluate(s // COLORS - 1, z, False)

            z, accs = absorb(s, z, True)
            cols = {q: columns(z[q]) for q in outer}
            far = pull([accs[q] for q in outer], outer, cols)
            for j, q in enumerate(outer):
                out_buf[1 - p, q] = jnp.sum(far[j], axis=0, keepdims=True)
            for slot in (2, 3):
                step_copy(slot, 1 - p).start()
            near_accs = pull([accs[q] for q in inner], inner, cols)
            for j, q in enumerate(inner):
                out_buf[1 - p, q] = jnp.sum(near_accs[j], axis=0, keepdims=True)
            for slot in (0, 1):
                step_copy(slot, 1 - p).start()
            for slot in range(4):
                step_copy(slot, p).wait_send()
            return tuple(z)

        z = lax.fori_loop(1, STEPS - 1, step, tuple(z))
        z, _ = absorb(STEPS - 1, z, False)
        evaluate(SWEEPS - 1, z, True)
        for i in range(len(PLANE)):
            plane_copy(i).start()
        mine = pltpu.make_async_copy(row_buf.at[0], plane.at[x * 4 + y], plane_recv)
        mine.start()
        whole(plane, plane_recv).wait()
        row_buf[1] = jnp.sum(plane[...].reshape(16, 128), axis=0, keepdims=True)
        for i in range(len(LINE)):
            line_copy(i).start()
        mine = pltpu.make_async_copy(row_buf.at[1], line.at[z_at % 4], line_recv)
        mine.start()
        for i in range(len(PLANE)):
            plane_copy(i).wait_send()
        for slot in range(4):
            step_copy(slot, (STEPS - 1) % 2).wait_send()

    @pl.when(jnp.logical_not(is_home))
    def _():
        pl.semaphore_wait(go, 1)
        mag_copy(band).start()

    @pl.when(moves)
    def _():
        @pl.when(band == teller)
        def _():
            table_copy(1, band).wait_send()

        table_copy(0, band).wait_send()
        table_copy(2, band).wait_send()
        for c in range(CHUNKS):
            for i in range(2):
                ship_copy(i, band, c).wait_send()
        mag_copy(band).wait_send()
        fin_copy(0).wait_recv()

    @pl.when(stays)
    def _():
        mine = pltpu.make_async_copy(fin.at[band], got, local.at[0])
        mine.start()
        mine.wait()

    out_ref[:, 0:256] = got[:, 0:256]
    pair = got[0:1, 256:384]
    out_ref[:, 256:512] = jnp.zeros((8, 256), F32)
    out_ref[0:1, 256:384] = jnp.where(band % 2 == 0, pair, pltpu.roll(pair, OWN, 1))

    whole(line, line_recv).wait()
    total = jnp.sum(line[...].reshape(4, 128), axis=0, keepdims=True)
    total = pltpu.roll(total, (128 - band * SWEEPS) % 128, 1)
    out_ref[0:1, 384:512] = total * (1.0 / (OBS * STARS * TILES))

    @pl.when(is_home)
    def _():
        for slot in range(BANDS):

            @pl.when(jnp.logical_not(owns(slot)))
            def _():
                fin_copy(slot).wait_send()

        for i in range(len(LINE)):
            line_copy(i).wait_send()


def solve(color_terms, m, w, s, owner, colors, lists):
    vmem = pl.BlockSpec(memory_space=pltpu.VMEM)
    hbm = pl.BlockSpec(memory_space=pl.ANY)
    dma = pltpu.SemaphoreType.DMA
    return pl.pallas_call(
        solve_kernel,
        out_shape=pltpu.VMEM((8, 512), F32),
        in_specs=[hbm] * 7,
        out_specs=vmem,
        scratch_shapes=[
            pltpu.SMEM(color_terms.shape, F32),
            pltpu.VMEM((OBS, STARS), F32),
            pltpu.VMEM((OBS, STARS), F32),
            pltpu.VMEM((OBS, STARS), jnp.int32),
            pltpu.VMEM(owner.shape, jnp.int32),
            pltpu.VMEM(colors.shape, jnp.int32),
            pltpu.VMEM(lists.shape, jnp.int32),
            pltpu.VMEM((BLOCKS, ROWS), F32),
            pltpu.VMEM((BANDS, BLOCKS, ROWS), F32),
            pltpu.VMEM((8, 128), F32),
            pltpu.VMEM((8, 384), F32),
            pltpu.VMEM((BANDS, OBS, STARS), F32),
            pltpu.VMEM((BANDS, OBS, STARS), F32),
            pltpu.VMEM((BANDS, OBS, STARS), jnp.int32),
            pltpu.VMEM((BANDS, BLOCKS, ROWS), F32),
            pltpu.VMEM((BANDS, 8, 128), F32),
            pltpu.VMEM((8, 384), F32),
            pltpu.VMEM((BANDS, BLOCKS * LIST, ROWS), F32),
            pltpu.VMEM((2, BANDS, BLOCKS * LIST, WIDE), BF16),
            pltpu.VMEM((WIDE, WIDE), F32),
            pltpu.VMEM((3, 128, 512), BF16),
            pltpu.VMEM((2, 6, 1, 128), F32),
            pltpu.VMEM((2, 4, 6, 1, 128), F32),
            pltpu.VMEM((2, 6, 1, 128), F32),
            pltpu.VMEM((2, 4, 6, 1, 128), F32),
            pltpu.VMEM((BANDS, 8, 384), F32),
            pltpu.VMEM((8, 384), F32),
            pltpu.VMEM((2, 1, 128), F32),
            pltpu.VMEM((16, 1, 128), F32),
            pltpu.VMEM((4, 1, 128), F32),
            dma((7,)),
            dma((BANDS - 1,)),
            dma((BANDS - 1,)),
            dma((2, CHUNKS)),
            dma((BANDS, 2, CHUNKS)),
            dma,
            dma((BANDS,)),
            dma((3,)),
            dma((BANDS, 3)),
            dma((5,)),
            dma((2, 4)),
            dma((2, 4)),
            dma((2, 4)),
            dma((2, 4)),
            dma((BANDS,)),
            dma,
            dma((len(PLANE),)),
            dma,
            dma((len(LINE),)),
            dma,
            pltpu.SemaphoreType.REGULAR,
        ],
        compiler_params=pltpu.CompilerParams(has_side_effects=True, collective_id=0),
        name="solve",
    )(color_terms, m, w, s, owner, colors, lists)


def unpack_kernel(out_ref, zp_ref, mags_ref, mis_ref):
    zp_ref[...] = out_ref[0:1, 256 : 256 + OWN]
    mis_ref[...] = out_ref[0:1, 384 : 384 + SWEEPS]
    for blk in range(BLOCKS):
        mags_ref[0:1, blk * ROWS : (blk + 1) * ROWS] = out_ref[blk : blk + 1, 0:ROWS]


def body(magnitudes, weights, slots, block_fields, owner, colors, color_terms):
    out = solve(
        color_terms, magnitudes[0], weights[0], slots[0],
        owner.reshape(-1, 128), colors.reshape(-1, 128), block_fields,
    )
    vmem = pl.BlockSpec(memory_space=pltpu.VMEM)
    out = pltpu.with_memory_space_constraint(out, pltpu.VMEM)
    zp, mags, misfit = pl.pallas_call(
        unpack_kernel,
        out_shape=(
            jax.ShapeDtypeStruct((1, OWN), F32),
            jax.ShapeDtypeStruct((1, STARS), F32),
            jax.ShapeDtypeStruct((1, SWEEPS), F32),
        ),
        in_specs=[vmem],
        out_specs=(vmem,) * 3,
        name="unpack",
    )(out)
    return zp, mags, misfit.T


def solution(mesh):
    in_specs = (
        P("band", None, "sky"),
        P("band", None, "sky"),
        P("band", None, "sky"),
        P("sky", None),
        P(),
        P(),
        P(),
    )
    out_specs = (P("band", "sky"), P("band", "sky"), P(None, "band"))
    return jax.shard_map(body, mesh=mesh, in_specs=in_specs, out_specs=out_specs, check_vma=False)
```

```python
import functools

import jax
import jax.numpy as jnp
from jax import lax
from jax.experimental import pallas as pl
from jax.experimental.pallas import tpu as pltpu
from jax.sharding import PartitionSpec as P

COLORS = 8
SWEEPS = 4
PRIOR_WEIGHT = 1.0

TILES = 64
BANDS = 4
OBS = 8
BLOCKS = 8
ROWS = 256
STARS = BLOCKS * ROWS
LIST = 32
OWN = 64
NEAR = 3 * OWN
CUTS = (0, 2, 4, 6, 8)
CHUNKS = len(CUTS) - 1
EARLY = 2
WIDE = BANDS * NEAR
STEPS = COLORS * SWEEPS
PLANE = [(i, j) for i in (2, 1, 3, 0) for j in (2, 1, 3, 0)][:-1]
LINE = [(k, c) for k in (4, 3, 5, 2, 6, 1, 7, 0) for c in (0, 1)][:-1]
MESH = pl.DeviceIdType.MESH
HIGH = lax.Precision.HIGHEST
F32 = jnp.float32
BF16 = jnp.bfloat16


def home_of(tile):
    half = tile // 32
    row = tile // 8
    y = row % 4
    z = tile % 8
    leg = z // 4
    y_new = y + half * (3 - 2 * y)
    z_new = z + leg * (7 - 2 * z)
    x_lo = (1 - half + row + leg) % 2
    return half * 32 + y_new * 8 + z_new, x_lo * 2 + 1


def tile_at(sky, band):
    half = sky // 32
    y_new = (sky // 8) % 4
    z_new = sky % 8
    y = y_new + half * (3 - 2 * y_new)
    row = half * 4 + y
    leg = (band // 2 + 1 + half + row) % 2
    z = z_new + leg * (7 - 2 * z_new)
    is_home = (band % 2 == 1) & (z_new < 4)
    return is_home, (row * 8 + z) % TILES


def iota(shape, dim):
    return lax.broadcasted_iota(jnp.int32, shape, dim)


def as_column(row, count):
    eye = iota((count, 128), 0) == iota((count, 128), 1)
    full = jnp.broadcast_to(row, (count, 128))
    return jnp.sum(jnp.where(eye, full, 0.0), axis=1, keepdims=True)


def as_row(col, shift):
    n = col.shape[0]
    hit = iota((n, 128), 1) == iota((n, 128), 0) + shift
    return jnp.sum(jnp.where(hit, col, 0.0), axis=0, keepdims=True)


def split(x, terms):
    parts = []
    for _ in range(terms - 1):
        part = x.astype(BF16)
        parts.append(part)
        x = x - part.astype(F32)
    return parts + [x.astype(BF16)]


def tile_tables(tile, own_ref, col_ref, lst_ref, near_ref):
    rows = own_ref.shape[0]
    until = jnp.where(iota((128, 128), 0) <= iota((128, 128), 1), 1.0, 0.0).astype(BF16)
    before = jnp.where(iota((rows, rows), 1) < iota((rows, rows), 0), 1.0, 0.0).astype(BF16)
    number = (iota((rows, 128), 0) * 128 + iota((rows, 128), 1)).astype(F32)
    shade = col_ref[...].astype(F32)
    rank_at = iota((OWN, 128), 0).astype(F32)
    for tr in range(3):
        mine = own_ref[...] == (tile + tr - 1 + TILES) % TILES
        one = jnp.where(mine, 1.0, 0.0)
        inside = jnp.dot(one.astype(BF16), until, preferred_element_type=F32)
        above = jnp.dot(before, one.astype(BF16), preferred_element_type=F32)
        above = jnp.sum(above, axis=1, keepdims=True)
        rank = jnp.where(mine, inside + above - 1.0, -1.0)
        ids = jnp.zeros((OWN, 128), F32)
        cols = jnp.zeros((OWN, 128), F32)
        for i in range(rows):
            hit = rank[i : i + 1] == rank_at
            ids = ids + jnp.where(hit, number[i : i + 1], 0.0)
            cols = cols + jnp.where(hit, shade[i : i + 1], 0.0)
        for value, at in ((ids, 0), (cols, 128)):
            col = jnp.sum(value, axis=1, keepdims=True)
            row = as_row(col, 0) + as_row(col, OWN)
            near_ref[2 * tr : 2 * tr + 1, at : at + 128] = row
            near_ref[2 * tr + 1 : 2 * tr + 2, at : at + 128] = row
    near_ref[6:8, 128:256] = jnp.zeros((2, 128), F32)
    listed = lst_ref[...].astype(F32)
    near_ref[:, 256:384] = jnp.concatenate([listed] * BANDS, axis=1)
    for h in range(2):
        row = [listed[i : i + 1] for i in range(4 * h, 4 * h + 4)]
        near_ref[6 + h : 7 + h, 0:128] = jnp.concatenate(row, axis=1)


def star_means(m_ref, w_ref, mean_ref):
    for blk in range(BLOCKS):
        cols = slice(blk * ROWS, (blk + 1) * ROWS)
        top = jnp.sum(w_ref[:, cols] * m_ref[:, cols], axis=0, keepdims=True)
        mean_ref[blk : blk + 1, :] = top / jnp.sum(w_ref[:, cols], axis=0, keepdims=True)


def list_sums(m_ref, w_ref, s_ref, pred, aux_ref):
    entries = iota((LIST, ROWS), 0)
    rows = [jnp.zeros((1, 128), F32) for _ in range(4)]
    for blk in range(BLOCKS):
        cols = slice(blk * ROWS, (blk + 1) * ROWS)
        acc = jnp.zeros((LIST, ROWS), F32)
        wts = jnp.zeros((LIST, ROWS), F32)
        for k in range(OBS):
            hit = s_ref[k : k + 1, cols] == entries
            wk = w_ref[k : k + 1, cols]
            wts = wts + jnp.where(hit, wk, 0.0)
            acc = acc + jnp.where(hit, wk * (m_ref[k : k + 1, cols] - pred[blk : blk + 1]), 0.0)
        h, at = blk // 4, (blk % 4) * LIST
        rows[h] = rows[h] + as_row(jnp.sum(acc, axis=1, keepdims=True), at)
        rows[2 + h] = rows[2 + h] + as_row(jnp.sum(wts, axis=1, keepdims=True), at)
    aux_ref[...] = jnp.concatenate(rows + [jnp.zeros((4, 128), F32)], axis=0)


def solve_kernel(
    ct_hbm, m_hbm, w_hbm, s_hbm, own_hbm, col_hbm, lst_hbm,
    out_ref,
    ct_ref, m_ref, w_ref, s_ref, own_ref, col_ref, lst_ref,
    mean, mates, aux, near, bm, bw, bs, ba, bt, bn, u_ref, r_ref, mt_ref, pick2_ref,
    first_out, first_in, out_buf, in_buf, fin, got, row_buf, plane, line,
    load_sem, mate_send, mate_recv, ship_send, ship_recv, mag_send, mag_recv, tab_send, tab_recv, local,
    first_send, first_recv, send, recv,
    fin_send, fin_recv, plane_send, plane_recv, line_send, line_recv, go,
):
    sky = lax.axis_index("sky")
    band = lax.axis_index("band")
    home_sky, home_band = home_of(sky)
    stays = (home_sky == sky) & (home_band == band)
    moves = jnp.logical_not(stays)
    is_home, tile = tile_at(sky, band)
    places = [home_of((tile + d + TILES) % TILES) for d in (1, -1, 2, -2)]

    def owns(slot):
        return (tile == sky) & (band == slot)

    barrier = pltpu.get_barrier_semaphore()
    mates_of = [(band + i) % BANDS for i in range(1, BANDS)]
    for mate in mates_of:
        pl.semaphore_signal(barrier, inc=1, device_id=(sky, mate), device_id_type=MESH)

    @pl.when(moves)
    def _():
        pl.semaphore_signal(barrier, inc=1, device_id=(home_sky, home_band), device_id_type=MESH)

    @pl.when(is_home)
    def _():
        for place in places:
            pl.semaphore_signal(barrier, inc=1, device_id=place, device_id_type=MESH)
        for slot in range(BANDS):

            @pl.when(jnp.logical_not(owns(slot)))
            def _():
                pl.semaphore_signal(barrier, inc=1, device_id=(tile, slot), device_id_type=MESH)

    loads = [
        pltpu.make_async_copy(src, dst, load_sem.at[i])
        for i, (src, dst) in enumerate(
            (
                (w_hbm, w_ref), (s_hbm, s_ref), (m_hbm, m_ref),
                (own_hbm, own_ref), (col_hbm, col_ref), (lst_hbm, lst_ref), (ct_hbm, ct_ref),
            )
        )
    ]
    for load in loads:
        load.start()
    for load in loads[:2]:
        load.wait()

    @pl.when(is_home & moves)
    def _():
        pl.semaphore_wait(barrier, 12)

    @pl.when(is_home & stays)
    def _():
        pl.semaphore_wait(barrier, 10)

    @pl.when(jnp.logical_not(is_home))
    def _():
        pl.semaphore_wait(barrier, 4)

    def chunk(ref, slot, c):
        at = pl.ds(CUTS[c] * ROWS, (CUTS[c + 1] - CUTS[c]) * ROWS)
        return ref.at[:, at] if slot is None else ref.at[slot, :, at]

    def ship_copy(i, slot, c):
        src, dst = ((w_ref, bw), (s_ref, bs))[i]
        return pltpu.make_async_remote_copy(
            src_ref=chunk(src, None, c),
            dst_ref=chunk(dst, slot, c),
            send_sem=ship_send.at[i, c],
            recv_sem=ship_recv.at[slot, i, c],
            device_id=(home_sky, home_band),
            device_id_type=MESH,
        )

    def mag_copy(slot):
        return pltpu.make_async_remote_copy(
            src_ref=m_ref,
            dst_ref=bm.at[slot],
            send_sem=mag_send,
            recv_sem=mag_recv.at[slot],
            device_id=(home_sky, home_band),
            device_id_type=MESH,
        )

    def mate_copy(i):
        return pltpu.make_async_remote_copy(
            src_ref=mean,
            dst_ref=mates.at[band],
            send_sem=mate_send.at[i],
            recv_sem=mate_recv.at[i],
            device_id=(sky, mates_of[i]),
            device_id_type=MESH,
        )

    def table_copy(i, slot):
        src, dst = ((mean, ba.at[slot]), (near, bn), (aux, bt.at[slot]))[i]
        return pltpu.make_async_remote_copy(
            src_ref=src,
            dst_ref=dst,
            send_sem=tab_send.at[i],
            recv_sem=tab_recv.at[slot, i],
            device_id=(home_sky, home_band),
            device_id_type=MESH,
        )

    teller = 0

    @pl.when(moves)
    def _():
        for i in range(2):
            ship_copy(i, band, 0).start()

    loads[2].wait()
    star_means(m_ref, w_ref, mean)
    for i in range(BANDS - 1):
        mate_copy(i).start()
    keep = pltpu.make_async_copy(mean, mates.at[band], local.at[4])
    keep.start()

    for load in loads[3:]:
        load.wait()
    tile_tables(sky, own_ref, col_ref, lst_ref, near)

    @pl.when(moves)
    def _():
        @pl.when(band == teller)
        def _():
            table_copy(1, band).start()

        for c in range(1, EARLY):
            for i in range(2):
                ship_copy(i, band, c).start()

    mix = []
    for b in range(BANDS):
        total = ct_ref[b, 0]
        for b2 in range(1, BANDS):
            total = total + ct_ref[b, b2]
        mix.append([ct_ref[b, b2] + (1.0 - total if b == b2 else 0.0) for b2 in range(BANDS)])

    keep.wait()
    for i in range(BANDS - 1):
        mate_copy(i).wait_recv()
    pred = jnp.zeros((BLOCKS, ROWS), F32)
    for b2 in range(BANDS):
        factor = mix[0][b2]
        for b in range(1, BANDS):
            factor = jnp.where(band == b, mix[b][b2], factor)
        pred = pred + factor * mates[b2]
    list_sums(m_ref, w_ref, s_ref, pred, aux)

    @pl.when(moves)
    def _():
        table_copy(2, band).start()
        for c in range(EARLY, CHUNKS):
            for i in range(2):
                ship_copy(i, band, c).start()
        table_copy(0, band).start()

    @pl.when(stays)
    def _():
        copies = [
            pltpu.make_async_copy(mean, ba.at[band], local.at[0]),
            pltpu.make_async_copy(w_ref, bw.at[band], local.at[1]),
            pltpu.make_async_copy(s_ref, bs.at[band], local.at[2]),
            pltpu.make_async_copy(m_ref, bm.at[band], local.at[3]),
            pltpu.make_async_copy(aux, bt.at[band], local.at[4]),
        ]
        for copy in copies:
            copy.start()
        for copy in copies:
            copy.wait()

    for i in range(BANDS - 1):
        mate_copy(i).wait_send()

    def await_tables():
        table_copy(1, teller).wait_recv()

    def await_sums():
        for slot in range(BANDS):

            @pl.when(jnp.logical_not(owns(slot)))
            def _():
                table_copy(2, slot).wait_recv()

    def await_chunk(c):
        for slot in range(BANDS):

            @pl.when(jnp.logical_not(owns(slot)))
            def _():
                for i in range(2):
                    ship_copy(i, slot, c).wait_recv()

    def build():
        row_band = iota((128, 128), 0) // LIST
        lane_list = iota((128, 128), 1) // LIST
        lane_own = iota((128, 128), 1) // OWN
        mixes = jnp.zeros((128, 128), F32)
        for b2 in range(BANDS):
            for b in range(BANDS):
                mixes = jnp.where((row_band == b2) & (lane_list == b), mix[b][b2], mixes)
        entries = iota((LIST, ROWS), 0)
        await_tables()
        pick = []
        for tr in range(3):
            col = as_column(bn[2 * tr : 2 * tr + 1, 0:128], OWN)
            one = jnp.concatenate(
                [jnp.where(col == bn[6 + h : 7 + h, 0:128], 1.0, 0.0) for h in range(2)], axis=1
            ).astype(BF16)
            none = jnp.zeros((OWN, 256), BF16)
            pick2_ref[tr, 0:OWN, 0:256] = one
            pick2_ref[tr, OWN:128, 0:256] = none
            pick2_ref[tr, 0:OWN, 256:512] = none
            pick2_ref[tr, OWN:128, 256:512] = one
            pick.append(one)
        pick = jnp.concatenate(pick, axis=0)
        for blk in range(BLOCKS):
            if blk in CUTS:
                await_chunk(CUTS.index(blk))
            if blk == CUTS[-2]:
                for slot in range(BANDS):

                    @pl.when(jnp.logical_not(owns(slot)))
                    def _():
                        pl.semaphore_signal(go, inc=1, device_id=(tile, slot), device_id_type=MESH)

            cols = slice(blk * ROWS, (blk + 1) * ROWS)
            wide, scaled = [], []
            for b in range(BANDS):
                acc = jnp.zeros((LIST, ROWS), F32)
                for k in range(OBS):
                    wk = bw[b, k : k + 1, cols]
                    acc = acc + jnp.where(bs[b, k : k + 1, cols] == entries, wk, 0.0)
                star_w = jnp.sum(bw[b, :, cols], axis=0, keepdims=True)
                wide.append(acc)
                scaled.append(acc * (1.0 / star_w))
                u_ref[b, blk * LIST : (blk + 1) * LIST, :] = scaled[b]
            w_hi, w_lo = split(jnp.concatenate(wide, axis=0), 2)
            u_hi, u_lo = split(jnp.concatenate(scaled, axis=0), 2)
            dims = (((1,), (1,)), ((), ()))
            both = lax.dot_general(
                jnp.concatenate([u_hi, u_lo], axis=0), w_hi, dims, preferred_element_type=F32
            )
            gt = both[0:128] + both[128:256]
            gt = gt + lax.dot_general(u_hi, w_lo, dims, preferred_element_type=F32)
            lhs = jnp.concatenate(split(gt * mixes, 2), axis=0)
            col = as_column(bn[blk : blk + 1, 256:384], 128)
            for q in range(6):
                hit = (col == bn[q : q + 1, 0:128]) & (row_band == lane_own + 2 * (q % 2))
                moved = jnp.dot(
                    lhs, jnp.where(hit, 1.0, 0.0).astype(BF16), preferred_element_type=F32
                ).astype(BF16)
                for i in range(2):
                    for b2 in range(BANDS):
                        at = i * 128 + b2 * LIST
                        r_ref[
                            i, b2, blk * LIST : (blk + 1) * LIST, q * 128 : (q + 1) * 128
                        ] = moved[at : at + LIST]
            if blk == CUTS[EARLY] - 1:
                await_sums()
                first_sums(pick)
            if blk in (3, 7):
                at = slice((blk - 3) * LIST, (blk + 1) * LIST)
                for b2 in range(BANDS):
                    total = jnp.dot(pick[:, at], r_ref[0, b2, at, :], preferred_element_type=F32)
                    total = total + jnp.dot(pick[:, at], r_ref[1, b2, at, :], preferred_element_type=F32)
                    rows = slice(b2 * NEAR, (b2 + 1) * NEAR)
                    mt_ref[rows, :] = total if blk == 3 else mt_ref[rows, :] + total

    def first_sums(pick):
        rows = [jnp.concatenate([bt[b, h : h + 1, :] for h in range(2)], axis=1) for b in range(BANDS)]
        rows += [jnp.concatenate([bt[b, h : h + 1, :] for h in (2, 3)], axis=1) for b in range(BANDS)]
        terms = jnp.concatenate(split(jnp.concatenate(rows, axis=0), 3), axis=0)
        sums = lax.dot_general(terms, pick, (((1,), (1,)), ((), ())), preferred_element_type=F32)
        sums = sums[0:8] + sums[8:16] + sums[16:24]
        for i in range(2):
            for q in range(6):
                tr, b = q // 2, 2 * (q % 2)
                at = slice(tr * OWN, (tr + 1) * OWN)
                low, high = i * BANDS + b, i * BANDS + b + 1
                first_out[i, q] = jnp.concatenate(
                    [sums[low : low + 1, at], sums[high : high + 1, at]], axis=1
                )
        for i in range(2):
            for slot in (2, 3, 0, 1):
                first_copy(slot, i).start()
    def first_copy(slot, i):
        return pltpu.make_async_remote_copy(
            src_ref=first_out.at[i],
            dst_ref=first_in.at[i, slot],
            send_sem=first_send.at[i, slot],
            recv_sem=first_recv.at[i, slot],
            device_id=places[slot],
            device_id_type=MESH,
        )

    part_of = (pl.ds(2, 4), pl.ds(0, 4), pl.ds(4, 2), pl.ds(0, 2))

    def step_copy(slot, p):
        return pltpu.make_async_remote_copy(
            src_ref=out_buf.at[p, part_of[slot]],
            dst_ref=in_buf.at[p, slot, part_of[slot]],
            send_sem=send.at[p, slot],
            recv_sem=recv.at[p, slot],
            device_id=places[slot],
            device_id_type=MESH,
        )

    below, above, far_below, far_above = range(4)

    def combine_mid(own, got):
        return [own[q] + got(below, q + 2) + got(above, q - 2) for q in (2, 3)]

    def combine_rest(own, got):
        low = [own[q] + got(below, q + 2) + got(far_below, q + 4) for q in (0, 1)]
        top = [own[q] + got(above, q - 2) + got(far_above, q - 4) for q in (4, 5)]
        return low, top

    def columns(row):
        eye = iota((128, 128), 0) == iota((128, 128), 1)
        full = jnp.where(eye, jnp.broadcast_to(row, (128, 128)), 0.0)
        return jnp.sum(full, axis=1, keepdims=True)

    def pull(accs, pieces, cols):
        for r, col in cols.items():
            for half in range(2):
                b = (r % 2) * 2 + half
                base = b * NEAR + (r // 2) * OWN
                for i in range(0, OWN, 8):
                    at = half * OWN + i
                    c = col[at : at + 8, :]
                    for j, q in enumerate(pieces):
                        accs[j] = accs[j] + mt_ref[base + i : base + i + 8, q * 128 : (q + 1) * 128] * c
        return accs

    outer, inner = (0, 1, 4, 5), (2, 3)

    def evaluate(n, z, last):
        total = jnp.zeros((8, 512), F32)
        for tr in range(3):
            pair = jnp.concatenate([z[2 * tr], z[2 * tr + 1]], axis=0)
            lhs = jnp.concatenate(split(pair, 3) + [jnp.zeros((2, 128), BF16)], axis=0)
            total = total + jnp.dot(lhs, pick2_ref[tr], preferred_element_type=F32)
        total = total[0:2] + total[2:4] + total[4:6]
        means, tables = [], []
        for b in range(BANDS):
            rows = []
            tables.append([])
            for h in range(2):
                at = (b % 2) * 256 + h * 128
                row = total[b // 2 : b // 2 + 1, at : at + 128]
                tables[b].append(jnp.broadcast_to(row, (8, 128)))
                col = columns(row)
                for i in range(4):
                    blk = h * 4 + i
                    value = u_ref[b, blk * LIST : (blk + 1) * LIST, :] * col[i * LIST : (i + 1) * LIST, :]
                    rows.append(jnp.sum(value, axis=0, keepdims=True))
            means.append(ba[b] - jnp.concatenate(rows, axis=0))
        if last:
            for b in range(BANDS):
                fin[b, :, 0:ROWS] = means[b]
                fin[b, 0:1, 256:384] = z[2 + b // 2]
                fin[b, 1:8, 256:384] = jnp.zeros((7, 128), F32)
        lane = iota((1, 128), 1)
        found = jnp.zeros((1, 128), F32)
        for b in range(BANDS):
            pred = mix[b][0] * means[0]
            for b2 in range(1, BANDS):
                pred = pred + mix[b][b2] * means[b2]
            acc = jnp.zeros((8, 128), F32)
            for blk in range(BLOCKS):
                for half in range(2):
                    at = blk * ROWS + half * 128
                    idx = bs[b, :, at : at + 128] + (blk % 4) * LIST
                    picked = jnp.take_along_axis(tables[b][blk // 4], idx, axis=1)
                    left = bm[b, :, at : at + 128] - pred[blk : blk + 1, half * 128 : half * 128 + 128]
                    left = left - picked
                    acc = acc + bw[b, :, at : at + 128] * left * left
            value = jnp.sum(jnp.sum(acc, axis=0, keepdims=True), axis=1, keepdims=True)
            found = jnp.where(lane == n + b * SWEEPS, value, found)
        row_buf[0] = row_buf[0] + found

    def fin_copy(slot):
        return pltpu.make_async_remote_copy(
            src_ref=fin.at[slot],
            dst_ref=got,
            send_sem=fin_send.at[slot],
            recv_sem=fin_recv,
            device_id=(tile, slot),
            device_id_type=MESH,
        )

    x = (sky // 32) * 2 + band // 2
    y = (sky // 8) % 4
    z_at = sky % 8

    def core_at(dx, dy, dz, core):
        x_to, y_to, z_to = (x + dx) % 4, (y + dy) % 4, (z_at + dz) % 8
        return (x_to // 2) * 32 + y_to * 8 + z_to, (x_to % 2) * 2 + core

    def plane_copy(i):
        return pltpu.make_async_remote_copy(
            src_ref=row_buf.at[0],
            dst_ref=plane.at[x * 4 + y],
            send_sem=plane_send.at[i],
            recv_sem=plane_recv,
            device_id=core_at(PLANE[i][0], PLANE[i][1], 0, 1),
            device_id_type=MESH,
        )

    def line_copy(i):
        return pltpu.make_async_remote_copy(
            src_ref=row_buf.at[1],
            dst_ref=line.at[z_at % 4],
            send_sem=line_send.at[i],
            recv_sem=line_recv,
            device_id=core_at(0, 0, LINE[i][0], LINE[i][1]),
            device_id_type=MESH,
        )

    def whole(ref, sem):
        return pltpu.make_async_copy(ref, ref, sem)

    @pl.when(is_home)
    def _():
        build()
        for i in range(2):
            for slot in range(4):
                first_copy(slot, i).wait()
        start = []
        for i in range(2):
            own = [first_out[i, q] for q in range(6)]
            low, top = combine_rest(own, lambda s, q: first_in[i, s, q])
            start.append(low + combine_mid(own, lambda s, q: first_in[i, s, q]) + top)
        known, dens = start
        scale = [1.0 / (d + PRIOR_WEIGHT) for d in dens]
        colors = [bn[q : q + 1, 128:256] for q in range(6)]
        zero = jnp.zeros((1, 128), F32)
        z = [jnp.where(colors[q] == 0.0, known[q] * scale[q], zero) for q in range(6)]
        cols = {q: columns(z[q]) for q in range(6)}
        for pieces, slots in ((outer, (2, 3)), (inner, (0, 1))):
            accs = pull([jnp.zeros((8, 128), F32) for _ in pieces], pieces, cols)
            for j, q in enumerate(pieces):
                out_buf[1, q] = jnp.sum(accs[j], axis=0, keepdims=True)
            for slot in slots:
                step_copy(slot, 1).start()
        row_buf[0] = zero

        def renew(q, color, pulled, old):
            return jnp.where(colors[q] == color, (known[q] + pulled) * scale[q], old)

        def absorb(s, z, then):
            p = s % 2
            color = (s % COLORS).astype(F32) if not isinstance(s, int) else float(s % COLORS)
            own = [out_buf[p, q] for q in range(6)]
            take = lambda i, q: in_buf[p, i, q]
            z = list(z)
            for slot in (0, 1):
                step_copy(slot, p).wait_recv()
            mid = combine_mid(own, take)
            for q in inner:
                z[q] = renew(q, color, mid[q - 2], z[q])
            accs = None
            if then:
                cols = {q: columns(z[q]) for q in inner}
                accs = pull([jnp.zeros((8, 128), F32) for _ in range(6)], range(6), cols)
            for slot in (2, 3):
                step_copy(slot, p).wait_recv()
            low, top = combine_rest(own, take)
            for j, q in enumerate(outer):
                z[q] = renew(q, color, (low + top)[j], z[q])
            return z, accs

        def step(s, z):
            p = s % 2

            @pl.when((s == 2) & moves)
            def _():
                pl.semaphore_wait(go, 1)
                mag_copy(band).start()

            @pl.when(s % COLORS == 0)
            def _():
                @pl.when(s == COLORS)
                def _():
                    for slot in range(BANDS):

                        @pl.when(jnp.logical_not(owns(slot)))
                        def _():
                            table_copy(0, slot).wait_recv()
                            mag_copy(slot).wait_recv()

                evaluate(s // COLORS - 1, z, False)

            z, accs = absorb(s, z, True)
            cols = {q: columns(z[q]) for q in outer}
            far = pull([accs[q] for q in outer], outer, cols)
            for j, q in enumerate(outer):
                out_buf[1 - p, q] = jnp.sum(far[j], axis=0, keepdims=True)
            for slot in (2, 3):
                step_copy(slot, 1 - p).start()
            near_accs = pull([accs[q] for q in inner], inner, cols)
            for j, q in enumerate(inner):
                out_buf[1 - p, q] = jnp.sum(near_accs[j], axis=0, keepdims=True)
            for slot in (0, 1):
                step_copy(slot, 1 - p).start()
            for slot in range(4):
                step_copy(slot, p).wait_send()
            return tuple(z)

        z = lax.fori_loop(1, STEPS - 1, step, tuple(z))
        z, _ = absorb(STEPS - 1, z, False)
        evaluate(SWEEPS - 1, z, True)
        for i in range(len(PLANE)):
            plane_copy(i).start()
        mine = pltpu.make_async_copy(row_buf.at[0], plane.at[x * 4 + y], plane_recv)
        mine.start()
        for slot in range(BANDS):

            @pl.when(jnp.logical_not(owns(slot)))
            def _():
                fin_copy(slot).start()

        whole(plane, plane_recv).wait()
        row_buf[1] = jnp.sum(plane[...].reshape(16, 128), axis=0, keepdims=True)
        for i in range(len(LINE)):
            line_copy(i).start()
        mine = pltpu.make_async_copy(row_buf.at[1], line.at[z_at % 4], line_recv)
        mine.start()
        for i in range(len(PLANE)):
            plane_copy(i).wait_send()
        for slot in range(4):
            step_copy(slot, (STEPS - 1) % 2).wait_send()

    @pl.when(jnp.logical_not(is_home))
    def _():
        pl.semaphore_wait(go, 1)
        mag_copy(band).start()

    @pl.when(moves)
    def _():
        @pl.when(band == teller)
        def _():
            table_copy(1, band).wait_send()

        table_copy(0, band).wait_send()
        table_copy(2, band).wait_send()
        for c in range(CHUNKS):
            for i in range(2):
                ship_copy(i, band, c).wait_send()
        mag_copy(band).wait_send()
        fin_copy(0).wait_recv()

    @pl.when(stays)
    def _():
        mine = pltpu.make_async_copy(fin.at[band], got, local.at[0])
        mine.start()
        mine.wait()

    out_ref[:, 0:256] = got[:, 0:256]
    pair = got[0:1, 256:384]
    out_ref[:, 256:512] = jnp.zeros((8, 256), F32)
    out_ref[0:1, 256:384] = jnp.where(band % 2 == 0, pair, pltpu.roll(pair, OWN, 1))

    whole(line, line_recv).wait()
    total = jnp.sum(line[...].reshape(4, 128), axis=0, keepdims=True)
    total = pltpu.roll(total, (128 - band * SWEEPS) % 128, 1)
    out_ref[0:1, 384:512] = total * (1.0 / (OBS * STARS * TILES))

    @pl.when(is_home)
    def _():
        for slot in range(BANDS):

            @pl.when(jnp.logical_not(owns(slot)))
            def _():
                fin_copy(slot).wait_send()

        for i in range(len(LINE)):
            line_copy(i).wait_send()


def solve(color_terms, m, w, s, owner, colors, lists):
    vmem = pl.BlockSpec(memory_space=pltpu.VMEM)
    hbm = pl.BlockSpec(memory_space=pl.ANY)
    dma = pltpu.SemaphoreType.DMA
    return pl.pallas_call(
        solve_kernel,
        out_shape=pltpu.VMEM((8, 512), F32),
        in_specs=[hbm] * 7,
        out_specs=vmem,
        scratch_shapes=[
            pltpu.SMEM(color_terms.shape, F32),
            pltpu.VMEM((OBS, STARS), F32),
            pltpu.VMEM((OBS, STARS), F32),
            pltpu.VMEM((OBS, STARS), jnp.int32),
            pltpu.VMEM(owner.shape, jnp.int32),
            pltpu.VMEM(colors.shape, jnp.int32),
            pltpu.VMEM(lists.shape, jnp.int32),
            pltpu.VMEM((BLOCKS, ROWS), F32),
            pltpu.VMEM((BANDS, BLOCKS, ROWS), F32),
            pltpu.VMEM((8, 128), F32),
            pltpu.VMEM((8, 384), F32),
            pltpu.VMEM((BANDS, OBS, STARS), F32),
            pltpu.VMEM((BANDS, OBS, STARS), F32),
            pltpu.VMEM((BANDS, OBS, STARS), jnp.int32),
            pltpu.VMEM((BANDS, BLOCKS, ROWS), F32),
            pltpu.VMEM((BANDS, 8, 128), F32),
            pltpu.VMEM((8, 384), F32),
            pltpu.VMEM((BANDS, BLOCKS * LIST, ROWS), F32),
            pltpu.VMEM((2, BANDS, BLOCKS * LIST, WIDE), BF16),
            pltpu.VMEM((WIDE, WIDE), F32),
            pltpu.VMEM((3, 128, 512), BF16),
            pltpu.VMEM((2, 6, 1, 128), F32),
            pltpu.VMEM((2, 4, 6, 1, 128), F32),
            pltpu.VMEM((2, 6, 1, 128), F32),
            pltpu.VMEM((2, 4, 6, 1, 128), F32),
            pltpu.VMEM((BANDS, 8, 384), F32),
            pltpu.VMEM((8, 384), F32),
            pltpu.VMEM((2, 1, 128), F32),
            pltpu.VMEM((16, 1, 128), F32),
            pltpu.VMEM((4, 1, 128), F32),
            dma((7,)),
            dma((BANDS - 1,)),
            dma((BANDS - 1,)),
            dma((2, CHUNKS)),
            dma((BANDS, 2, CHUNKS)),
            dma,
            dma((BANDS,)),
            dma((3,)),
            dma((BANDS, 3)),
            dma((5,)),
            dma((2, 4)),
            dma((2, 4)),
            dma((2, 4)),
            dma((2, 4)),
            dma((BANDS,)),
            dma,
            dma((len(PLANE),)),
            dma,
            dma((len(LINE),)),
            dma,
            pltpu.SemaphoreType.REGULAR,
        ],
        compiler_params=pltpu.CompilerParams(has_side_effects=True, collective_id=0),
        name="solve",
    )(color_terms, m, w, s, owner, colors, lists)


def unpack_kernel(out_ref, zp_ref, mags_ref, mis_ref):
    zp_ref[...] = out_ref[0:1, 256 : 256 + OWN]
    mis_ref[...] = out_ref[0:1, 384 : 384 + SWEEPS]
    for blk in range(BLOCKS):
        mags_ref[0:1, blk * ROWS : (blk + 1) * ROWS] = out_ref[blk : blk + 1, 0:ROWS]


def body(magnitudes, weights, slots, block_fields, owner, colors, color_terms):
    out = solve(
        color_terms, magnitudes[0], weights[0], slots[0],
        owner.reshape(-1, 128), colors.reshape(-1, 128), block_fields,
    )
    vmem = pl.BlockSpec(memory_space=pltpu.VMEM)
    out = pltpu.with_memory_space_constraint(out, pltpu.VMEM)
    zp, mags, misfit = pl.pallas_call(
        unpack_kernel,
        out_shape=(
            jax.ShapeDtypeStruct((1, OWN), F32),
            jax.ShapeDtypeStruct((1, STARS), F32),
            jax.ShapeDtypeStruct((1, SWEEPS), F32),
        ),
        in_specs=[vmem],
        out_specs=(vmem,) * 3,
        name="unpack",
    )(out)
    return zp, mags, misfit.T


def solution(mesh):
    in_specs = (
        P("band", None, "sky"),
        P("band", None, "sky"),
        P("band", None, "sky"),
        P("sky", None),
        P(),
        P(),
        P(),
    )
    out_specs = (P("band", "sky"), P("band", "sky"), P(None, "band"))
    return jax.shard_map(body, mesh=mesh, in_specs=in_specs, out_specs=out_specs, check_vma=False)
```
